32 devices in a mesh: dp: 2 (over x), tp: 4 (over z), sp: 4 (over y, core).
Axes of the slice: x: 2, y: 2, z: 4, core: 2. Of those that a mesh axis runs over, the one named last changes fastest.
Arguments:
- hidden: bfloat16 [512, 6144], P('dp'), parts along dimension 0
- ln_gain: bfloat16 [6144], replicated
- ln_bias: bfloat16 [6144], replicated
- w_q: bfloat16 [6144, 6144], P(None, 'tp')
- w_k: bfloat16 [6144, 1024], P(None, 'tp')
- w_v: bfloat16 [6144, 1024], P(None, 'tp')
- w_o: bfloat16 [6144, 6144], P('tp')
- k_cache: bfloat16 [512, 512, 8, 128], P('dp', 'sp', 'tp'), parts along dimension 0
- v_cache: bfloat16 [512, 512, 8, 128], P('dp', 'sp', 'tp'), parts along dimension 0
- lengths: int32 [512], P('dp'), parts along dimension 0
Outputs:
- output 1: bfloat16 [512, 6144], P('dp'), parts along dimension 0
- output 2: bfloat16 [512, 8, 128], P('dp', 'tp'), parts along dimension 0
- output 3: bfloat16 [512, 8, 128], P('dp', 'tp'), parts along dimension 0
There are 2 independent parts. The reference program is written for one: setup_inputs(seed, part) draws one part's arguments, and reference() takes and returns one part's arrays. A program takes and returns all parts, laid end to end along the dimension named above; an argument that names none is the same for every part.
All inputs are finite; a program needn't handle non-finite values.
Results may differ from the reference program's by a relative error of at most 0.00411564.
Values sent between devices are 32-bit elements.
A program may use at most 1 GiB of HBM per device.

```python
import jax
import jax.numpy as jnp
from jax import lax

D_MODEL = 6144
Q_HEADS = 48
KV_HEADS = 8
HEAD_DIM = 128
BATCH_ROWS = 256
SEQ_LEN = 512
GROUP_SIZE = Q_HEADS // KV_HEADS
ROT_DIM = HEAD_DIM // 2


def norm_one_plus(hidden, ln_gain, ln_bias):
    wide = hidden.astype(jnp.float32)
    row_mean = jnp.mean(wide, axis=-1, keepdims=True)
    centred = wide - row_mean
    row_var = jnp.mean(centred * centred, axis=-1, keepdims=True)
    scaled = centred * lax.rsqrt(row_var + 1e-5)
    return (scaled * (1.0 + ln_gain.astype(jnp.float32)) + ln_bias.astype(jnp.float32)).astype(jnp.bfloat16)


def rotate_first(head_vecs, rot_pos):
    half_rot = ROT_DIM // 2
    inv_freq = 10000.0 ** (-2.0 * jnp.arange(half_rot, dtype=jnp.float32) / ROT_DIM)
    rot_angle = rot_pos.astype(jnp.float32)[..., None] * inv_freq
    cos_part = jnp.cos(rot_angle)
    sin_part = jnp.sin(rot_angle)
    lead_part = head_vecs[..., :half_rot]
    tail_part = head_vecs[..., half_rot:ROT_DIM]
    return jnp.concatenate([lead_part * cos_part - tail_part * sin_part, tail_part * cos_part + lead_part * sin_part, head_vecs[..., ROT_DIM:]], axis=-1)


def setup_inputs(seed: int = 0, part: int = 0) -> dict:
    shared_keys = jax.random.split(jax.random.key(seed), 6)
    part_keys = jax.random.split(jax.random.fold_in(jax.random.key(seed), part), 6)
    q_width = Q_HEADS * HEAD_DIM
    kv_width = KV_HEADS * HEAD_DIM
    seg_count = 16
    seg_len = SEQ_LEN // seg_count
    hidden = jax.random.normal(part_keys[0], (BATCH_ROWS, D_MODEL), jnp.float32)
    ln_gain = 0.5 * jax.random.normal(shared_keys[0], (D_MODEL,), jnp.float32)
    ln_bias = 0.5 * jax.random.normal(shared_keys[1], (D_MODEL,), jnp.float32)
    w_q = jax.random.normal(shared_keys[2], (D_MODEL, q_width), jnp.float32) * D_MODEL ** -0.5
    w_k = jax.random.normal(shared_keys[3], (D_MODEL, kv_width), jnp.float32) * D_MODEL ** -0.5
    w_v = jax.random.normal(shared_keys[4], (D_MODEL, kv_width), jnp.float32) * D_MODEL ** -0.5
    w_o = jax.random.normal(shared_keys[5], (q_width, D_MODEL), jnp.float32) * q_width ** -0.5
    seg_shape = (BATCH_ROWS, seg_count, 1, KV_HEADS, HEAD_DIM)
    full_shape = (BATCH_ROWS, seg_count, seg_len, KV_HEADS, HEAD_DIM)
    cache_shape = (BATCH_ROWS, SEQ_LEN, KV_HEADS, HEAD_DIM)
    k_cache = (jax.random.normal(part_keys[1], seg_shape, jnp.float32) + jax.random.normal(part_keys[2], full_shape, jnp.float32)).reshape(cache_shape)
    v_cache = (1.5 * jax.random.normal(part_keys[3], seg_shape, jnp.float32) + 0.5 * jax.random.normal(part_keys[4], full_shape, jnp.float32)).reshape(cache_shape)
    lengths = jax.random.randint(part_keys[5], (BATCH_ROWS,), SEQ_LEN // 8, SEQ_LEN, dtype=jnp.int32)
    lengths = lengths.at[0].set(SEQ_LEN - 1).at[BATCH_ROWS - 1].set(SEQ_LEN // 8)
    return {'hidden': hidden.astype(jnp.bfloat16), 'ln_gain': ln_gain.astype(jnp.bfloat16), 'ln_bias': ln_bias.astype(jnp.bfloat16), 'w_q': w_q.astype(jnp.bfloat16), 'w_k': w_k.astype(jnp.bfloat16), 'w_v': w_v.astype(jnp.bfloat16), 'w_o': w_o.astype(jnp.bfloat16), 'k_cache': k_cache.astype(jnp.bfloat16), 'v_cache': v_cache.astype(jnp.bfloat16), 'lengths': lengths}


def reference(hidden, ln_gain, ln_bias, w_q, w_k, w_v, w_o, k_cache, v_cache, lengths):
    normed = norm_one_plus(hidden, ln_gain, ln_bias)
    q_proj = jnp.dot(normed, w_q, preferred_element_type=jnp.float32).reshape(BATCH_ROWS, KV_HEADS, GROUP_SIZE, HEAD_DIM)
    queries = rotate_first(q_proj, lengths[:, None, None]).astype(jnp.bfloat16)
    k_proj = jnp.dot(normed, w_k, preferred_element_type=jnp.float32).reshape(BATCH_ROWS, KV_HEADS, HEAD_DIM)
    k_new = rotate_first(k_proj, lengths[:, None]).astype(jnp.bfloat16)
    v_new = jnp.dot(normed, w_v, preferred_element_type=jnp.float32).astype(jnp.bfloat16).reshape(BATCH_ROWS, KV_HEADS, HEAD_DIM)
    score_scale = HEAD_DIM ** -0.5
    positions = jnp.arange(SEQ_LEN)

    def one_sequence(row_args):
        q_row, k_row, v_row, k_self, v_self, length = row_args
        q_wide = q_row.astype(jnp.float32)
        scores = jnp.einsum('kgd,skd->kgs', q_wide, k_row.astype(jnp.float32)) * score_scale
        scores = jnp.where(positions < length, scores, -jnp.inf)
        self_score = jnp.einsum('kgd,kd->kg', q_wide, k_self.astype(jnp.float32)) * score_scale
        row_max = jnp.maximum(jnp.max(scores, axis=-1), self_score)
        weights = jnp.exp(scores - row_max[..., None])
        self_weight = jnp.exp(self_score - row_max)
        weight_sum = jnp.sum(weights, axis=-1) + self_weight
        narrow_w = weights.astype(jnp.bfloat16).astype(jnp.float32)
        weighted = jnp.einsum('kgs,skd->kgd', narrow_w, v_row.astype(jnp.float32))
        weighted = weighted + self_weight[..., None] * v_self.astype(jnp.float32)[:, None, :]
        return (weighted / weight_sum[..., None]).astype(jnp.bfloat16)

    context = lax.map(one_sequence, (queries, k_cache, v_cache, k_new, v_new, lengths))
    attn_out = jnp.dot(context.reshape(BATCH_ROWS, Q_HEADS * HEAD_DIM), w_o, preferred_element_type=jnp.float32)
    out = (hidden.astype(jnp.float32) + attn_out).astype(jnp.bfloat16)
    return (out, k_new, v_new)
```

```python
import functools

import jax
import jax.numpy as jnp
import numpy as np
from jax import lax
from jax.experimental import pallas as pl
from jax.experimental.pallas import tpu as pltpu
from jax.sharding import PartitionSpec as P

F32 = jnp.float32
BF16 = jnp.bfloat16
MESH = pl.DeviceIdType.MESH
NEG = -0.7 * float(np.finfo(np.float32).max)
VMEM_LIMIT = 60 * 1024 * 1024
ANY = pl.BlockSpec(memory_space=pl.ANY)
VMEM = pl.BlockSpec(memory_space=pltpu.VMEM)


def qkv_kernel(gain_ref, bias_ref, cos_ref, sin_ref, x_hbm, wq_hbm, wk_hbm, wv_hbm,
               q_out, k_out, v_out, xbuf, hbuf, wbuf, qf, kf, xsem, wsem):
    rows, width = xbuf.shape
    n_q = wq_hbm.shape[1] // 256

    pltpu.make_async_copy(x_hbm, xbuf, xsem).start()

    def q_copy(i):
        return pltpu.make_async_copy(wq_hbm.at[:, pl.ds(i * 256, 256)], wbuf.at[i], wsem.at[i])

    k_copy = pltpu.make_async_copy(wk_hbm, wbuf.at[n_q], wsem.at[n_q])
    v_copy = pltpu.make_async_copy(wv_hbm, wbuf.at[n_q + 1], wsem.at[n_q + 1])
    for i in range(n_q):
        q_copy(i).start()
    k_copy.start()
    v_copy.start()

    qf[...] = jnp.zeros_like(qf)
    pltpu.make_async_copy(x_hbm, xbuf, xsem).wait()
    gain = 1.0 + gain_ref[...].astype(F32)
    bias = bias_ref[...].astype(F32)

    def norm(i, carry):
        at = pl.ds(pl.multiple_of(i * 16, 16), 16)
        wide = xbuf[at, :].astype(F32)
        mean = jnp.sum(wide, axis=-1, keepdims=True) * (1.0 / width)
        centred = wide - mean
        var = jnp.sum(centred * centred, axis=-1, keepdims=True) * (1.0 / width)
        hbuf[at, :] = (centred * lax.rsqrt(var + 1e-5) * gain + bias).astype(BF16)
        return carry

    lax.fori_loop(0, rows // 16, norm, 0)

    lane = lax.broadcasted_iota(jnp.int32, (rows, 128), 1)

    def rotate(u):
        other = jnp.where(lane < 32, -pltpu.roll(u, 96, 1), pltpu.roll(u, 32, 1))
        turned = u * cos_ref[...] + other * sin_ref[...]
        return jnp.where(lane < 64, turned, u)

    def project(i):
        return jnp.dot(hbuf[...], wbuf[i], preferred_element_type=F32)

    def q_tile(i, carry):
        q_copy(i).wait()
        prod = project(i)
        for head in range(2):
            qf[pl.ds(2 * i + head, rows, stride=16), :] = rotate(prod[:, head * 128:(head + 1) * 128])
        return carry

    lax.fori_loop(0, n_q, q_tile, 0)
    k_copy.wait()
    prod = project(n_q)
    for head in range(2):
        kf[pl.ds(head, rows, stride=2), :] = rotate(prod[:, head * 128:(head + 1) * 128])
    k_out[...] = kf[...].astype(BF16)
    v_copy.wait()
    prod = project(n_q + 1)
    for head in range(2):
        kf[pl.ds(head, rows, stride=2), :] = prod[:, head * 128:(head + 1) * 128]
    v_out[...] = kf[...].astype(BF16)
    q_out[...] = qf[...].astype(BF16)


def qkv(hidden, gain, bias, cos, sin, w_q, w_k, w_v):
    rows, width = hidden.shape
    n_tiles = w_q.shape[1] // 256 + 2
    return pl.pallas_call(
        qkv_kernel,
        out_shape=(jax.ShapeDtypeStruct((rows * 16, 128), BF16),
                   jax.ShapeDtypeStruct((rows * 2, 128), BF16),
                   jax.ShapeDtypeStruct((rows * 2, 128), BF16)),
        in_specs=[VMEM, VMEM, VMEM, VMEM, ANY, ANY, ANY, ANY],
        out_specs=(VMEM, VMEM, VMEM),
        scratch_shapes=[pltpu.VMEM((rows, width), BF16), pltpu.VMEM((rows, width), BF16),
                        pltpu.VMEM((n_tiles, width, 256), BF16),
                        pltpu.VMEM((rows * 16, 128), F32), pltpu.VMEM((rows * 2, 128), F32),
                        pltpu.SemaphoreType.DMA, pltpu.SemaphoreType.DMA((n_tiles,))],
        compiler_params=pltpu.CompilerParams(vmem_limit_bytes=VMEM_LIMIT),
        name="qkv",
    )(gain.reshape(1, width), bias.reshape(1, width), cos, sin, hidden, w_q, w_k, w_v)


def attend_kernel(len_ref, q_ref, kn_ref, vn_ref, k_ref, v_ref, o_ref, stat, *, positions, scale):
    step = pl.program_id(0)
    first = lax.axis_index("sp") * positions
    col = lax.broadcasted_iota(jnp.int32, (16, 2 * positions), 1)
    row = lax.broadcasted_iota(jnp.int32, (16, 2 * positions), 0)
    group = jnp.where(row >= 6, 1, 0)
    place = jnp.where(lax.rem(col, 2) == group, first + col // 2, 1 << 30)
    row16 = lax.broadcasted_iota(jnp.int32, (16, 16), 0)
    col16 = lax.broadcasted_iota(jnp.int32, (16, 16), 1)
    group16 = jnp.where(row16 >= 6, 1, 0)
    lane = lax.broadcasted_iota(jnp.int32, (16, 128), 1)
    pick_row = lax.broadcasted_iota(jnp.int32, (128, 16), 0)
    pick_col = lax.broadcasted_iota(jnp.int32, (128, 16), 1)
    pick = pick_col == 2 * (pick_row // 16) + jnp.where(lax.rem(pick_row, 16) >= 6, 1, 0)
    pick = jnp.where(pick, 1.0, 0.0).astype(BF16)
    nt = (((1,), (1,)), ((), ()))
    stat[...] = jnp.zeros_like(stat)
    for half in range(2):
        q8 = q_ref[half * 128:(half + 1) * 128, :]
        self8 = lax.dot_general(q8, kn_ref[half * 16:(half + 1) * 16, :], nt, preferred_element_type=F32) * scale
        v8 = jnp.dot(pick, vn_ref[half * 16:(half + 1) * 16, :], preferred_element_type=F32)
        for b in range(8):
            length = len_ref[step * 16 + half * 8 + b]
            owner = (length >= first) & (length < first + positions)
            s = lax.dot_general(q8[b * 16:(b + 1) * 16, :], k_ref[half * 8 + b], nt, preferred_element_type=F32) * scale
            s = jnp.where(place < length, s, NEG)
            mine = jnp.where(col16 == 2 * b + group16, self8[b * 16:(b + 1) * 16, :], NEG)
            own = jnp.max(mine, axis=1, keepdims=True)
            own = jnp.where(owner, own, NEG)
            top = jnp.maximum(jnp.max(s, axis=1, keepdims=True), own)
            w = jnp.exp(s - top)
            w_own = jnp.exp(own - top)
            total = jnp.sum(w, axis=1, keepdims=True) + w_own
            acc = jnp.dot(w.astype(BF16), v_ref[half * 8 + b], preferred_element_type=F32)
            acc = acc + w_own * v8[b * 16:(b + 1) * 16, :]
            o_ref[half, b * 12:(b + 1) * 12, :] = acc[:12, :]
            pair = jnp.where(lane == 0, top, total)
            stat[half, b * 12:(b + 1) * 12, :] = pair[:12, :]
        o_ref[half, 96:104, :] = jnp.transpose(stat[half])[:8, :]


def attend(lengths, q, k_new, v_new, k_cache, v_cache):
    batch, positions, kv, head = k_cache.shape
    k_rows = k_cache.reshape(batch, positions * kv, head)
    v_rows = v_cache.reshape(batch, positions * kv, head)
    steps = batch // 16
    return pl.pallas_call(
        functools.partial(attend_kernel, positions=positions, scale=head ** -0.5),
        out_shape=jax.ShapeDtypeStruct((batch // 8, 104, 128), F32),
        grid_spec=pltpu.PrefetchScalarGridSpec(
            num_scalar_prefetch=1, grid=(steps,),
            in_specs=[pl.BlockSpec((256, 128), lambda i, n: (i, 0)),
                      pl.BlockSpec((32, 128), lambda i, n: (i, 0)),
                      pl.BlockSpec((32, 128), lambda i, n: (i, 0)),
                      pl.BlockSpec((16, positions * kv, head), lambda i, n: (i, 0, 0)),
                      pl.BlockSpec((16, positions * kv, head), lambda i, n: (i, 0, 0))],
            out_specs=pl.BlockSpec((2, 104, 128), lambda i, n: (i, 0, 0)),
            scratch_shapes=[pltpu.VMEM((2, 128, 128), F32)]),
        compiler_params=pltpu.CompilerParams(vmem_limit_bytes=VMEM_LIMIT),
        name="attend",
    )(lengths, q, k_new, v_new, k_rows, v_rows)


RCH = 4
QCH = 4
NMSG = RCH * QCH


def scaled_sum(a, b):
    m_a, l_a, m_b, l_b = a[96:97, :], a[97:98, :], b[96:97, :], b[97:98, :]
    top = jnp.maximum(m_a, m_b)
    f_a, f_b = jnp.exp(m_a - top), jnp.exp(m_b - top)
    total = l_a * f_a + l_b * f_b
    r = lax.broadcasted_iota(jnp.int32, (128, 128), 0)
    turned = jnp.transpose(jnp.where(r == 0, f_a, jnp.where(r == 1, f_b, total)))
    acc = a[:96, :] * turned[:96, 0:1] + b[:96, :] * turned[:96, 1:2]
    return acc, top, total, turned[:96, 2:3]


def finish_kernel(msg, x_hbm, w_hbm, out_hbm,
                  part_y, part_o, send_y, recv_y, comb_o, ctx_t, ctx_s, ctx_r, lhs, wbuf, xbuf, prod,
                  rs_in, rs_out, fin, obuf,
                  s_py, r_py, s_po, r_po, s_y, r_y, s_c, r_c, s_w, s_x,
                  s_rs, r_rs, s_ag, r_ag, s_fy, r_fy, s_fd, r_fd, s_fe, r_fe, s_out):
    d, z, s = lax.axis_index("dp"), lax.axis_index("tp"), lax.axis_index("sp")
    y, c = s // 2, s % 2
    yo, co = 1 - y, 1 - c
    u = c * z + co * (3 - z)
    partner, across = (d, z, 2 * y + co), (d, z, 2 * yo + c)
    ahead, behind = (d, z + 2 * c - 1, s), (d, z - 2 * c + 1, s)
    half = wbuf.shape[0] * wbuf.shape[2]
    width = wbuf.shape[2]

    def remote(src, dst, send, recv, dev):
        return pltpu.make_async_remote_copy(src_ref=src, dst_ref=dst, send_sem=send, recv_sem=recv,
                                            device_id=dev, device_id_type=MESH)

    barrier = pltpu.get_barrier_semaphore()
    pl.semaphore_signal(barrier, inc=1, device_id=partner, device_id_type=MESH)
    pl.semaphore_signal(barrier, inc=1, device_id=across, device_id_type=MESH)

    @pl.when(u < 3)
    def _():
        pl.semaphore_signal(barrier, inc=1, device_id=ahead, device_id_type=MESH)

    @pl.when(u > 0)
    def _():
        pl.semaphore_signal(barrier, inc=1, device_id=behind, device_id_type=MESH)

    def w_copy(q):
        return pltpu.make_async_copy(w_hbm.at[:, pl.ds(c * half + q * width, width)], wbuf.at[q], s_w.at[q])

    x_copy = pltpu.make_async_copy(x_hbm.at[pl.ds(y * 128, 128), pl.ds(c * half, half)], xbuf, s_x)

    pl.semaphore_wait(barrier, 2 + (z + 2) // 3 + (5 - z) // 3)

    def block(h, r, core):
        return msg.at[pl.ds(16 * h + 4 * r + 2 * core, 2)]

    def to_partner_y(r):
        return remote(block(yo, r, co), part_y.at[r], s_py.at[r], r_py.at[r], partner)

    def to_partner_o(r):
        return remote(block(y, r, co), part_o.at[r], s_po.at[r], r_po.at[r], partner)

    def to_across(r):
        return remote(send_y.at[r], recv_y.at[r], s_y.at[r], r_y.at[r], across)

    def ctx_copy(r):
        return remote(ctx_s.at[r], ctx_r.at[r], s_c.at[r], r_c.at[r], partner)

    for r in range(RCH):
        to_partner_y(r).start()
    for r in range(RCH):
        to_partner_o(r).start()
    for q in range(QCH):
        w_copy(q).start()
    x_copy.start()

    def put(dst, k, acc, top, total):
        dst[k, :96, :] = acc
        row = lax.broadcasted_iota(jnp.int32, (8, 128), 0)
        dst[k, 96:104, :] = jnp.where(row == 0, top, total)

    def other_rows(r, carry):
        to_partner_y(r).wait_recv()
        for k in range(2):
            acc, top, total, _ = scaled_sum(msg[16 * yo + 4 * r + 2 * c + k], part_y[r, k])
            put(send_y.at[r], k, acc, top, total)
        to_across(r).start()
        return carry

    lax.fori_loop(0, RCH, other_rows, 0)

    def own_rows(r, carry):
        to_partner_o(r).wait_recv()
        for k in range(2):
            acc, top, total, _ = scaled_sum(msg[16 * y + 4 * r + 2 * c + k], part_o[r, k])
            put(comb_o.at[r], k, acc, top, total)
        return carry

    lax.fori_loop(0, RCH, own_rows, 0)

    def context(r):
        to_across(r).wait_recv()
        for k in range(2):
            acc, _, _, total = scaled_sum(comb_o[r, k], recv_y[r, k])
            ctx_t[...] = acc / total
            for h in range(12):
                ctx_s[r, k * 8:(k + 1) * 8, h * 128:(h + 1) * 128] = ctx_t[pl.ds(h, 8, stride=12), :]
        ctx_copy(r).start()

    context(0)
    x_copy.wait()
    for q in range(QCH):
        w_copy(q).wait()

    def rs(j):
        return remote(rs_out.at[j], rs_in.at[j], s_rs.at[j], r_rs.at[j], ahead)

    def ag(j):
        f = fin.at[y, c, j]
        return remote(f, f, s_ag.at[j], r_ag.at[j], behind)

    def fy(j):
        f = fin.at[y, c, j]
        return remote(f, f, s_fy.at[j], r_fy.at[j], across)

    def fy_in(j):
        f = fin.at[yo, c, j]
        return remote(f, f, s_fy.at[j], r_fy.at[j], across)

    def fd(j):
        f = fin.at[y, c, j]
        return remote(f, f, s_fd.at[j], r_fd.at[j], partner)

    def fd_in(j):
        f = fin.at[y, co, j]
        return remote(f, f, s_fd.at[j], r_fd.at[j], partner)

    def fe(j):
        f = fin.at[yo, c, j]
        return remote(f, f, s_fe.at[j], r_fe.at[j], partner)

    def fe_in(j):
        f = fin.at[yo, co, j]
        return remote(f, f, s_fe.at[j], r_fe.at[j], partner)

    lag = 4 * (3 - u)
    lag_y = lag + 4

    def tick(t, carry):
        @pl.when(t < NMSG)
        def _():
            r, q = t // QCH, t % QCH

            @pl.when(q == 0)
            def _():
                ctx_copy(r).wait_recv()
                lhs[c] = ctx_s[r].astype(BF16)
                lhs[co] = ctx_r[r].astype(BF16)

            prod[...] = jnp.dot(lhs[...].reshape(32, lhs.shape[2]), wbuf[q], preferred_element_type=F32)

            @pl.when(u == 0)
            def _():
                rs_out[t] = prod[...]
                rs(t).start()

            @pl.when((u > 0) & (u < 3))
            def _():
                rs(t).wait_recv()
                rs_out[t] = rs_in[t] + prod[...]
                rs(t).start()

            @pl.when(u == 3)
            def _():
                rs(t).wait_recv()
                x = xbuf[pl.ds(pl.multiple_of(r * 32, 32), 32), pl.ds(pl.multiple_of(q * width, width), width)]
                fin[y, c, t] = rs_in[t] + prod[...] + x.astype(F32)
                ag(t).start()
                fy(t).start()
                fd(t).start()

            @pl.when((q == 1) & (r < RCH - 1))
            def _():
                context(r + 1)

        ta = t - lag

        @pl.when((u < 3) & (ta >= 0) & (ta < NMSG))
        def _():
            ag(ta).wait_recv()

            @pl.when(u > 0)
            def _():
                ag(ta).start()

            fy(ta).start()
            fd(ta).start()

        ty = t - lag_y

        @pl.when((ty >= 0) & (ty < NMSG))
        def _():
            fy_in(ty).wait_recv()
            fe(ty).start()

        return carry

    lax.fori_loop(0, NMSG + lag_y, tick, 0)

    def out_copy(h, r):
        at = pl.ds(h * 128 + r * 32, 32)
        return pltpu.make_async_copy(obuf.at[at], out_hbm.at[at], s_out.at[h, r])

    def convert(j, carry):
        r, q = j // QCH, j % QCH
        fd_in(j).wait_recv()
        fe_in(j).wait_recv()
        for h in range(2):
            at = pl.ds(pl.multiple_of(h * 128 + r * 32, 32), 32)
            for k in range(2):
                obuf[at, pl.ds(pl.multiple_of(k * half + q * width, width), width)] = fin[h, k, j].astype(BF16)

        @pl.when(q == QCH - 1)
        def _():
            out_copy(0, r).start()
            out_copy(1, r).start()

        return carry

    lax.fori_loop(0, NMSG, convert, 0)

    def drain(j, carry):
        @pl.when(u < 3)
        def _():
            rs(j).wait_send()

        @pl.when(u > 0)
        def _():
            ag(j).wait_send()

        fy(j).wait_send()
        fd(j).wait_send()
        fe(j).wait_send()
        return carry

    lax.fori_loop(0, NMSG, drain, 0)
    for r in range(RCH):
        to_partner_y(r).wait_send()
        to_partner_o(r).wait_send()
        to_across(r).wait_send()
        ctx_copy(r).wait_send()
        out_copy(0, r).wait()
        out_copy(1, r).wait()


def finish(msg, hidden, w_o):
    rows, width = hidden.shape
    depth = w_o.shape[0]
    half = width // 2
    cols = half // QCH
    dma = pltpu.SemaphoreType.DMA
    part = pltpu.VMEM((RCH, 2, 104, 128), F32)
    return pl.pallas_call(
        finish_kernel,
        out_shape=jax.ShapeDtypeStruct((rows, width), BF16),
        in_specs=[VMEM, ANY, ANY],
        out_specs=ANY,
        scratch_shapes=[part, part, part, part, part,
                        pltpu.VMEM((96, 128), F32),
                        pltpu.VMEM((RCH, 16, depth), F32), pltpu.VMEM((RCH, 16, depth), F32),
                        pltpu.VMEM((2, 16, depth), BF16),
                        pltpu.VMEM((QCH, depth, cols), BF16),
                        pltpu.VMEM((rows // 2, half), BF16),
                        pltpu.VMEM((32, cols), F32),
                        pltpu.VMEM((NMSG, 32, cols), F32), pltpu.VMEM((NMSG, 32, cols), F32),
                        pltpu.VMEM((2, 2, NMSG, 32, cols), F32),
                        pltpu.VMEM((rows, width), BF16),
                        dma((RCH,)), dma((RCH,)), dma((RCH,)), dma((RCH,)), dma((RCH,)), dma((RCH,)),
                        dma((RCH,)), dma((RCH,)), dma((QCH,)), dma,
                        dma((NMSG,)), dma((NMSG,)), dma((NMSG,)), dma((NMSG,)), dma((NMSG,)), dma((NMSG,)),
                        dma((NMSG,)), dma((NMSG,)), dma((NMSG,)), dma((NMSG,)), dma((2, RCH))],
        compiler_params=pltpu.CompilerParams(collective_id=0, has_side_effects=True, vmem_limit_bytes=VMEM_LIMIT),
        name="finish",
    )(msg, hidden, w_o)


def solution(mesh):
    def local_step(hidden, ln_gain, ln_bias, w_q, w_k, w_v, w_o, k_cache, v_cache, lengths):
        batch, _, kv, head = k_cache.shape
        freq = 10000.0 ** (-2.0 * np.arange(32, dtype=np.float32) / np.float32(64))
        freq = np.concatenate([freq, freq, np.zeros(64)]).astype(np.float32)
        angle = lengths.astype(F32)[:, None] * freq
        q, k_new, v_new = qkv(hidden, ln_gain, ln_bias, jnp.cos(angle), jnp.sin(angle), w_q, w_k, w_v)
        msg = attend(lengths, q, k_new, v_new, k_cache, v_cache)
        out = finish(msg, hidden, w_o)
        return out, k_new.reshape(batch, kv, head), v_new.reshape(batch, kv, head)

    row_spec = P('dp', None)
    cache_spec = P('dp', 'sp', 'tp', None)
    head_spec = P('dp', 'tp', None)
    return jax.shard_map(local_step, mesh=mesh, in_specs=(row_spec, P(None), P(None), P(None, 'tp'), P(None, 'tp'), P(None, 'tp'), P('tp', None), cache_spec, cache_spec, P('dp')), out_specs=(row_spec, head_spec, head_spec), check_vma=False)
```

```python
import functools

import jax
import jax.numpy as jnp
import numpy as np
from jax import lax
from jax.experimental import pallas as pl
from jax.experimental.pallas import tpu as pltpu
from jax.sharding import PartitionSpec as P

F32 = jnp.float32
BF16 = jnp.bfloat16
MESH = pl.DeviceIdType.MESH
NEG = -0.7 * float(np.finfo(np.float32).max)
VMEM_LIMIT = 60 * 1024 * 1024
ANY = pl.BlockSpec(memory_space=pl.ANY)
VMEM = pl.BlockSpec(memory_space=pltpu.VMEM)


def qkv_kernel(len_ref, freq_ref, gain_ref, bias_ref, x_hbm, wq_hbm, wk_hbm, wv_hbm,
               q_out, k_out, v_out, xbuf, hbuf, wbuf, pbuf, qf, kf, cosb, sinb, gainb, biasb, xsem, wsem):
    rows, width = xbuf.shape
    n_q = wq_hbm.shape[1] // 256
    tiles = width // 128

    x_copy = pltpu.make_async_copy(x_hbm, xbuf, xsem)
    x_copy.start()

    def q_copy(i):
        return pltpu.make_async_copy(wq_hbm.at[:, pl.ds(i * 256, 256)], wbuf.at[i], wsem.at[i])

    k_copy = pltpu.make_async_copy(wk_hbm, wbuf.at[n_q], wsem.at[n_q])
    v_copy = pltpu.make_async_copy(wv_hbm, wbuf.at[n_q + 1], wsem.at[n_q + 1])
    for i in range(n_q):
        q_copy(i).start()
    k_copy.start()
    v_copy.start()

    for k in range(tiles):
        gainb[:, k * 128:(k + 1) * 128] = jnp.broadcast_to(1.0 + gain_ref[k:k + 1, :].astype(F32), (8, 128))
        biasb[:, k * 128:(k + 1) * 128] = jnp.broadcast_to(bias_ref[k:k + 1, :].astype(F32), (8, 128))
    for i in range(rows // 128):
        place = jnp.transpose(jnp.broadcast_to(len_ref[i:i + 1, :].astype(F32), (128, 128)))
        angle = place * freq_ref[...]
        cosb[i * 128:(i + 1) * 128, :] = jnp.cos(angle)
        sinb[i * 128:(i + 1) * 128, :] = jnp.sin(angle)

    x_copy.wait()

    def norm(i, carry):
        ats = [pl.ds(pl.multiple_of(i * 64 + j * 16, 16), 16) for j in range(4)]
        lanes = [slice(k * 128, (k + 1) * 128) for k in range(tiles)]
        means, scales = [], []
        for at in ats:
            accs = [xbuf[at, lanes[k]].astype(F32) for k in range(2)]
            for k in range(2, tiles):
                accs[k % 2] = accs[k % 2] + xbuf[at, lanes[k]].astype(F32)
            mean = jnp.sum(accs[0] + accs[1], axis=-1, keepdims=True) * (1.0 / width)
            means.append(jnp.broadcast_to(mean, (16, 128)))
        for at, mean in zip(ats, means):
            accs = [jnp.zeros((16, 128), F32) for _ in range(2)]
            for k in range(tiles):
                centred = xbuf[at, lanes[k]].astype(F32) - mean
                accs[k % 2] = accs[k % 2] + centred * centred
            var = jnp.sum(accs[0] + accs[1], axis=-1, keepdims=True) * (1.0 / width)
            scales.append(jnp.broadcast_to(lax.rsqrt(var + 1e-5), (16, 128)))
        for k in range(tiles):
            gain = jnp.concatenate([gainb[:, lanes[k]]] * 2, axis=0)
            bias = jnp.concatenate([biasb[:, lanes[k]]] * 2, axis=0)
            for at, mean, scale in zip(ats, means, scales):
                hbuf[at, lanes[k]] = ((xbuf[at, lanes[k]].astype(F32) - mean) * scale * gain + bias).astype(BF16)
        return carry

    lax.fori_loop(0, rows // 64, norm, 0)

    lane = lax.broadcasted_iota(jnp.int32, (rows, 128), 1)

    def rotate(u):
        other = jnp.where(lane < 32, -pltpu.roll(u, 96, 1), pltpu.roll(u, 32, 1))
        turned = u * cosb[...] + other * sinb[...]
        return jnp.where(lane < 64, turned, u)

    def project(i):
        return jnp.dot(hbuf[...], wbuf[i], preferred_element_type=F32)

    def place_heads(i, prod):
        for head in range(2):
            u = prod[:, head * 128:(head + 1) * 128]
            qf[pl.ds(lax.rem(2 * i + head, 16), rows, stride=16), :] = jnp.where(i == n_q + 1, u, rotate(u))

    pbuf[1] = jnp.zeros((rows, 256), F32)

    def tile(i, carry):
        pltpu.make_async_copy(wk_hbm, wbuf.at[i], wsem.at[i]).wait()
        pbuf[lax.rem(i, 2)] = project(i)
        place_heads(i + n_q + 1, pbuf[lax.rem(i + 1, 2)])
        return carry

    lax.fori_loop(0, n_q + 2, tile, 0)
    place_heads(n_q + 1, pbuf[(n_q + 1) % 2])
    for ref, row in ((k_out, 12), (v_out, 14)):
        for head in range(2):
            kf[pl.ds(head, rows, stride=2), :] = qf[pl.ds(row + head, rows, stride=16), :]
        ref[...] = kf[...].astype(BF16)
    q_out[...] = qf[...].astype(BF16)


def qkv(hidden, gain, bias, lengths, w_q, w_k, w_v):
    rows, width = hidden.shape
    n_tiles = w_q.shape[1] // 256 + 2
    freq = 10000.0 ** (-2.0 * np.arange(32, dtype=np.float32) / np.float32(64))
    freq = np.concatenate([freq, freq, np.zeros(64)]).astype(np.float32).reshape(1, 128)
    return pl.pallas_call(
        qkv_kernel,
        out_shape=(jax.ShapeDtypeStruct((rows * 16, 128), BF16),
                   jax.ShapeDtypeStruct((rows * 2, 128), BF16),
                   jax.ShapeDtypeStruct((rows * 2, 128), BF16)),
        in_specs=[VMEM, VMEM, VMEM, VMEM, ANY, ANY, ANY, ANY],
        out_specs=(VMEM, VMEM, VMEM),
        scratch_shapes=[pltpu.VMEM((rows, width), BF16), pltpu.VMEM((rows, width), BF16),
                        pltpu.VMEM((n_tiles, width, 256), BF16), pltpu.VMEM((2, rows, 256), F32),
                        pltpu.VMEM((rows * 16, 128), F32), pltpu.VMEM((rows * 2, 128), F32),
                        pltpu.VMEM((rows, 128), F32), pltpu.VMEM((rows, 128), F32),
                        pltpu.VMEM((8, width), F32), pltpu.VMEM((8, width), F32),
                        pltpu.SemaphoreType.DMA, pltpu.SemaphoreType.DMA((n_tiles,))],
        compiler_params=pltpu.CompilerParams(vmem_limit_bytes=VMEM_LIMIT),
        name="qkv",
    )(lengths.reshape(rows // 128, 128), jnp.asarray(freq), gain.reshape(width // 128, 128),
      bias.reshape(width // 128, 128), hidden, w_q, w_k, w_v)


STEP8 = 4


def attend_kernel(len_ref, q_ref, kn_ref, vn_ref, k_ref, v_ref, o_ref, sbuf, self_buf, wbuf, stat, *, positions, scale):
    step = pl.program_id(0)
    first = lax.axis_index("sp") * positions
    col = lax.broadcasted_iota(jnp.int32, (16, 2 * positions), 1)
    row = lax.broadcasted_iota(jnp.int32, (16, 2 * positions), 0)
    group = jnp.where(row >= 6, 1, 0)
    place = jnp.where(lax.rem(col, 2) == group, first + col // 2, 1 << 30)
    pick_row = lax.broadcasted_iota(jnp.int32, (128, 16), 0)
    pick_col = lax.broadcasted_iota(jnp.int32, (128, 16), 1)
    pick = pick_col == 2 * (pick_row // 16) + jnp.where(lax.rem(pick_row, 16) >= 6, 1, 0)
    spread = jnp.where(pick, 1.0, 0.0).astype(BF16)
    lane = lax.broadcasted_iota(jnp.int32, (128, 128), 1)
    nt = (((1,), (1,)), ((), ()))
    own_w = [None] * STEP8

    def scores(g):
        q8 = q_ref[g * 128:(g + 1) * 128, :]
        self8 = lax.dot_general(q8, kn_ref[g * 16:(g + 1) * 16, :], nt, preferred_element_type=F32) * scale
        self8 = jnp.where(pick, self8, NEG)
        for b in range(8):
            at = slice(g * 128 + b * 16, g * 128 + (b + 1) * 16)
            length = len_ref[(step * STEP8 + g) * 8 + b]
            owner = (length >= first) & (length < first + positions)
            s = lax.dot_general(q_ref[at, :], k_ref[g * 8 + b], nt, preferred_element_type=F32) * scale
            sbuf[at, :] = jnp.where(place < length, s, NEG)
            self_buf[at, :] = jnp.where(owner, self8[b * 16:(b + 1) * 16, :], NEG)

    def weights(g):
        at = slice(g * 128, (g + 1) * 128)
        s = sbuf[at, :]
        own = jnp.max(self_buf[at, :], axis=1, keepdims=True)
        top = jnp.maximum(jnp.max(s, axis=1, keepdims=True), own)
        w = jnp.exp(s - top)
        own_w[g] = jnp.exp(own - top)
        total = jnp.sum(w, axis=1, keepdims=True) + own_w[g]
        wbuf[at, :] = w.astype(BF16)
        stat[at, :] = jnp.where(lane == 0, top, total)

    def sums(g):
        v8 = jnp.dot(spread, vn_ref[g * 16:(g + 1) * 16, :], preferred_element_type=F32)
        own8 = own_w[g] * v8
        turned = jnp.transpose(stat[g * 128:(g + 1) * 128, :])[:8, :]
        o_ref[g, 96:104, :] = jnp.concatenate([turned[:, b * 16:b * 16 + 12] for b in range(8)] + [jnp.zeros((8, 32), F32)], axis=1)
        for b in range(8):
            at = slice(g * 128 + b * 16, g * 128 + (b + 1) * 16)
            acc = jnp.dot(wbuf[at, :], v_ref[g * 8 + b], preferred_element_type=F32) + own8[b * 16:(b + 1) * 16, :]
            o_ref[g, b * 12:(b + 1) * 12, :] = acc[:12, :]

    for g in range(STEP8 + 2):
        if g < STEP8:
            scores(g)
        if 1 <= g <= STEP8:
            weights(g - 1)
        if g >= 2:
            sums(g - 2)


def attend(lengths, q, k_new, v_new, k_cache, v_cache):
    batch, positions, kv, head = k_cache.shape
    k_rows = k_cache.reshape(batch, positions * kv, head)
    v_rows = v_cache.reshape(batch, positions * kv, head)
    take = STEP8 * 8
    return pl.pallas_call(
        functools.partial(attend_kernel, positions=positions, scale=head ** -0.5),
        out_shape=jax.ShapeDtypeStruct((batch // 8, 104, 128), F32),
        grid_spec=pltpu.PrefetchScalarGridSpec(
            num_scalar_prefetch=1, grid=(batch // take,),
            in_specs=[pl.BlockSpec((take * 16, 128), lambda i, n: (i, 0)),
                      pl.BlockSpec((take * 2, 128), lambda i, n: (i, 0)),
                      pl.BlockSpec((take * 2, 128), lambda i, n: (i, 0)),
                      pl.BlockSpec((take, positions * kv, head), lambda i, n: (i, 0, 0)),
                      pl.BlockSpec((take, positions * kv, head), lambda i, n: (i, 0, 0))],
            out_specs=pl.BlockSpec((STEP8, 104, 128), lambda i, n: (i, 0, 0)),
            scratch_shapes=[pltpu.VMEM((take * 16, positions * kv), F32), pltpu.VMEM((take * 16, 16), F32),
                            pltpu.VMEM((take * 16, positions * kv), BF16), pltpu.VMEM((take * 16, 128), F32)]),
        compiler_params=pltpu.CompilerParams(vmem_limit_bytes=VMEM_LIMIT),
        name="attend",
    )(lengths, q, k_new, v_new, k_rows, v_rows)


RCH = 4
QCH = 4
NMSG = RCH * QCH


def scaled_sum(a, b):
    m_a, l_a, m_b, l_b = a[96:97, :], a[97:98, :], b[96:97, :], b[97:98, :]
    top = jnp.maximum(m_a, m_b)
    f_a, f_b = jnp.exp(m_a - top), jnp.exp(m_b - top)
    total = l_a * f_a + l_b * f_b
    r = lax.broadcasted_iota(jnp.int32, (128, 128), 0)
    turned = jnp.transpose(jnp.where(r == 0, f_a, jnp.where(r == 1, f_b, total)))
    acc = a[:96, :] * turned[:96, 0:1] + b[:96, :] * turned[:96, 1:2]
    return acc, top, total, turned[:96, 2:3]


def finish_kernel(msg, x_hbm, w_hbm, out_hbm,
                  part_y, part_o, send_y, recv_y, comb_o, ctx_t, ctx_s, ctx_r, lhs, wbuf, xbuf, prod,
                  rs_in, rs_out, fin, obuf,
                  s_py, r_py, s_po, r_po, s_y, r_y, s_c, r_c, s_w, s_x,
                  s_rs, r_rs, s_ag, r_ag, s_fy, r_fy, s_fd, r_fd, s_fe, r_fe, s_out):
    d, z, s = lax.axis_index("dp"), lax.axis_index("tp"), lax.axis_index("sp")
    y, c = s // 2, s % 2
    yo, co = 1 - y, 1 - c
    u = c * z + co * (3 - z)
    partner, across = (d, z, 2 * y + co), (d, z, 2 * yo + c)
    ahead, behind = (d, z + 2 * c - 1, s), (d, z - 2 * c + 1, s)
    half = wbuf.shape[0] * wbuf.shape[2]
    width = wbuf.shape[2]

    def remote(src, dst, send, recv, dev):
        return pltpu.make_async_remote_copy(src_ref=src, dst_ref=dst, send_sem=send, recv_sem=recv,
                                            device_id=dev, device_id_type=MESH)

    barrier = pltpu.get_barrier_semaphore()
    pl.semaphore_signal(barrier, inc=1, device_id=partner, device_id_type=MESH)
    pl.semaphore_signal(barrier, inc=1, device_id=across, device_id_type=MESH)

    @pl.when(u < 3)
    def _():
        pl.semaphore_signal(barrier, inc=1, device_id=ahead, device_id_type=MESH)

    @pl.when(u > 0)
    def _():
        pl.semaphore_signal(barrier, inc=1, device_id=behind, device_id_type=MESH)

    def w_copy(q):
        return pltpu.make_async_copy(w_hbm.at[:, pl.ds(c * half + q * width, width)], wbuf.at[q], s_w.at[q])

    x_copy = pltpu.make_async_copy(x_hbm.at[pl.ds(y * 128, 128), pl.ds(c * half, half)], xbuf, s_x)

    pl.semaphore_wait(barrier, 2 + (z + 2) // 3 + (5 - z) // 3)

    def block(h, r, core):
        return msg.at[pl.ds(16 * h + 4 * r + 2 * core, 2)]

    def to_partner_y(r):
        return remote(block(yo, r, co), part_y.at[r], s_py.at[r], r_py.at[r], partner)

    def to_partner_o(r):
        return remote(block(y, r, co), part_o.at[r], s_po.at[r], r_po.at[r], partner)

    def to_across(r):
        return remote(send_y.at[r], recv_y.at[r], s_y.at[r], r_y.at[r], across)

    def ctx_copy(r):
        return remote(ctx_s.at[r], ctx_r.at[r], s_c.at[r], r_c.at[r], partner)

    for r in range(RCH):
        to_partner_y(r).start()
    for r in range(RCH):
        to_partner_o(r).start()
    for q in range(QCH):
        w_copy(q).start()
    x_copy.start()

    def put(dst, k, acc, top, total):
        dst[k, :96, :] = acc
        row = lax.broadcasted_iota(jnp.int32, (8, 128), 0)
        dst[k, 96:104, :] = jnp.where(row == 0, top, total)

    def other_rows(r, carry):
        to_partner_y(r).wait_recv()
        for k in range(2):
            acc, top, total, _ = scaled_sum(msg[16 * yo + 4 * r + 2 * c + k], part_y[r, k])
            put(send_y.at[r], k, acc, top, total)
        to_across(r).start()
        return carry

    lax.fori_loop(0, RCH, other_rows, 0)

    def own_rows(r, carry):
        to_partner_o(r).wait_recv()
        for k in range(2):
            acc, top, total, _ = scaled_sum(msg[16 * y + 4 * r + 2 * c + k], part_o[r, k])
            put(comb_o.at[r], k, acc, top, total)
        return carry

    lax.fori_loop(0, RCH, own_rows, 0)

    def context(r):
        to_across(r).wait_recv()
        for k in range(2):
            acc, _, _, total = scaled_sum(comb_o[r, k], recv_y[r, k])
            ctx_t[...] = acc / total
            for h in range(12):
                ctx_s[r, k * 8:(k + 1) * 8, h * 128:(h + 1) * 128] = ctx_t[pl.ds(h, 8, stride=12), :]
        ctx_copy(r).start()

    context(0)
    x_copy.wait()
    for q in range(QCH):
        w_copy(q).wait()

    def rs(j):
        return remote(rs_out.at[j], rs_in.at[j], s_rs.at[j], r_rs.at[j], ahead)

    def ag(j):
        f = fin.at[y, c, j]
        return remote(f, f, s_ag.at[j], r_ag.at[j], behind)

    def fy(j):
        f = fin.at[y, c, j]
        return remote(f, f, s_fy.at[j], r_fy.at[j], across)

    def fy_in(j):
        f = fin.at[yo, c, j]
        return remote(f, f, s_fy.at[j], r_fy.at[j], across)

    def fd(j):
        f = fin.at[y, c, j]
        return remote(f, f, s_fd.at[j], r_fd.at[j], partner)

    def fd_in(j):
        f = fin.at[y, co, j]
        return remote(f, f, s_fd.at[j], r_fd.at[j], partner)

    def fe(j):
        f = fin.at[yo, c, j]
        return remote(f, f, s_fe.at[j], r_fe.at[j], partner)

    def fe_in(j):
        f = fin.at[yo, co, j]
        return remote(f, f, s_fe.at[j], r_fe.at[j], partner)

    lag = 4 * (3 - u)
    lag_y = lag + 4

    def tick(t, carry):
        @pl.when(t < NMSG)
        def _():
            r, q = t // QCH, t % QCH

            @pl.when(q == 0)
            def _():
                ctx_copy(r).wait_recv()
                lhs[c] = ctx_s[r].astype(BF16)
                lhs[co] = ctx_r[r].astype(BF16)

            prod[...] = jnp.dot(lhs[...].reshape(32, lhs.shape[2]), wbuf[q], preferred_element_type=F32)

            @pl.when(u == 0)
            def _():
                rs_out[t] = prod[...]
                rs(t).start()

            @pl.when((u > 0) & (u < 3))
            def _():
                rs(t).wait_recv()
                rs_out[t] = rs_in[t] + prod[...]
                rs(t).start()

            @pl.when(u == 3)
            def _():
                rs(t).wait_recv()
                x = xbuf[pl.ds(pl.multiple_of(r * 32, 32), 32), pl.ds(pl.multiple_of(q * width, width), width)]
                fin[y, c, t] = rs_in[t] + prod[...] + x.astype(F32)
                ag(t).start()
                fy(t).start()
                fd(t).start()

            @pl.when((q == 1) & (r < RCH - 1))
            def _():
                context(r + 1)

        ta = t - lag

        @pl.when((u < 3) & (ta >= 0) & (ta < NMSG))
        def _():
            ag(ta).wait_recv()

            @pl.when(u > 0)
            def _():
                ag(ta).start()

            fy(ta).start()
            fd(ta).start()

        ty = t - lag_y

        @pl.when((ty >= 0) & (ty < NMSG))
        def _():
            fy_in(ty).wait_recv()
            fe(ty).start()

        return carry

    lax.fori_loop(0, NMSG + lag_y, tick, 0)

    def out_copy(h, r):
        at = pl.ds(h * 128 + r * 32, 32)
        return pltpu.make_async_copy(obuf.at[at], out_hbm.at[at], s_out.at[h, r])

    def convert(j, carry):
        r, q = j // QCH, j % QCH
        fd_in(j).wait_recv()
        fe_in(j).wait_recv()
        for h in range(2):
            at = pl.ds(pl.multiple_of(h * 128 + r * 32, 32), 32)
            for k in range(2):
                obuf[at, pl.ds(pl.multiple_of(k * half + q * width, width), width)] = fin[h, k, j].astype(BF16)

        @pl.when(q == QCH - 1)
        def _():
            out_copy(0, r).start()
            out_copy(1, r).start()

        return carry

    lax.fori_loop(0, NMSG, convert, 0)

    def drain(j, carry):
        @pl.when(u < 3)
        def _():
            rs(j).wait_send()

        @pl.when(u > 0)
        def _():
            ag(j).wait_send()

        fy(j).wait_send()
        fd(j).wait_send()
        fe(j).wait_send()
        return carry

    lax.fori_loop(0, NMSG, drain, 0)
    for r in range(RCH):
        to_partner_y(r).wait_send()
        to_partner_o(r).wait_send()
        to_across(r).wait_send()
        ctx_copy(r).wait_send()
        out_copy(0, r).wait()
        out_copy(1, r).wait()


def finish(msg, hidden, w_o):
    rows, width = hidden.shape
    depth = w_o.shape[0]
    half = width // 2
    cols = half // QCH
    dma = pltpu.SemaphoreType.DMA
    part = pltpu.VMEM((RCH, 2, 104, 128), F32)
    return pl.pallas_call(
        finish_kernel,
        out_shape=jax.ShapeDtypeStruct((rows, width), BF16),
        in_specs=[VMEM, ANY, ANY],
        out_specs=ANY,
        scratch_shapes=[part, part, part, part, part,
                        pltpu.VMEM((96, 128), F32),
                        pltpu.VMEM((RCH, 16, depth), F32), pltpu.VMEM((RCH, 16, depth), F32),
                        pltpu.VMEM((2, 16, depth), BF16),
                        pltpu.VMEM((QCH, depth, cols), BF16),
                        pltpu.VMEM((rows // 2, half), BF16),
                        pltpu.VMEM((32, cols), F32),
                        pltpu.VMEM((NMSG, 32, cols), F32), pltpu.VMEM((NMSG, 32, cols), F32),
                        pltpu.VMEM((2, 2, NMSG, 32, cols), F32),
                        pltpu.VMEM((rows, width), BF16),
                        dma((RCH,)), dma((RCH,)), dma((RCH,)), dma((RCH,)), dma((RCH,)), dma((RCH,)),
                        dma((RCH,)), dma((RCH,)), dma((QCH,)), dma,
                        dma((NMSG,)), dma((NMSG,)), dma((NMSG,)), dma((NMSG,)), dma((NMSG,)), dma((NMSG,)),
                        dma((NMSG,)), dma((NMSG,)), dma((NMSG,)), dma((NMSG,)), dma((2, RCH))],
        compiler_params=pltpu.CompilerParams(collective_id=0, has_side_effects=True, vmem_limit_bytes=VMEM_LIMIT),
        name="finish",
    )(msg, hidden, w_o)


def solution(mesh):
    def local_step(hidden, ln_gain, ln_bias, w_q, w_k, w_v, w_o, k_cache, v_cache, lengths):
        batch, _, kv, head = k_cache.shape
        q, k_new, v_new = qkv(hidden, ln_gain, ln_bias, lengths, w_q, w_k, w_v)
        msg = attend(lengths, q, k_new, v_new, k_cache, v_cache)
        out = finish(msg, hidden, w_o)
        return out, k_new.reshape(batch, kv, head), v_new.reshape(batch, kv, head)

    row_spec = P('dp', None)
    cache_spec = P('dp', 'sp', 'tp', None)
    head_spec = P('dp', 'tp', None)
    return jax.shard_map(local_step, mesh=mesh, in_specs=(row_spec, P(None), P(None), P(None, 'tp'), P(None, 'tp'), P(None, 'tp'), P('tp', None), cache_spec, cache_spec, P('dp')), out_specs=(row_spec, head_spec, head_spec), check_vma=False)
```

```python
import functools

import jax
import jax.numpy as jnp
import numpy as np
from jax import lax
from jax.experimental import pallas as pl
from jax.experimental.pallas import tpu as pltpu
from jax.sharding import PartitionSpec as P

F32 = jnp.float32
BF16 = jnp.bfloat16
MESH = pl.DeviceIdType.MESH
NEG = -0.7 * float(np.finfo(np.float32).max)
VMEM_LIMIT = 60 * 1024 * 1024
ANY = pl.BlockSpec(memory_space=pl.ANY)
VMEM = pl.BlockSpec(memory_space=pltpu.VMEM)


def qkv_kernel(len_ref, freq_ref, gain_ref, bias_ref, x_hbm, wq_hbm, wk_hbm, wv_hbm,
               q_out, k_out, v_out, xbuf, hbuf, wbuf, pbuf, qf, kf, cosb, sinb, gainb, biasb, xsem, wsem):
    rows, width = xbuf.shape
    n_q = wq_hbm.shape[1] // 256
    tiles = width // 128

    x_copy = pltpu.make_async_copy(x_hbm, xbuf, xsem)
    x_copy.start()

    def q_copy(i):
        return pltpu.make_async_copy(wq_hbm.at[:, pl.ds(i * 256, 256)], wbuf.at[i], wsem.at[i])

    k_copy = pltpu.make_async_copy(wk_hbm, wbuf.at[n_q], wsem.at[n_q])
    v_copy = pltpu.make_async_copy(wv_hbm, wbuf.at[n_q + 1], wsem.at[n_q + 1])
    for k in range(tiles):
        gainb[:, k * 128:(k + 1) * 128] = jnp.broadcast_to(1.0 + gain_ref[k:k + 1, :].astype(F32), (8, 128))
        biasb[:, k * 128:(k + 1) * 128] = jnp.broadcast_to(bias_ref[k:k + 1, :].astype(F32), (8, 128))
    for i in range(rows // 128):
        place = jnp.transpose(jnp.broadcast_to(len_ref[i:i + 1, :].astype(F32), (128, 128)))
        angle = place * freq_ref[...]
        cosb[i * 128:(i + 1) * 128, :] = jnp.cos(angle)
        sinb[i * 128:(i + 1) * 128, :] = jnp.sin(angle)

    x_copy.wait()
    q_copy(0).start()
    q_copy(1).start()

    def norm(i, carry):
        @pl.when(i < n_q - 2)
        def _():
            q_copy(i + 2).start()

        ats = [pl.ds(pl.multiple_of(i * 64 + j * 16, 16), 16) for j in range(4)]
        lanes = [slice(k * 128, (k + 1) * 128) for k in range(tiles)]
        means, scales = [], []
        for at in ats:
            accs = [xbuf[at, lanes[k]].astype(F32) for k in range(2)]
            for k in range(2, tiles):
                accs[k % 2] = accs[k % 2] + xbuf[at, lanes[k]].astype(F32)
            mean = jnp.sum(accs[0] + accs[1], axis=-1, keepdims=True) * (1.0 / width)
            means.append(jnp.broadcast_to(mean, (16, 128)))
        for at, mean in zip(ats, means):
            accs = [jnp.zeros((16, 128), F32) for _ in range(2)]
            for k in range(tiles):
                centred = xbuf[at, lanes[k]].astype(F32) - mean
                accs[k % 2] = accs[k % 2] + centred * centred
            var = jnp.sum(accs[0] + accs[1], axis=-1, keepdims=True) * (1.0 / width)
            scales.append(jnp.broadcast_to(lax.rsqrt(var + 1e-5), (16, 128)))
        for k in range(tiles):
            gain = jnp.concatenate([gainb[:, lanes[k]]] * 2, axis=0)
            bias = jnp.concatenate([biasb[:, lanes[k]]] * 2, axis=0)
            for at, mean, scale in zip(ats, means, scales):
                hbuf[at, lanes[k]] = ((xbuf[at, lanes[k]].astype(F32) - mean) * scale * gain + bias).astype(BF16)
        return carry

    lax.fori_loop(0, rows // 64, norm, 0)
    k_copy.start()
    v_copy.start()

    lane = lax.broadcasted_iota(jnp.int32, (rows, 128), 1)

    def rotate(u):
        other = jnp.where(lane < 32, -pltpu.roll(u, 96, 1), pltpu.roll(u, 32, 1))
        turned = u * cosb[...] + other * sinb[...]
        return jnp.where(lane < 64, turned, u)

    def project(i):
        return jnp.dot(hbuf[...], wbuf[i], preferred_element_type=F32)

    def place_heads(i, prod):
        for head in range(2):
            u = prod[:, head * 128:(head + 1) * 128]
            qf[pl.ds(lax.rem(2 * i + head, 16), rows, stride=16), :] = jnp.where(i == n_q + 1, u, rotate(u))

    pbuf[1] = jnp.zeros((rows, 256), F32)

    def tile(i, carry):
        pltpu.make_async_copy(wk_hbm, wbuf.at[i], wsem.at[i]).wait()
        pbuf[lax.rem(i, 2)] = project(i)
        place_heads(i + n_q + 1, pbuf[lax.rem(i + 1, 2)])
        return carry

    lax.fori_loop(0, n_q + 2, tile, 0)
    place_heads(n_q + 1, pbuf[(n_q + 1) % 2])
    for ref, row in ((k_out, 12), (v_out, 14)):
        for head in range(2):
            kf[pl.ds(head, rows, stride=2), :] = qf[pl.ds(row + head, rows, stride=16), :]
        ref[...] = kf[...].astype(BF16)
    q_out[...] = qf[...].astype(BF16)


def qkv(hidden, gain, bias, lengths, w_q, w_k, w_v):
    rows, width = hidden.shape
    n_tiles = w_q.shape[1] // 256 + 2
    freq = 10000.0 ** (-2.0 * np.arange(32, dtype=np.float32) / np.float32(64))
    freq = np.concatenate([freq, freq, np.zeros(64)]).astype(np.float32).reshape(1, 128)
    return pl.pallas_call(
        qkv_kernel,
        out_shape=(jax.ShapeDtypeStruct((rows * 16, 128), BF16),
                   jax.ShapeDtypeStruct((rows * 2, 128), BF16),
                   jax.ShapeDtypeStruct((rows * 2, 128), BF16)),
        in_specs=[VMEM, VMEM, VMEM, VMEM, ANY, ANY, ANY, ANY],
        out_specs=(VMEM, VMEM, VMEM),
        scratch_shapes=[pltpu.VMEM((rows, width), BF16), pltpu.VMEM((rows, width), BF16),
                        pltpu.VMEM((n_tiles, width, 256), BF16), pltpu.VMEM((2, rows, 256), F32),
                        pltpu.VMEM((rows * 16, 128), F32), pltpu.VMEM((rows * 2, 128), F32),
                        pltpu.VMEM((rows, 128), F32), pltpu.VMEM((rows, 128), F32),
                        pltpu.VMEM((8, width), F32), pltpu.VMEM((8, width), F32),
                        pltpu.SemaphoreType.DMA, pltpu.SemaphoreType.DMA((n_tiles,))],
        compiler_params=pltpu.CompilerParams(vmem_limit_bytes=VMEM_LIMIT),
        name="qkv",
    )(lengths.reshape(rows // 128, 128), jnp.asarray(freq), gain.reshape(width // 128, 128),
      bias.reshape(width // 128, 128), hidden, w_q, w_k, w_v)


RCH = 4
QCH = 6
NMSG = RCH * QCH
PER = QCH // 2
STEPS = 2 * RCH
HOP = 3
LAG = 6
SLOTS = 3


def scaled_sum(a, b):
    m_a, l_a, m_b, l_b = a[96:97, :], a[97:98, :], b[96:97, :], b[97:98, :]
    top = jnp.maximum(m_a, m_b)
    f_a, f_b = jnp.exp(m_a - top), jnp.exp(m_b - top)
    total = l_a * f_a + l_b * f_b
    r = lax.broadcasted_iota(jnp.int32, (128, 128), 0)
    turned = jnp.transpose(jnp.where(r == 0, f_a, jnp.where(r == 1, f_b, total)))
    acc = a[:96, :] * turned[:96, 0:1] + b[:96, :] * turned[:96, 1:2]
    return acc, top, total, turned[:96, 2:3]


def block_kernel(len_ref, q_ref, kn_ref, vn_ref, k_hbm, v_hbm, x_hbm, w_hbm, out_hbm,
                 kbuf, vbuf, sbuf, self_buf, pbuf, stat, msg, part, send_y, recv_y, comb_o, ctx_t, ctx_s, ctx_r,
                 lhs, wbuf, xbuf, prod, rs_in, rs_out, fin, obuf,
                 s_k, s_v, s_p, r_p, s_y, r_y, s_c, r_c, s_w, s_x,
                 s_rs, r_rs, s_ag, r_ag, s_fy, r_fy, s_fd, r_fd, s_fe, r_fe, s_out, *, positions, scale):
    d, z, s = lax.axis_index("dp"), lax.axis_index("tp"), lax.axis_index("sp")
    y, c = s // 2, s % 2
    yo, co = 1 - y, 1 - c
    u = c * z + co * (3 - z)
    partner, across = (d, z, 2 * y + co), (d, z, 2 * yo + c)
    ahead, behind = (d, z + 2 * c - 1, s), (d, z - 2 * c + 1, s)
    half = wbuf.shape[0] * wbuf.shape[2]
    width = wbuf.shape[2]

    def remote(src, dst, send, recv, dev):
        return pltpu.make_async_remote_copy(src_ref=src, dst_ref=dst, send_sem=send, recv_sem=recv,
                                            device_id=dev, device_id_type=MESH)

    barrier = pltpu.get_barrier_semaphore()
    pl.semaphore_signal(barrier, inc=1, device_id=partner, device_id_type=MESH)
    pl.semaphore_signal(barrier, inc=1, device_id=across, device_id_type=MESH)

    @pl.when(u < 3)
    def _():
        pl.semaphore_signal(barrier, inc=1, device_id=ahead, device_id_type=MESH)

    @pl.when(u > 0)
    def _():
        pl.semaphore_signal(barrier, inc=1, device_id=behind, device_id_type=MESH)

    def first_row(i):
        return 128 * ((i % 2) * y + (1 - i % 2) * yo) + 32 * (i // 2)

    def k_copy(i):
        return pltpu.make_async_copy(k_hbm.at[pl.ds(first_row(i), 32)], kbuf.at[i % SLOTS], s_k.at[i % SLOTS])

    def v_copy(i):
        return pltpu.make_async_copy(v_hbm.at[pl.ds(first_row(i), 32)], vbuf.at[i % SLOTS], s_v.at[i % SLOTS])

    def w_copy(q):
        return pltpu.make_async_copy(w_hbm.at[:, pl.ds(c * half + q * width, width)], wbuf.at[q], s_w.at[q])

    x_copy = pltpu.make_async_copy(x_hbm.at[pl.ds(y * 128, 128), pl.ds(c * half, half)], xbuf, s_x)

    for i in range(SLOTS):
        k_copy(i).start()
        v_copy(i).start()
    x_copy.start()
    pl.semaphore_wait(barrier, 2 + (z + 2) // 3 + (5 - z) // 3)

    first = s * positions
    col = lax.broadcasted_iota(jnp.int32, (16, 2 * positions), 1)
    row = lax.broadcasted_iota(jnp.int32, (16, 2 * positions), 0)
    place = jnp.where(lax.rem(col, 2) == jnp.where(row >= 6, 1, 0), first + col // 2, 1 << 30)
    pick_row = lax.broadcasted_iota(jnp.int32, (128, 16), 0)
    pick_col = lax.broadcasted_iota(jnp.int32, (128, 16), 1)
    pick = pick_col == 2 * (pick_row // 16) + jnp.where(lax.rem(pick_row, 16) >= 6, 1, 0)
    nt = (((1,), (1,)), ((), ()))

    def attention(i):
        k_copy(i).wait()
        v_copy(i).wait()
        slot = i % SLOTS
        base = first_row(i)
        spread = jnp.where(pick, 1.0, 0.0).astype(BF16)
        lane = lax.broadcasted_iota(jnp.int32, (128, 128), 1)
        begin = lax.broadcasted_iota(jnp.int32, (16, 16), 0) * 0 + first
        own_w = [None] * 4

        def scores(g):
            q8 = q_ref[pl.ds(pl.multiple_of(base * 16 + g * 128, 128), 128), :]
            kn = kn_ref[pl.ds(pl.multiple_of(base * 2 + g * 16, 16), 16), :]
            self8 = lax.dot_general(q8, kn, nt, preferred_element_type=F32) * scale
            self8 = jnp.where(pick, self8, NEG)
            for b in range(8):
                at = slice(g * 128 + b * 16, g * 128 + (b + 1) * 16)
                length = len_ref[base + g * 8 + b]
                owner = (length >= begin) & (length < begin + positions)
                sc = lax.dot_general(q8[b * 16:(b + 1) * 16, :], kbuf[slot, g * 8 + b], nt, preferred_element_type=F32) * scale
                sbuf[at, :] = jnp.where(place < length, sc, NEG)
                self_buf[at, :] = jnp.where(owner, self8[b * 16:(b + 1) * 16, :], NEG)

        def weights(g):
            at = slice(g * 128, (g + 1) * 128)
            sc = sbuf[at, :]
            own = jnp.max(self_buf[at, :], axis=1, keepdims=True)
            top = jnp.maximum(jnp.max(sc, axis=1, keepdims=True), own)
            w = jnp.exp(sc - top)
            own_w[g] = jnp.exp(own - top)
            total = jnp.sum(w, axis=1, keepdims=True) + own_w[g]
            pbuf[at, :] = w.astype(BF16)
            stat[at, :] = jnp.where(lane == 0, top, total)

        def sums(g):
            vn = vn_ref[pl.ds(pl.multiple_of(base * 2 + g * 16, 16), 16), :]
            own8 = own_w[g] * jnp.dot(spread, vn, preferred_element_type=F32)
            turned = jnp.transpose(stat[g * 128:(g + 1) * 128, :])[:8, :]
            msg[i, g, 96:104, :] = jnp.concatenate([turned[:, b * 16:b * 16 + 12] for b in range(8)] + [jnp.zeros((8, 32), F32)], axis=1)
            for b in range(8):
                at = slice(g * 128 + b * 16, g * 128 + (b + 1) * 16)
                acc = jnp.dot(pbuf[at, :], vbuf[slot, g * 8 + b], preferred_element_type=F32) + own8[b * 16:(b + 1) * 16, :]
                msg[i, g, b * 12:(b + 1) * 12, :] = acc[:12, :]

        for g in range(6):
            if g < 4:
                scores(g)
            if 1 <= g <= 4:
                weights(g - 1)
            if g >= 2:
                sums(g - 2)

    def to_partner(i):
        return remote(msg.at[i, pl.ds(2 * co, 2)], part.at[i], s_p.at[i], r_p.at[i], partner)

    def to_across(r):
        return remote(send_y.at[r], recv_y.at[r], s_y.at[r], r_y.at[r], across)

    def ctx_copy(r):
        return remote(ctx_s.at[r], ctx_r.at[r], s_c.at[r], r_c.at[r], partner)

    def merge(i, dst):
        to_partner(i).wait_recv()
        for k in range(2):
            acc, top, total, _ = scaled_sum(msg[i, 2 * c + k], part[i, k])
            dst[k, :96, :] = acc
            line = lax.broadcasted_iota(jnp.int32, (8, 128), 0)
            dst[k, 96:104, :] = jnp.where(line == 0, top, total)

    def context(r):
        to_across(r).wait_recv()
        for k in range(2):
            acc, _, _, total = scaled_sum(comb_o[r, k], recv_y[r, k])
            ctx_t[...] = acc / total
            for h in range(12):
                ctx_s[r, k * 8:(k + 1) * 8, h * 128:(h + 1) * 128] = ctx_t[pl.ds(h, 8, stride=12), :]
        ctx_copy(r).start()

    def rs(j):
        return remote(rs_out.at[j], rs_in.at[j], s_rs.at[j], r_rs.at[j], ahead)

    def final(dst, send, recv, h, core, j):
        f = fin.at[h, core, j]
        return remote(f, f, send.at[j], recv.at[j], dst)

    def ag(j):
        return final(behind, s_ag, r_ag, y, c, j)

    def fy(j):
        return final(across, s_fy, r_fy, y, c, j)

    def fy_in(j):
        return final(across, s_fy, r_fy, yo, c, j)

    def fd(j):
        return final(partner, s_fd, r_fd, y, c, j)

    def fd_in(j):
        return final(partner, s_fd, r_fd, y, co, j)

    def fe(j):
        return final(partner, s_fe, r_fe, yo, c, j)

    def fe_in(j):
        return final(partner, s_fe, r_fe, yo, co, j)

    def convert(h, core, j):
        at = pl.ds(pl.multiple_of(h * 128 + (j // QCH) * 32, 32), 32)
        obuf[at, pl.ds(pl.multiple_of(core * half + (j % QCH) * width, width), width)] = fin[h, core, j].astype(BF16)

    lag = LAG * (3 - u)
    lag_y = lag + LAG
    start = 2 * QCH + HOP * u

    def tick(t, carry):
        i, r6 = t // PER, t // QCH

        @pl.when((t < PER * STEPS) & (t % PER == 0))
        def _():
            attention(i)
            to_partner(i).start()

            @pl.when(i < STEPS - SLOTS)
            def _():
                k_copy(i + SLOTS).start()
                v_copy(i + SLOTS).start()

            @pl.when(i < QCH)
            def _():
                w_copy(i).start()

        @pl.when((t % QCH == PER + 1) & (t < NMSG))
        def _():
            merge(2 * r6, send_y.at[r6])
            to_across(r6).start()

        @pl.when((t % QCH == 1) & (t >= QCH) & (t < NMSG + QCH))
        def _():
            merge(2 * r6 - 1, comb_o.at[r6 - 1])

        @pl.when((t % QCH == QCH - 2) & (t >= QCH) & (t < NMSG + QCH))
        def _():
            context(r6 - 1)

        j = t - start

        @pl.when((j >= 0) & (j < NMSG))
        def _():
            r, q = j // QCH, j % QCH

            @pl.when(q == 0)
            def _():
                ctx_copy(r).wait_recv()
                lhs[c] = ctx_s[r].astype(BF16)
                lhs[co] = ctx_r[r].astype(BF16)

            @pl.when(r == 0)
            def _():
                w_copy(q).wait()

            @pl.when(j == 0)
            def _():
                x_copy.wait()

            prod[...] = jnp.dot(lhs[...].reshape(32, lhs.shape[2]), wbuf[q], preferred_element_type=F32)

            @pl.when(u == 0)
            def _():
                rs_out[j] = prod[...]
                rs(j).start()

            @pl.when((u > 0) & (u < 3))
            def _():
                rs(j).wait_recv()
                rs_out[j] = rs_in[j] + prod[...]
                rs(j).start()

            @pl.when(u == 3)
            def _():
                rs(j).wait_recv()
                x = xbuf[pl.ds(pl.multiple_of(r * 32, 32), 32), pl.ds(pl.multiple_of(q * width, width), width)]
                fin[y, c, j] = rs_in[j] + prod[...] + x.astype(F32)
                ag(j).start()
                fy(j).start()
                fd(j).start()
                convert(y, c, j)

        ja = j - lag

        @pl.when((u < 3) & (ja >= 0) & (ja < NMSG))
        def _():
            ag(ja).wait_recv()

            @pl.when(u > 0)
            def _():
                ag(ja).start()

            fy(ja).start()
            fd(ja).start()
            convert(y, c, ja)

        jy = j - lag_y

        @pl.when((jy >= 0) & (jy < NMSG))
        def _():
            fy_in(jy).wait_recv()
            fe(jy).start()
            convert(yo, c, jy)

        return carry

    lax.fori_loop(0, start + NMSG + lag_y, tick, 0)

    def out_copy(h, r):
        at = pl.ds(h * 128 + r * 32, 32)
        return pltpu.make_async_copy(obuf.at[at], out_hbm.at[at], s_out.at[h, r])

    def last(j, carry):
        fd_in(j).wait_recv()
        fe_in(j).wait_recv()
        convert(y, co, j)
        convert(yo, co, j)

        @pl.when(j % QCH == QCH - 1)
        def _():
            out_copy(0, j // QCH).start()
            out_copy(1, j // QCH).start()

        return carry

    lax.fori_loop(0, NMSG, last, 0)

    def drain(j, carry):
        @pl.when(u < 3)
        def _():
            rs(j).wait_send()

        @pl.when(u > 0)
        def _():
            ag(j).wait_send()

        fy(j).wait_send()
        fd(j).wait_send()
        fe(j).wait_send()
        return carry

    lax.fori_loop(0, NMSG, drain, 0)
    for i in range(STEPS):
        to_partner(i).wait_send()
    for r in range(RCH):
        to_across(r).wait_send()
        ctx_copy(r).wait_send()
        out_copy(0, r).wait()
        out_copy(1, r).wait()


def block(lengths, q, k_new, v_new, k_cache, v_cache, hidden, w_o):
    batch, positions, kv, head = k_cache.shape
    rows, width = hidden.shape
    depth = w_o.shape[0]
    half = width // 2
    cols = half // QCH
    dma = pltpu.SemaphoreType.DMA
    part = pltpu.VMEM((RCH, 2, 104, 128), F32)
    cache = pltpu.VMEM((SLOTS, 32, positions * kv, head), BF16)
    return pl.pallas_call(
        functools.partial(block_kernel, positions=positions, scale=head ** -0.5),
        out_shape=jax.ShapeDtypeStruct((rows, width), BF16),
        in_specs=[pl.BlockSpec(memory_space=pltpu.SMEM), VMEM, VMEM, VMEM, ANY, ANY, ANY, ANY],
        out_specs=ANY,
        scratch_shapes=[cache, cache,
                        pltpu.VMEM((512, positions * kv), F32), pltpu.VMEM((512, 16), F32),
                        pltpu.VMEM((512, positions * kv), BF16), pltpu.VMEM((512, 128), F32),
                        pltpu.VMEM((STEPS, 4, 104, 128), F32), pltpu.VMEM((STEPS, 2, 104, 128), F32),
                        part, part, part,
                        pltpu.VMEM((96, 128), F32),
                        pltpu.VMEM((RCH, 16, depth), F32), pltpu.VMEM((RCH, 16, depth), F32),
                        pltpu.VMEM((2, 16, depth), BF16),
                        pltpu.VMEM((QCH, depth, cols), BF16),
                        pltpu.VMEM((rows // 2, half), BF16),
                        pltpu.VMEM((32, cols), F32),
                        pltpu.VMEM((NMSG, 32, cols), F32), pltpu.VMEM((NMSG, 32, cols), F32),
                        pltpu.VMEM((2, 2, NMSG, 32, cols), F32),
                        pltpu.VMEM((rows, width), BF16),
                        dma((SLOTS,)), dma((SLOTS,)), dma((STEPS,)), dma((STEPS,)), dma((RCH,)), dma((RCH,)),
                        dma((RCH,)), dma((RCH,)), dma((QCH,)), dma] + [dma((NMSG,))] * 10 + [dma((2, RCH))],
        compiler_params=pltpu.CompilerParams(collective_id=0, has_side_effects=True, vmem_limit_bytes=VMEM_LIMIT),
        name="block",
    )(lengths, q, k_new, v_new, k_cache.reshape(batch, positions * kv, head), v_cache.reshape(batch, positions * kv, head), hidden, w_o)


def solution(mesh):
    def local_step(hidden, ln_gain, ln_bias, w_q, w_k, w_v, w_o, k_cache, v_cache, lengths):
        batch, _, kv, head = k_cache.shape
        q, k_new, v_new = qkv(hidden, ln_gain, ln_bias, lengths, w_q, w_k, w_v)
        out = block(lengths, q, k_new, v_new, k_cache, v_cache, hidden, w_o)
        return out, k_new.reshape(batch, kv, head), v_new.reshape(batch, kv, head)

    row_spec = P('dp', None)
    cache_spec = P('dp', 'sp', 'tp', None)
    head_spec = P('dp', 'tp', None)
    return jax.shard_map(local_step, mesh=mesh, in_specs=(row_spec, P(None), P(None), P(None, 'tp'), P(None, 'tp'), P(None, 'tp'), P('tp', None), cache_spec, cache_spec, P('dp')), out_specs=(row_spec, head_spec, head_spec), check_vma=False)
```

```python
import functools

import jax
import jax.numpy as jnp
import numpy as np
from jax import lax
from jax.experimental import pallas as pl
from jax.experimental.pallas import tpu as pltpu
from jax.sharding import PartitionSpec as P

F32 = jnp.float32
BF16 = jnp.bfloat16
MESH = pl.DeviceIdType.MESH
NEG = -0.7 * float(np.finfo(np.float32).max)
BLOCK_LIMIT = 49 * 1024 * 1024
ANY = pl.BlockSpec(memory_space=pl.ANY)
VMEM = pl.BlockSpec(memory_space=pltpu.VMEM)


RCH = 4
QCH = 6
NMSG = RCH * QCH
PER = QCH // 2
STEPS = 2 * RCH
HOP = 3
LAG = 6
SLOTS = 3


def scaled_sum(a, b):
    m_a, l_a, m_b, l_b = a[96:97, :], a[97:98, :], b[96:97, :], b[97:98, :]
    top = jnp.maximum(m_a, m_b)
    f_a, f_b = jnp.exp(m_a - top), jnp.exp(m_b - top)
    total = l_a * f_a + l_b * f_b
    r = lax.broadcasted_iota(jnp.int32, (128, 128), 0)
    turned = jnp.transpose(jnp.where(r == 0, f_a, jnp.where(r == 1, f_b, total)))
    acc = a[:96, :] * turned[:96, 0:1] + b[:96, :] * turned[:96, 1:2]
    return acc, top, total, turned[:96, 2:3]


def block_kernel(len_ref, len_rows, freq_ref, gain_ref, bias_ref, x_hbm, wq_hbm, wk_hbm, wv_hbm, k_hbm, v_hbm, w_hbm,
                 obuf, kn_ref, vn_ref,
                 hbuf, acc_ref, q_ref, kf, vf, xs, xr, cosb, sinb, gainb, biasb, s_h, s_q, s_g, s_xs, r_xs,
                 kbuf, vbuf, sbuf, self_buf, pbuf, stat, msg, part, send_y, recv_y, comb_o, ctx_t, ctx_s, ctx_r,
                 lhs, wbuf, xbuf, prod, rs_in, rs_out, fin,
                 s_k, s_v, s_p, r_p, s_y, r_y, s_c, r_c, s_w, s_x,
                 s_rs, r_rs, s_ag, r_ag, s_fy, r_fy, s_fd, r_fd, s_fe, r_fe, *, positions, scale):
    d, z, s = lax.axis_index("dp"), lax.axis_index("tp"), lax.axis_index("sp")
    y, c = s // 2, s % 2
    yo, co = 1 - y, 1 - c
    u = c * z + co * (3 - z)
    partner, across = (d, z, 2 * y + co), (d, z, 2 * yo + c)
    ahead, behind = (d, z + 2 * c - 1, s), (d, z - 2 * c + 1, s)
    width = wbuf.shape[2]
    half = QCH * width

    def remote(src, dst, send, recv, dev):
        return pltpu.make_async_remote_copy(src_ref=src, dst_ref=dst, send_sem=send, recv_sem=recv,
                                            device_id=dev, device_id_type=MESH)

    barrier = pltpu.get_barrier_semaphore()
    pl.semaphore_signal(barrier, inc=1, device_id=partner, device_id_type=MESH)
    pl.semaphore_signal(barrier, inc=1, device_id=across, device_id_type=MESH)

    @pl.when(u < 3)
    def _():
        pl.semaphore_signal(barrier, inc=1, device_id=ahead, device_id_type=MESH)

    @pl.when(u > 0)
    def _():
        pl.semaphore_signal(barrier, inc=1, device_id=behind, device_id_type=MESH)

    def first_row(i):
        return 128 * ((i % 2) * y + (1 - i % 2) * yo) + 32 * (i // 2)

    def k_copy(i):
        return pltpu.make_async_copy(k_hbm.at[pl.ds(first_row(i), 32)], kbuf.at[i % SLOTS], s_k.at[i % SLOTS])

    def v_copy(i):
        return pltpu.make_async_copy(v_hbm.at[pl.ds(first_row(i), 32)], vbuf.at[i % SLOTS], s_v.at[i % SLOTS])

    def w_copy(q):
        return pltpu.make_async_copy(w_hbm.at[:, pl.ds(c * half + q * width, width)], wbuf.at[q], s_w.at[q])

    x_copy = pltpu.make_async_copy(x_hbm.at[pl.ds(y * 128, 128), pl.ds(c * half, half)], xbuf, s_x)

    rows, model = hbuf.shape
    tiles = model // 128
    depth = wbuf.shape[1]
    h_copy = pltpu.make_async_copy(x_hbm, obuf, s_h)
    h_copy.start()

    def q_copy(n):
        return pltpu.make_async_copy(wq_hbm.at[pl.ds(n * depth, depth), pl.ds(c * 768, 512)], wbuf.at[n], s_q.at[n])

    def g_copies(n):
        at = pl.ds(n * depth, depth)
        return [pltpu.make_async_copy(wq_hbm.at[at, pl.ds(c * 768 + 512, 256)], wbuf.at[4 + n, :, pl.ds(0, 256)], s_g.at[0, n]),
                pltpu.make_async_copy(wk_hbm.at[at, pl.ds(c * 128, 128)], wbuf.at[4 + n, :, pl.ds(256, 128)], s_g.at[1, n]),
                pltpu.make_async_copy(wv_hbm.at[at, pl.ds(c * 128, 128)], wbuf.at[4 + n, :, pl.ds(384, 128)], s_g.at[2, n])]

    def share(g):
        at = pl.ds(4 * g, 4)
        return remote(xs.at[at], xr.at[at], s_xs.at[g], r_xs.at[g], partner)

    for k in range(tiles):
        gainb[:, k * 128:(k + 1) * 128] = jnp.broadcast_to(1.0 + gain_ref[k:k + 1, :].astype(F32), (8, 128))
        biasb[:, k * 128:(k + 1) * 128] = jnp.broadcast_to(bias_ref[k:k + 1, :].astype(F32), (8, 128))
    for i in range(rows // 128):
        angle = jnp.transpose(jnp.broadcast_to(len_rows[i:i + 1, :].astype(F32), (128, 128))) * freq_ref[...]
        cosb[i * 128:(i + 1) * 128, :] = jnp.cos(angle)
        sinb[i * 128:(i + 1) * 128, :] = jnp.sin(angle)
    h_copy.wait()
    for n in range(4):
        q_copy(n).start()

    def norm(i, carry):
        for copy in g_copies(i):
            copy.start()
        ats = [pl.ds(pl.multiple_of(i * 64 + j * 16, 16), 16) for j in range(4)]
        lanes = [slice(k * 128, (k + 1) * 128) for k in range(tiles)]
        means, scales = [], []
        for at in ats:
            accs = [obuf[at, lanes[k]].astype(F32) for k in range(2)]
            for k in range(2, tiles):
                accs[k % 2] = accs[k % 2] + obuf[at, lanes[k]].astype(F32)
            mean = jnp.sum(accs[0] + accs[1], axis=-1, keepdims=True) * (1.0 / model)
            means.append(jnp.broadcast_to(mean, (16, 128)))
        for at, mean in zip(ats, means):
            accs = [jnp.zeros((16, 128), F32) for _ in range(2)]
            for k in range(tiles):
                centred = obuf[at, lanes[k]].astype(F32) - mean
                accs[k % 2] = accs[k % 2] + centred * centred
            var = jnp.sum(accs[0] + accs[1], axis=-1, keepdims=True) * (1.0 / model)
            scales.append(jnp.broadcast_to(lax.rsqrt(var + 1e-5), (16, 128)))
        for k in range(tiles):
            gain = jnp.concatenate([gainb[:, lanes[k]]] * 2, axis=0)
            bias = jnp.concatenate([biasb[:, lanes[k]]] * 2, axis=0)
            for at, mean, factor in zip(ats, means, scales):
                hbuf[at, lanes[k]] = ((obuf[at, lanes[k]].astype(F32) - mean) * factor * gain + bias).astype(BF16)
        return carry

    lax.fori_loop(0, rows // 64, norm, 0)
    for i in range(SLOTS):
        k_copy(i).start()
        v_copy(i).start()
    x_copy.start()

    lane_r = lax.broadcasted_iota(jnp.int32, (rows, 128), 1)

    def rotate(v):
        other = jnp.where(lane_r < 32, -pltpu.roll(v, 96, 1), pltpu.roll(v, 32, 1))
        return jnp.where(lane_r < 64, v * cosb[...] + other * sinb[...], v)

    def spread_out(slot, core, v):
        if slot < 6:
            q_ref[pl.ds(6 * core + slot, rows, stride=16), :] = v
        else:
            dst = kf if slot == 6 else vf
            dst[pl.ds(core, rows, stride=2), :] = v

    for h in range(12, 16):
        q_ref[pl.ds(h, rows, stride=16), :] = jnp.zeros((rows, 128), F32)

    for g in range(2):
        acc_ref[...] = jnp.zeros_like(acc_ref)

        def accumulate(n, carry):
            if g == 0:
                q_copy(n).wait()
            else:
                for copy in g_copies(n):
                    copy.wait()
            left = hbuf[:, pl.ds(pl.multiple_of(n * depth, 128), depth)]
            acc_ref[...] += jnp.dot(left, wbuf[4 * g + n], preferred_element_type=F32)
            return carry

        lax.fori_loop(0, 4, accumulate, 0)
        if g == 0:
            pl.semaphore_wait(barrier, 2 + (z + 2) // 3 + (5 - z) // 3)
        for n in range(4):
            v = acc_ref[:, n * 128:(n + 1) * 128]
            if 4 * g + n < 7:
                v = rotate(v)
            xs[4 * g + n] = v
            spread_out(4 * g + n, c, v)
        share(g).start()
    for g in range(2):
        share(g).wait_recv()
        for n in range(4):
            spread_out(4 * g + n, co, xr[4 * g + n])
    kn_ref[...] = kf[...].astype(BF16)
    vn_ref[...] = vf[...].astype(BF16)

    first = s * positions
    col = lax.broadcasted_iota(jnp.int32, (16, 2 * positions), 1)
    row = lax.broadcasted_iota(jnp.int32, (16, 2 * positions), 0)
    place = jnp.where(lax.rem(col, 2) == jnp.where(row >= 6, 1, 0), first + col // 2, 1 << 30)
    pick_row = lax.broadcasted_iota(jnp.int32, (128, 16), 0)
    pick_col = lax.broadcasted_iota(jnp.int32, (128, 16), 1)
    pick = pick_col == 2 * (pick_row // 16) + jnp.where(lax.rem(pick_row, 16) >= 6, 1, 0)
    nt = (((1,), (1,)), ((), ()))

    def attention(i):
        k_copy(i).wait()
        v_copy(i).wait()
        slot = i % SLOTS
        base = first_row(i)
        spread = jnp.where(pick, 1.0, 0.0).astype(BF16)
        lane = lax.broadcasted_iota(jnp.int32, (128, 128), 1)
        begin = lax.broadcasted_iota(jnp.int32, (16, 16), 0) * 0 + first
        own_w = [None] * 4

        def scores(g):
            q8 = q_ref[pl.ds(pl.multiple_of(base * 16 + g * 128, 128), 128), :].astype(BF16)
            kn = kn_ref[pl.ds(pl.multiple_of(base * 2 + g * 16, 16), 16), :]
            self8 = lax.dot_general(q8, kn, nt, preferred_element_type=F32) * scale
            self8 = jnp.where(pick, self8, NEG)
            for b in range(8):
                at = slice(g * 128 + b * 16, g * 128 + (b + 1) * 16)
                length = len_ref[base + g * 8 + b]
                owner = (length >= begin) & (length < begin + positions)
                sc = lax.dot_general(q8[b * 16:(b + 1) * 16, :], kbuf[slot, g * 8 + b], nt, preferred_element_type=F32) * scale
                sbuf[at, :] = jnp.where(place < length, sc, NEG)
                self_buf[at, :] = jnp.where(owner, self8[b * 16:(b + 1) * 16, :], NEG)

        def weights(g):
            at = slice(g * 128, (g + 1) * 128)
            sc = sbuf[at, :]
            own = jnp.max(self_buf[at, :], axis=1, keepdims=True)
            top = jnp.maximum(jnp.max(sc, axis=1, keepdims=True), own)
            w = jnp.exp(sc - top)
            own_w[g] = jnp.exp(own - top)
            total = jnp.sum(w, axis=1, keepdims=True) + own_w[g]
            pbuf[at, :] = w.astype(BF16)
            stat[at, :] = jnp.where(lane == 0, top, total)

        def sums(g):
            vn = vn_ref[pl.ds(pl.multiple_of(base * 2 + g * 16, 16), 16), :]
            own8 = own_w[g] * jnp.dot(spread, vn, preferred_element_type=F32)
            turned = jnp.transpose(stat[g * 128:(g + 1) * 128, :])[:8, :]
            msg[i, g, 96:104, :] = jnp.concatenate([turned[:, b * 16:b * 16 + 12] for b in range(8)] + [jnp.zeros((8, 32), F32)], axis=1)
            for b in range(8):
                at = slice(g * 128 + b * 16, g * 128 + (b + 1) * 16)
                acc = jnp.dot(pbuf[at, :], vbuf[slot, g * 8 + b], preferred_element_type=F32) + own8[b * 16:(b + 1) * 16, :]
                msg[i, g, b * 12:(b + 1) * 12, :] = acc[:12, :]

        for g in range(6):
            if g < 4:
                scores(g)
            if 1 <= g <= 4:
                weights(g - 1)
            if g >= 2:
                sums(g - 2)

    def to_partner(i):
        return remote(msg.at[i, pl.ds(2 * co, 2)], part.at[i], s_p.at[i], r_p.at[i], partner)

    def to_across(r):
        return remote(send_y.at[r], recv_y.at[r], s_y.at[r], r_y.at[r], across)

    def ctx_copy(r):
        return remote(ctx_s.at[r], ctx_r.at[r], s_c.at[r], r_c.at[r], partner)

    def merge(i, dst):
        to_partner(i).wait_recv()
        for k in range(2):
            acc, top, total, _ = scaled_sum(msg[i, 2 * c + k], part[i, k])
            dst[k, :96, :] = acc
            line = lax.broadcasted_iota(jnp.int32, (8, 128), 0)
            dst[k, 96:104, :] = jnp.where(line == 0, top, total)

    def context(r):
        to_across(r).wait_recv()
        for k in range(2):
            acc, _, _, total = scaled_sum(comb_o[r, k], recv_y[r, k])
            ctx_t[...] = acc / total
            for h in range(12):
                ctx_s[r, k * 8:(k + 1) * 8, h * 128:(h + 1) * 128] = ctx_t[pl.ds(h, 8, stride=12), :]
        ctx_copy(r).start()

    def rs(j):
        return remote(rs_out.at[j], rs_in.at[j], s_rs.at[j], r_rs.at[j], ahead)

    def final(dst, send, recv, h, core, j):
        f = fin.at[h, core, j]
        return remote(f, f, send.at[j], recv.at[j], dst)

    def ag(j):
        return final(behind, s_ag, r_ag, y, c, j)

    def fy(j):
        return final(across, s_fy, r_fy, y, c, j)

    def fy_in(j):
        return final(across, s_fy, r_fy, yo, c, j)

    def fd(j):
        return final(partner, s_fd, r_fd, y, c, j)

    def fd_in(j):
        return final(partner, s_fd, r_fd, y, co, j)

    def fe(j):
        return final(partner, s_fe, r_fe, yo, c, j)

    def fe_in(j):
        return final(partner, s_fe, r_fe, yo, co, j)

    def convert(h, core, j):
        at = pl.ds(pl.multiple_of(h * 128 + (j // QCH) * 32, 32), 32)
        obuf[at, pl.ds(pl.multiple_of(core * half + (j % QCH) * width, width), width)] = fin[h, core, j].astype(BF16)

    lag = LAG * (3 - u)
    lag_y = lag + LAG
    start = 2 * QCH + HOP * u

    def tick(t, carry):
        i, r6 = t // PER, t // QCH

        @pl.when((t < PER * STEPS) & (t % PER == 0))
        def _():
            attention(i)
            to_partner(i).start()

            @pl.when(i < STEPS - SLOTS)
            def _():
                k_copy(i + SLOTS).start()
                v_copy(i + SLOTS).start()

            @pl.when(i < QCH)
            def _():
                w_copy(i).start()

        @pl.when((t % QCH == PER + 1) & (t < NMSG))
        def _():
            merge(2 * r6, send_y.at[r6])
            to_across(r6).start()

        @pl.when((t % QCH == 1) & (t >= QCH) & (t < NMSG + QCH))
        def _():
            merge(2 * r6 - 1, comb_o.at[r6 - 1])

        @pl.when((t % QCH == QCH - 2) & (t >= QCH) & (t < NMSG + QCH))
        def _():
            context(r6 - 1)

        j = t - start

        @pl.when((j >= 0) & (j < NMSG))
        def _():
            r, q = j // QCH, j % QCH

            @pl.when(q == 0)
            def _():
                ctx_copy(r).wait_recv()
                lhs[c] = ctx_s[r].astype(BF16)
                lhs[co] = ctx_r[r].astype(BF16)

            @pl.when(r == 0)
            def _():
                w_copy(q).wait()

            @pl.when(j == 0)
            def _():
                x_copy.wait()

            prod[...] = jnp.dot(lhs[...].reshape(32, lhs.shape[2]), wbuf[q], preferred_element_type=F32)

            @pl.when(u == 0)
            def _():
                rs_out[j] = prod[...]
                rs(j).start()

            @pl.when((u > 0) & (u < 3))
            def _():
                rs(j).wait_recv()
                rs_out[j] = rs_in[j] + prod[...]
                rs(j).start()

            @pl.when(u == 3)
            def _():
                rs(j).wait_recv()
                x = xbuf[pl.ds(pl.multiple_of(r * 32, 32), 32), pl.ds(pl.multiple_of(q * width, width), width)]
                fin[y, c, j] = rs_in[j] + prod[...] + x.astype(F32)
                ag(j).start()
                fy(j).start()
                fd(j).start()
                convert(y, c, j)

        ja = j - lag

        @pl.when((u < 3) & (ja >= 0) & (ja < NMSG))
        def _():
            ag(ja).wait_recv()

            @pl.when(u > 0)
            def _():
                ag(ja).start()

            fy(ja).start()
            fd(ja).start()
            convert(y, c, ja)

        jy = j - lag_y

        @pl.when((jy >= 0) & (jy < NMSG))
        def _():
            fy_in(jy).wait_recv()
            fe(jy).start()
            convert(yo, c, jy)

        return carry

    lax.fori_loop(0, start + NMSG + lag_y, tick, 0)

    def last(j, carry):
        fd_in(j).wait_recv()
        fe_in(j).wait_recv()
        convert(y, co, j)
        convert(yo, co, j)
        return carry

    lax.fori_loop(0, NMSG, last, 0)

    def drain(j, carry):
        @pl.when(u < 3)
        def _():
            rs(j).wait_send()

        @pl.when(u > 0)
        def _():
            ag(j).wait_send()

        fy(j).wait_send()
        fd(j).wait_send()
        fe(j).wait_send()
        return carry

    lax.fori_loop(0, NMSG, drain, 0)
    for g in range(2):
        share(g).wait_send()
    for i in range(STEPS):
        to_partner(i).wait_send()
    for r in range(RCH):
        to_across(r).wait_send()
        ctx_copy(r).wait_send()


def block(lengths, gain, bias, hidden, w_q, w_k, w_v, k_cache, v_cache, w_o):
    batch, positions, kv, head = k_cache.shape
    rows, width = hidden.shape
    depth = w_o.shape[0]
    half = width // 2
    cols = half // QCH
    freq = 10000.0 ** (-2.0 * np.arange(32, dtype=np.float32) / np.float32(64))
    freq = np.concatenate([freq, freq, np.zeros(64)]).astype(np.float32).reshape(1, 128)
    dma = pltpu.SemaphoreType.DMA
    part = pltpu.VMEM((RCH, 2, 104, 128), F32)
    cache = pltpu.VMEM((SLOTS, 32, positions * kv, head), BF16)
    table = pltpu.VMEM((rows, 128), F32)
    pair = pltpu.VMEM((rows * 2, 128), F32)
    shared = pltpu.VMEM((8, rows, 128), F32)
    line = pltpu.VMEM((8, width), F32)
    new = jax.ShapeDtypeStruct((rows * kv, head), BF16)
    return pl.pallas_call(
        functools.partial(block_kernel, positions=positions, scale=head ** -0.5),
        out_shape=(jax.ShapeDtypeStruct((rows, width), BF16), new, new),
        in_specs=[pl.BlockSpec(memory_space=pltpu.SMEM), VMEM, VMEM, VMEM, VMEM] + [ANY] * 7,
        out_specs=(VMEM, VMEM, VMEM),
        scratch_shapes=[pltpu.VMEM((rows, width), BF16), pltpu.VMEM((rows, 512), F32), pltpu.VMEM((rows * 16, 128), F32),
                        pair, pair, shared, shared, table, table, line, line,
                        dma, dma((4,)), dma((3, 4)), dma((2,)), dma((2,)),
                        cache, cache,
                        pltpu.VMEM((512, positions * kv), F32), pltpu.VMEM((512, 16), F32),
                        pltpu.VMEM((512, positions * kv), BF16), pltpu.VMEM((512, 128), F32),
                        pltpu.VMEM((STEPS, 4, 104, 128), F32), pltpu.VMEM((STEPS, 2, 104, 128), F32),
                        part, part, part,
                        pltpu.VMEM((96, 128), F32),
                        pltpu.VMEM((RCH, 16, depth), F32), pltpu.VMEM((RCH, 16, depth), F32),
                        pltpu.VMEM((2, 16, depth), BF16),
                        pltpu.VMEM((8, depth, cols), BF16),
                        pltpu.VMEM((rows // 2, half), BF16),
                        pltpu.VMEM((32, cols), F32),
                        pltpu.VMEM((NMSG, 32, cols), F32), pltpu.VMEM((NMSG, 32, cols), F32),
                        pltpu.VMEM((2, 2, NMSG, 32, cols), F32),
                        dma((SLOTS,)), dma((SLOTS,)), dma((STEPS,)), dma((STEPS,)), dma((RCH,)), dma((RCH,)),
                        dma((RCH,)), dma((RCH,)), dma((QCH,)), dma] + [dma((NMSG,))] * 10,
        compiler_params=pltpu.CompilerParams(collective_id=0, has_side_effects=True, vmem_limit_bytes=BLOCK_LIMIT),
        name="block",
    )(lengths, lengths.reshape(rows // 128, 128), jnp.asarray(freq), gain.reshape(width // 128, 128), bias.reshape(width // 128, 128),
      hidden, w_q, w_k, w_v, k_cache.reshape(batch, positions * kv, head), v_cache.reshape(batch, positions * kv, head), w_o)


def solution(mesh):
    def local_step(hidden, ln_gain, ln_bias, w_q, w_k, w_v, w_o, k_cache, v_cache, lengths):
        batch, _, kv, head = k_cache.shape
        out, k_new, v_new = block(lengths, ln_gain, ln_bias, hidden, w_q, w_k, w_v, k_cache, v_cache, w_o)
        return out, k_new.reshape(batch, kv, head), v_new.reshape(batch, kv, head)

    row_spec = P('dp', None)
    cache_spec = P('dp', 'sp', 'tp', None)
    head_spec = P('dp', 'tp', None)
    return jax.shard_map(local_step, mesh=mesh, in_specs=(row_spec, P(None), P(None), P(None, 'tp'), P(None, 'tp'), P(None, 'tp'), P('tp', None), cache_spec, cache_spec, P('dp')), out_specs=(row_spec, head_spec, head_spec), check_vma=False)
```

```python
import functools

import jax
import jax.numpy as jnp
import numpy as np
from jax import lax
from jax.experimental import pallas as pl
from jax.experimental.pallas import tpu as pltpu
from jax.sharding import PartitionSpec as P

F32 = jnp.float32
BF16 = jnp.bfloat16
MESH = pl.DeviceIdType.MESH
NEG = -0.7 * float(np.finfo(np.float32).max)
BLOCK_LIMIT = 49 * 1024 * 1024
HBM = pl.BlockSpec(memory_space=pltpu.HBM)
VMEM = pl.BlockSpec(memory_space=pltpu.VMEM)


RCH = 4
QCH = 6
NMSG = RCH * QCH
PER = QCH // 2
STEPS = 2 * RCH
HOP = 3
LAG = 5
LAG_Y = 6
SLOTS = 3


def scaled_sum(a, b):
    m_a, l_a, m_b, l_b = a[96:97, :], a[97:98, :], b[96:97, :], b[97:98, :]
    top = jnp.maximum(m_a, m_b)
    f_a, f_b = jnp.exp(m_a - top), jnp.exp(m_b - top)
    total = l_a * f_a + l_b * f_b
    r = lax.broadcasted_iota(jnp.int32, (128, 128), 0)
    turned = jnp.transpose(jnp.where(r == 0, f_a, jnp.where(r == 1, f_b, total)))
    acc = a[:96, :] * turned[:96, 0:1] + b[:96, :] * turned[:96, 1:2]
    return acc, top, total, turned[:96, 2:3]


def block_kernel(len_hbm, freq_hbm, gain_hbm, bias_hbm, x_hbm, wq_hbm, wk_hbm, wv_hbm, k_hbm, v_hbm, w_hbm,
                 obuf, kn_ref, vn_ref,
                 len_ref, len_rows, freq_ref, gain_ref, bias_ref, s_in,
                 hbuf, acc_ref, q_ref, kf, vf, xs, xr, cosb, sinb, gainb, biasb, s_h, s_q, s_g, s_xs, r_xs,
                 kbuf, vbuf, sbuf, self_buf, pbuf, stat, msg, part, send_y, recv_y, comb_o, ctx_t, ctx_s, ctx_r,
                 lhs, wbuf, xbuf, prod, rs_in, rs_out, fin,
                 s_k, s_v, s_p, r_p, s_y, r_y, s_c, r_c, s_w, s_x,
                 s_rs, r_rs, r_re, s_ag, r_ag, s_ae, s_fy, r_fy, s_fd, r_fd, s_fe, r_fe, *, positions, scale):
    d, z, s = lax.axis_index("dp"), lax.axis_index("tp"), lax.axis_index("sp")
    y, c = s // 2, s % 2
    yo, co = 1 - y, 1 - c
    u = c * z + co * (3 - z)
    partner, across = (d, z, 2 * y + co), (d, z, 2 * yo + c)
    ahead, behind = (d, z + 2 * c - 1, s), (d, z - 2 * c + 1, s)
    width = wbuf.shape[2]
    half = QCH * width

    def remote(src, dst, send, recv, dev):
        return pltpu.make_async_remote_copy(src_ref=src, dst_ref=dst, send_sem=send, recv_sem=recv,
                                            device_id=dev, device_id_type=MESH)

    barrier = pltpu.get_barrier_semaphore()
    pl.semaphore_signal(barrier, inc=1, device_id=partner, device_id_type=MESH)
    pl.semaphore_signal(barrier, inc=1, device_id=across, device_id_type=MESH)

    @pl.when(u < 3)
    def _():
        pl.semaphore_signal(barrier, inc=1, device_id=ahead, device_id_type=MESH)

    @pl.when(u > 0)
    def _():
        pl.semaphore_signal(barrier, inc=1, device_id=behind, device_id_type=MESH)

    def first_row(i):
        return 128 * ((i % 2) * y + (1 - i % 2) * yo) + 32 * (i // 2)

    def k_copy(i):
        return pltpu.make_async_copy(k_hbm.at[pl.ds(first_row(i), 32)], kbuf.at[i % SLOTS], s_k.at[i % SLOTS])

    def v_copy(i):
        return pltpu.make_async_copy(v_hbm.at[pl.ds(first_row(i), 32)], vbuf.at[i % SLOTS], s_v.at[i % SLOTS])

    def w_copy(q):
        return pltpu.make_async_copy(w_hbm.at[:, pl.ds(c * half + q * width, width)], wbuf.at[q], s_w.at[q])

    x_copy = pltpu.make_async_copy(x_hbm.at[pl.ds(y * 128, 128), pl.ds(c * half, half)], xbuf, s_x)

    rows, model = hbuf.shape
    tiles = model // 128
    depth = wbuf.shape[1]
    h_copy = pltpu.make_async_copy(x_hbm, obuf, s_h)
    inputs = ((len_hbm, len_ref), (len_hbm, len_rows), (freq_hbm, freq_ref), (gain_hbm, gain_ref), (bias_hbm, bias_ref))
    small = [pltpu.make_async_copy(src, dst, s_in.at[n]) for n, (src, dst) in enumerate(inputs)]
    for copy in small:
        copy.start()
    h_copy.start()

    def q_copy(n):
        return pltpu.make_async_copy(wq_hbm.at[pl.ds(n * depth, depth), pl.ds(c * 768, 512)], wbuf.at[n], s_q.at[n])

    def g_copies(n):
        at = pl.ds(n * depth, depth)
        return [pltpu.make_async_copy(wq_hbm.at[at, pl.ds(c * 768 + 512, 256)], wbuf.at[4 + n, :, pl.ds(0, 256)], s_g.at[0, n]),
                pltpu.make_async_copy(wk_hbm.at[at, pl.ds(c * 128, 128)], wbuf.at[4 + n, :, pl.ds(256, 128)], s_g.at[1, n]),
                pltpu.make_async_copy(wv_hbm.at[at, pl.ds(c * 128, 128)], wbuf.at[4 + n, :, pl.ds(384, 128)], s_g.at[2, n])]

    def share(g):
        at = pl.ds(4 * g, 4)
        return remote(xs.at[at], xr.at[at], s_xs.at[g], r_xs.at[g], partner)

    for copy in small:
        copy.wait()
    for k in range(tiles):
        gainb[:, k * 128:(k + 1) * 128] = jnp.broadcast_to(1.0 + gain_ref[k:k + 1, :].astype(F32), (8, 128))
        biasb[:, k * 128:(k + 1) * 128] = jnp.broadcast_to(bias_ref[k:k + 1, :].astype(F32), (8, 128))
    for i in range(rows // 128):
        angle = jnp.transpose(jnp.broadcast_to(len_rows[i:i + 1, :].astype(F32), (128, 128))) * freq_ref[...]
        cosb[i * 128:(i + 1) * 128, :] = jnp.cos(angle)
        sinb[i * 128:(i + 1) * 128, :] = jnp.sin(angle)
    h_copy.wait()
    for n in range(4):
        q_copy(n).start()

    def norm(i, carry):
        for copy in g_copies(i):
            copy.start()
        ats = [pl.ds(pl.multiple_of(i * 64 + j * 16, 16), 16) for j in range(4)]
        lanes = [slice(k * 128, (k + 1) * 128) for k in range(tiles)]
        means, scales = [], []
        for at in ats:
            accs = [obuf[at, lanes[k]].astype(F32) for k in range(2)]
            for k in range(2, tiles):
                accs[k % 2] = accs[k % 2] + obuf[at, lanes[k]].astype(F32)
            mean = jnp.sum(accs[0] + accs[1], axis=-1, keepdims=True) * (1.0 / model)
            means.append(jnp.broadcast_to(mean, (16, 128)))
        for at, mean in zip(ats, means):
            accs = [jnp.zeros((16, 128), F32) for _ in range(2)]
            for k in range(tiles):
                centred = obuf[at, lanes[k]].astype(F32) - mean
                accs[k % 2] = accs[k % 2] + centred * centred
            var = jnp.sum(accs[0] + accs[1], axis=-1, keepdims=True) * (1.0 / model)
            scales.append(jnp.broadcast_to(lax.rsqrt(var + 1e-5), (16, 128)))
        for k in range(tiles):
            gain = jnp.concatenate([gainb[:, lanes[k]]] * 2, axis=0)
            bias = jnp.concatenate([biasb[:, lanes[k]]] * 2, axis=0)
            for at, mean, factor in zip(ats, means, scales):
                hbuf[at, lanes[k]] = ((obuf[at, lanes[k]].astype(F32) - mean) * factor * gain + bias).astype(BF16)
        return carry

    lax.fori_loop(0, rows // 64, norm, 0)
    for i in range(SLOTS):
        k_copy(i).start()
        v_copy(i).start()
    x_copy.start()

    lane_r = lax.broadcasted_iota(jnp.int32, (rows, 128), 1)

    def rotate(v):
        other = jnp.where(lane_r < 32, -pltpu.roll(v, 96, 1), pltpu.roll(v, 32, 1))
        return jnp.where(lane_r < 64, v * cosb[...] + other * sinb[...], v)

    def spread_out(slot, core, v):
        if slot < 6:
            q_ref[pl.ds(6 * core + slot, rows, stride=16), :] = v
        else:
            dst = kf if slot == 6 else vf
            dst[pl.ds(core, rows, stride=2), :] = v

    for h in range(12, 16):
        q_ref[pl.ds(h, rows, stride=16), :] = jnp.zeros((rows, 128), F32)

    for g in range(2):
        acc_ref[...] = jnp.zeros_like(acc_ref)

        def accumulate(n, carry):
            if g == 0:
                q_copy(n).wait()
            else:
                for copy in g_copies(n):
                    copy.wait()
            left = hbuf[:, pl.ds(pl.multiple_of(n * depth, 128), depth)]
            acc_ref[...] += jnp.dot(left, wbuf[4 * g + n], preferred_element_type=F32)
            return carry

        lax.fori_loop(0, 4, accumulate, 0)
        if g == 0:
            pl.semaphore_wait(barrier, 2 + (z + 2) // 3 + (5 - z) // 3)
        for n in range(4):
            v = acc_ref[:, n * 128:(n + 1) * 128]
            if 4 * g + n < 7:
                v = rotate(v)
            xs[4 * g + n] = v
            spread_out(4 * g + n, c, v)
        share(g).start()
    for g in range(2):
        share(g).wait_recv()
        for n in range(4):
            spread_out(4 * g + n, co, xr[4 * g + n])
    kn_ref[...] = kf[...].astype(BF16)
    vn_ref[...] = vf[...].astype(BF16)

    first = s * positions
    col = lax.broadcasted_iota(jnp.int32, (16, 2 * positions), 1)
    row = lax.broadcasted_iota(jnp.int32, (16, 2 * positions), 0)
    place = jnp.where(lax.rem(col, 2) == jnp.where(row >= 6, 1, 0), first + col // 2, 1 << 30)
    pick_row = lax.broadcasted_iota(jnp.int32, (128, 16), 0)
    pick_col = lax.broadcasted_iota(jnp.int32, (128, 16), 1)
    pick = pick_col == 2 * (pick_row // 16) + jnp.where(lax.rem(pick_row, 16) >= 6, 1, 0)
    nt = (((1,), (1,)), ((), ()))

    def attention(i):
        k_copy(i).wait()
        v_copy(i).wait()
        slot = i % SLOTS
        base = first_row(i)
        spread = jnp.where(pick, 1.0, 0.0).astype(BF16)
        lane = lax.broadcasted_iota(jnp.int32, (128, 128), 1)
        begin = lax.broadcasted_iota(jnp.int32, (16, 16), 0) * 0 + first
        own_w = [None] * 4

        def scores(g):
            q8 = q_ref[pl.ds(pl.multiple_of(base * 16 + g * 128, 128), 128), :].astype(BF16)
            kn = kn_ref[pl.ds(pl.multiple_of(base * 2 + g * 16, 16), 16), :]
            self8 = lax.dot_general(q8, kn, nt, preferred_element_type=F32) * scale
            self8 = jnp.where(pick, self8, NEG)
            for b in range(8):
                at = slice(g * 128 + b * 16, g * 128 + (b + 1) * 16)
                length = len_ref[base // 128, base % 128 + g * 8 + b]
                owner = (length >= begin) & (length < begin + positions)
                sc = lax.dot_general(q8[b * 16:(b + 1) * 16, :], kbuf[slot, g * 8 + b], nt, preferred_element_type=F32) * scale
                sbuf[at, :] = jnp.where(place < length, sc, NEG)
                self_buf[at, :] = jnp.where(owner, self8[b * 16:(b + 1) * 16, :], NEG)

        def weights(g):
            at = slice(g * 128, (g + 1) * 128)
            sc = sbuf[at, :]
            own = jnp.max(self_buf[at, :], axis=1, keepdims=True)
            top = jnp.maximum(jnp.max(sc, axis=1, keepdims=True), own)
            w = jnp.exp(sc - top)
            own_w[g] = jnp.exp(own - top)
            total = jnp.sum(w, axis=1, keepdims=True) + own_w[g]
            pbuf[at, :] = w.astype(BF16)
            stat[at, :] = jnp.where(lane == 0, top, total)

        def sums(g):
            vn = vn_ref[pl.ds(pl.multiple_of(base * 2 + g * 16, 16), 16), :]
            own8 = own_w[g] * jnp.dot(spread, vn, preferred_element_type=F32)
            turned = jnp.transpose(stat[g * 128:(g + 1) * 128, :])[:8, :]
            msg[i, g, 96:104, :] = jnp.concatenate([turned[:, b * 16:b * 16 + 12] for b in range(8)] + [jnp.zeros((8, 32), F32)], axis=1)
            for b in range(8):
                at = slice(g * 128 + b * 16, g * 128 + (b + 1) * 16)
                acc = jnp.dot(pbuf[at, :], vbuf[slot, g * 8 + b], preferred_element_type=F32) + own8[b * 16:(b + 1) * 16, :]
                msg[i, g, b * 12:(b + 1) * 12, :] = acc[:12, :]

        for g in range(6):
            if g < 4:
                scores(g)
            if 1 <= g <= 4:
                weights(g - 1)
            if g >= 2:
                sums(g - 2)

    def to_partner(i):
        return remote(msg.at[i, pl.ds(2 * co, 2)], part.at[i], s_p.at[i], r_p.at[i], partner)

    def to_across(r):
        return remote(send_y.at[r], recv_y.at[r], s_y.at[r], r_y.at[r], across)

    def ctx_copy(r):
        return remote(ctx_s.at[r], ctx_r.at[r], s_c.at[r], r_c.at[r], partner)

    def merge(i, dst):
        to_partner(i).wait_recv()
        for k in range(2):
            acc, top, total, _ = scaled_sum(msg[i, 2 * c + k], part[i, k])
            dst[k, :96, :] = acc
            line = lax.broadcasted_iota(jnp.int32, (8, 128), 0)
            dst[k, 96:104, :] = jnp.where(line == 0, top, total)

    def context(r):
        to_across(r).wait_recv()
        for k in range(2):
            acc, _, _, total = scaled_sum(comb_o[r, k], recv_y[r, k])
            ctx_t[...] = acc / total
            for h in range(12):
                ctx_s[r, k * 8:(k + 1) * 8, h * 128:(h + 1) * 128] = ctx_t[pl.ds(h, 8, stride=12), :]
        ctx_copy(r).start()

    def rs(j):
        return remote(rs_out.at[j], rs_in.at[j], s_rs.at[j], r_rs.at[j], ahead)

    def rs_end(j):
        return remote(rs_out.at[j], fin.at[y, c, j], s_rs.at[j], r_re.at[j], behind)

    def final(dst, send, recv, h, core, j):
        f = fin.at[h, core, j]
        return remote(f, f, send.at[j], recv.at[j], dst)

    def ag(j):
        return final(behind, s_ag, r_ag, y, c, j)

    def ag_end(j):
        return final(ahead, s_ae, r_ag, y, c, j)

    def fy(j):
        return final(across, s_fy, r_fy, y, c, j)

    def fy_in(j):
        return final(across, s_fy, r_fy, yo, c, j)

    def fd(j):
        return final(partner, s_fd, r_fd, y, c, j)

    def fd_in(j):
        return final(partner, s_fd, r_fd, y, co, j)

    def fe(j):
        return final(partner, s_fe, r_fe, yo, c, j)

    def fe_in(j):
        return final(partner, s_fe, r_fe, yo, co, j)

    def convert(h, core, j):
        at = pl.ds(pl.multiple_of(h * 128 + (j // QCH) * 32, 32), 32)
        obuf[at, pl.ds(pl.multiple_of(core * half + (j % QCH) * width, width), width)] = fin[h, core, j].astype(BF16)

    hops = u - 2 * (u // 3)
    lag = LAG * (2 - hops)
    lag_y = lag + LAG_Y
    start = 2 * QCH + HOP * hops

    def tick(t, carry):
        i, r6 = t // PER, t // QCH

        @pl.when((t < PER * STEPS) & (t % PER == 0))
        def _():
            attention(i)
            to_partner(i).start()

            @pl.when(i < STEPS - SLOTS)
            def _():
                k_copy(i + SLOTS).start()
                v_copy(i + SLOTS).start()

            @pl.when(i < QCH)
            def _():
                w_copy(i).start()

        @pl.when((t % QCH == PER + 1) & (t < NMSG))
        def _():
            merge(2 * r6, send_y.at[r6])
            to_across(r6).start()

        @pl.when((t % QCH == 1) & (t >= QCH) & (t < NMSG + QCH))
        def _():
            merge(2 * r6 - 1, comb_o.at[r6 - 1])

        @pl.when((t % QCH == QCH - 2) & (t >= QCH) & (t < NMSG + QCH))
        def _():
            context(r6 - 1)

        j = t - start

        @pl.when((j >= 0) & (j < NMSG))
        def _():
            r, q = j // QCH, j % QCH

            @pl.when(q == 0)
            def _():
                ctx_copy(r).wait_recv()
                lhs[c] = ctx_s[r].astype(BF16)
                lhs[co] = ctx_r[r].astype(BF16)

            @pl.when(r == 0)
            def _():
                w_copy(q).wait()

            @pl.when(j == 0)
            def _():
                x_copy.wait()

            prod[...] = jnp.dot(lhs[...].reshape(32, lhs.shape[2]), wbuf[q], preferred_element_type=F32)

            @pl.when(u == 0)
            def _():
                rs_out[j] = prod[...]
                rs(j).start()

            @pl.when(u == 3)
            def _():
                rs_out[j] = prod[...]
                rs_end(j).start()

            @pl.when(u == 1)
            def _():
                rs(j).wait_recv()
                rs_out[j] = rs_in[j] + prod[...]
                rs(j).start()

            @pl.when(u == 2)
            def _():
                x = xbuf[pl.ds(pl.multiple_of(r * 32, 32), 32), pl.ds(pl.multiple_of(q * width, width), width)]
                rs_end(j).wait_recv()
                rs(j).wait_recv()
                fin[y, c, j] = (rs_in[j] + prod[...]) + fin[y, c, j] + x.astype(F32)
                ag(j).start()
                ag_end(j).start()
                fy(j).start()
                fd(j).start()
                convert(y, c, j)

        ja = j - lag

        @pl.when((lag > 0) & (ja >= 0) & (ja < NMSG))
        def _():
            ag(ja).wait_recv()

            @pl.when(u == 1)
            def _():
                ag(ja).start()

            fy(ja).start()
            fd(ja).start()
            convert(y, c, ja)

        jy = j - lag_y

        @pl.when((jy >= 0) & (jy < NMSG))
        def _():
            fy_in(jy).wait_recv()
            fe(jy).start()
            convert(yo, c, jy)

        return carry

    lax.fori_loop(0, start + NMSG + lag_y, tick, 0)

    def last(j, carry):
        fd_in(j).wait_recv()
        fe_in(j).wait_recv()
        convert(y, co, j)
        convert(yo, co, j)
        return carry

    lax.fori_loop(0, NMSG, last, 0)

    def drain(j, carry):
        @pl.when(u < 2)
        def _():
            rs(j).wait_send()

        @pl.when(u == 3)
        def _():
            rs_end(j).wait_send()

        @pl.when((u == 1) | (u == 2))
        def _():
            ag(j).wait_send()

        @pl.when(u == 2)
        def _():
            ag_end(j).wait_send()

        fy(j).wait_send()
        fd(j).wait_send()
        fe(j).wait_send()
        return carry

    lax.fori_loop(0, NMSG, drain, 0)
    for g in range(2):
        share(g).wait_send()
    for i in range(STEPS):
        to_partner(i).wait_send()
    for r in range(RCH):
        to_across(r).wait_send()
        ctx_copy(r).wait_send()


def block(lengths, gain, bias, hidden, w_q, w_k, w_v, k_cache, v_cache, w_o):
    batch, positions, kv, head = k_cache.shape
    rows, width = hidden.shape
    depth = w_o.shape[0]
    half = width // 2
    cols = half // QCH
    freq = 10000.0 ** (-2.0 * np.arange(32, dtype=np.float32) / np.float32(64))
    freq = np.concatenate([freq, freq, np.zeros(64)]).astype(np.float32).reshape(1, 128)
    dma = pltpu.SemaphoreType.DMA
    part = pltpu.VMEM((RCH, 2, 104, 128), F32)
    cache = pltpu.VMEM((SLOTS, 32, positions * kv, head), BF16)
    table = pltpu.VMEM((rows, 128), F32)
    pair = pltpu.VMEM((rows * 2, 128), F32)
    shared = pltpu.VMEM((8, rows, 128), F32)
    line = pltpu.VMEM((8, width), F32)
    new = jax.ShapeDtypeStruct((rows * kv, head), BF16)
    pin = functools.partial(pltpu.with_memory_space_constraint, memory_space=pltpu.HBM)
    return pl.pallas_call(
        functools.partial(block_kernel, positions=positions, scale=head ** -0.5),
        out_shape=(jax.ShapeDtypeStruct((rows, width), BF16), new, new),
        in_specs=[HBM] * 11,
        out_specs=(VMEM, VMEM, VMEM),
        scratch_shapes=[pltpu.SMEM((rows // 128, 128), jnp.int32), pltpu.VMEM((rows // 128, 128), jnp.int32), pltpu.VMEM((1, 128), F32),
                        pltpu.VMEM((width // 128, 128), BF16), pltpu.VMEM((width // 128, 128), BF16), dma((5,)),
                        pltpu.VMEM((rows, width), BF16), pltpu.VMEM((rows, 512), F32), pltpu.VMEM((rows * 16, 128), F32),
                        pair, pair, shared, shared, table, table, line, line,
                        dma, dma((4,)), dma((3, 4)), dma((2,)), dma((2,)),
                        cache, cache,
                        pltpu.VMEM((512, positions * kv), F32), pltpu.VMEM((512, 16), F32),
                        pltpu.VMEM((512, positions * kv), BF16), pltpu.VMEM((512, 128), F32),
                        pltpu.VMEM((STEPS, 4, 104, 128), F32), pltpu.VMEM((STEPS, 2, 104, 128), F32),
                        part, part, part,
                        pltpu.VMEM((96, 128), F32),
                        pltpu.VMEM((RCH, 16, depth), F32), pltpu.VMEM((RCH, 16, depth), F32),
                        pltpu.VMEM((2, 16, depth), BF16),
                        pltpu.VMEM((8, depth, cols), BF16),
                        pltpu.VMEM((rows // 2, half), BF16),
                        pltpu.VMEM((32, cols), F32),
                        pltpu.VMEM((NMSG, 32, cols), F32), pltpu.VMEM((NMSG, 32, cols), F32),
                        pltpu.VMEM((2, 2, NMSG, 32, cols), F32),
                        dma((SLOTS,)), dma((SLOTS,)), dma((STEPS,)), dma((STEPS,)), dma((RCH,)), dma((RCH,)),
                        dma((RCH,)), dma((RCH,)), dma((QCH,)), dma] + [dma((NMSG,))] * 12,
        compiler_params=pltpu.CompilerParams(collective_id=0, has_side_effects=True, vmem_limit_bytes=BLOCK_LIMIT),
        name="block",
    )(pin(lengths.reshape(rows // 128, 128)), pin(jnp.asarray(freq)), pin(gain.reshape(width // 128, 128)), pin(bias.reshape(width // 128, 128)),
      hidden, w_q, w_k, w_v, k_cache.reshape(batch, positions * kv, head), v_cache.reshape(batch, positions * kv, head), w_o)


def emit_kernel(*refs):
    n = len(refs) // 2
    copies = [pltpu.make_async_copy(refs[i], refs[n + i], refs[2 * n].at[i]) for i in range(n)]
    for copy in copies:
        copy.start()
    for copy in copies:
        copy.wait()


def emit(*values):
    n = len(values)
    return pl.pallas_call(
        emit_kernel,
        out_shape=tuple(jax.ShapeDtypeStruct(v.shape, v.dtype) for v in values),
        in_specs=[VMEM] * n, out_specs=(HBM,) * n,
        scratch_shapes=[pltpu.SemaphoreType.DMA((n,))],
        compiler_params=pltpu.CompilerParams(vmem_limit_bytes=4 * 1024 * 1024),
        name="emit",
    )(*values)


def solution(mesh):
    def local_step(hidden, ln_gain, ln_bias, w_q, w_k, w_v, w_o, k_cache, v_cache, lengths):
        batch, _, kv, head = k_cache.shape
        out, k_new, v_new = emit(*block(lengths, ln_gain, ln_bias, hidden, w_q, w_k, w_v, k_cache, v_cache, w_o))
        return out, k_new.reshape(batch, kv, head), v_new.reshape(batch, kv, head)

    row_spec = P('dp', None)
    cache_spec = P('dp', 'sp', 'tp', None)
    head_spec = P('dp', 'tp', None)
    return jax.shard_map(local_step, mesh=mesh, in_specs=(row_spec, P(None), P(None), P(None, 'tp'), P(None, 'tp'), P(None, 'tp'), P('tp', None), cache_spec, cache_spec, P('dp')), out_specs=(row_spec, head_spec, head_spec), check_vma=False)
```

```python
import functools

import jax
import jax.numpy as jnp
import numpy as np
from jax import lax
from jax.experimental import pallas as pl
from jax.experimental.pallas import tpu as pltpu
from jax.sharding import PartitionSpec as P

F32 = jnp.float32
BF16 = jnp.bfloat16
MESH = pl.DeviceIdType.MESH
NEG = -0.7 * float(np.finfo(np.float32).max)
BLOCK_LIMIT = 49 * 1024 * 1024
HBM = pl.BlockSpec(memory_space=pltpu.HBM)
VMEM = pl.BlockSpec(memory_space=pltpu.VMEM)


RCH = 4
QCH = 6
NMSG = RCH * QCH
PER = QCH // 2
STEPS = 2 * RCH
HOP = 3
LAG = 5
LAG_Y = 6
SLOTS = 3


def scaled_sum(a, b):
    m_a, l_a, m_b, l_b = a[96:97, :], a[97:98, :], b[96:97, :], b[97:98, :]
    top = jnp.maximum(m_a, m_b)
    f_a, f_b = jnp.exp(m_a - top), jnp.exp(m_b - top)
    total = l_a * f_a + l_b * f_b
    r = lax.broadcasted_iota(jnp.int32, (128, 128), 0)
    turned = jnp.transpose(jnp.where(r == 0, f_a, jnp.where(r == 1, f_b, total)))
    acc = a[:96, :] * turned[:96, 0:1] + b[:96, :] * turned[:96, 1:2]
    return acc, top, total, turned[:96, 2:3]


def block_kernel(len_hbm, freq_hbm, gain_hbm, bias_hbm, x_hbm, wq_hbm, wk_hbm, wv_hbm, k_hbm, v_hbm, w_hbm,
                 obuf, kn_ref, vn_ref,
                 len_ref, len_rows, freq_ref, gain_ref, bias_ref, s_in,
                 hbuf, acc_ref, q_ref, kf, vf, xs, xr, cosb, sinb, gainb, biasb, s_h, s_q, s_g, s_xs, r_xs,
                 kbuf, vbuf, sbuf, self_buf, pbuf, stat, msg, part, send_y, recv_y, comb_o, ctx_t, ctx_s, ctx_r,
                 lhs, wbuf, xbuf, prod, rs_in, rs_out, fin,
                 s_k, s_v, s_p, r_p, s_y, r_y, s_c, r_c, s_w, s_x,
                 s_rs, r_rs, r_re, s_ag, r_ag, s_ae, s_fy, r_fy, s_fd, r_fd, s_fe, r_fe, *, positions, scale):
    d, z, s = lax.axis_index("dp"), lax.axis_index("tp"), lax.axis_index("sp")
    y, c = s // 2, s % 2
    yo, co = 1 - y, 1 - c
    u = c * z + co * (3 - z)
    partner, across = (d, z, 2 * y + co), (d, z, 2 * yo + c)
    ahead, behind = (d, z + 2 * c - 1, s), (d, z - 2 * c + 1, s)
    width = wbuf.shape[2]
    half = QCH * width

    def remote(src, dst, send, recv, dev):
        return pltpu.make_async_remote_copy(src_ref=src, dst_ref=dst, send_sem=send, recv_sem=recv,
                                            device_id=dev, device_id_type=MESH)

    barrier = pltpu.get_barrier_semaphore()
    pl.semaphore_signal(barrier, inc=1, device_id=partner, device_id_type=MESH)
    pl.semaphore_signal(barrier, inc=1, device_id=across, device_id_type=MESH)

    @pl.when(u < 3)
    def _():
        pl.semaphore_signal(barrier, inc=1, device_id=ahead, device_id_type=MESH)

    @pl.when(u > 0)
    def _():
        pl.semaphore_signal(barrier, inc=1, device_id=behind, device_id_type=MESH)

    def first_row(i):
        return 128 * ((i % 2) * y + (1 - i % 2) * yo) + 32 * (i // 2)

    def k_copy(i):
        return pltpu.make_async_copy(k_hbm.at[pl.ds(first_row(i), 32)], kbuf.at[i % SLOTS], s_k.at[i % SLOTS])

    def v_copy(i):
        return pltpu.make_async_copy(v_hbm.at[pl.ds(first_row(i), 32)], vbuf.at[i % SLOTS], s_v.at[i % SLOTS])

    def w_copy(q):
        return pltpu.make_async_copy(w_hbm.at[:, pl.ds(c * half + q * width, width)], wbuf.at[q], s_w.at[q])

    x_copy = pltpu.make_async_copy(x_hbm.at[pl.ds(y * 128, 128), pl.ds(c * half, half)], xbuf, s_x)

    rows, model = hbuf.shape
    tiles = model // 128
    depth = wbuf.shape[1]

    def h_copy(i):
        at = pl.ds(i * 64, 64)
        return pltpu.make_async_copy(x_hbm.at[at], obuf.at[at], s_h.at[i])

    inputs = ((len_hbm, len_ref), (len_hbm, len_rows), (freq_hbm, freq_ref), (gain_hbm, gain_ref), (bias_hbm, bias_ref))
    small = [pltpu.make_async_copy(src, dst, s_in.at[n]) for n, (src, dst) in enumerate(inputs)]
    for copy in small:
        copy.start()
    for i in range(rows // 64):
        h_copy(i).start()

    def q_copy(n):
        return pltpu.make_async_copy(wq_hbm.at[pl.ds(n * depth, depth), pl.ds(c * 768, 512)], wbuf.at[n], s_q.at[n])

    def g_copies(n):
        at = pl.ds(n * depth, depth)
        return [pltpu.make_async_copy(wq_hbm.at[at, pl.ds(c * 768 + 512, 256)], wbuf.at[4 + n, :, pl.ds(0, 256)], s_g.at[0, n]),
                pltpu.make_async_copy(wk_hbm.at[at, pl.ds(c * 128, 128)], wbuf.at[4 + n, :, pl.ds(256, 128)], s_g.at[1, n]),
                pltpu.make_async_copy(wv_hbm.at[at, pl.ds(c * 128, 128)], wbuf.at[4 + n, :, pl.ds(384, 128)], s_g.at[2, n])]

    def share(slot):
        return remote(xs.at[slot], xr.at[slot], s_xs.at[slot], r_xs.at[slot], partner)

    for copy in small:
        copy.wait()
    for k in range(tiles):
        gainb[:, k * 128:(k + 1) * 128] = jnp.broadcast_to(1.0 + gain_ref[k:k + 1, :].astype(F32), (8, 128))
        biasb[:, k * 128:(k + 1) * 128] = jnp.broadcast_to(bias_ref[k:k + 1, :].astype(F32), (8, 128))
    for i in range(rows // 128):
        angle = jnp.transpose(jnp.broadcast_to(len_rows[i:i + 1, :].astype(F32), (128, 128))) * freq_ref[...]
        cosb[i * 128:(i + 1) * 128, :] = jnp.cos(angle)
        sinb[i * 128:(i + 1) * 128, :] = jnp.sin(angle)

    def norm(i, carry):
        h_copy(i).wait()

        @pl.when(i < 2)
        def _():
            q_copy(2 * i).start()
            q_copy(2 * i + 1).start()

        @pl.when(i >= 2)
        def _():
            for copy in g_copies(2 * i - 4) + g_copies(2 * i - 3):
                copy.start()

        ats = [pl.ds(pl.multiple_of(i * 64 + j * 16, 16), 16) for j in range(4)]
        lanes = [slice(k * 128, (k + 1) * 128) for k in range(tiles)]
        means, scales = [], []
        for at in ats:
            accs = [obuf[at, lanes[k]].astype(F32) for k in range(2)]
            for k in range(2, tiles):
                accs[k % 2] = accs[k % 2] + obuf[at, lanes[k]].astype(F32)
            mean = jnp.sum(accs[0] + accs[1], axis=-1, keepdims=True) * (1.0 / model)
            means.append(jnp.broadcast_to(mean, (16, 128)))
        for at, mean in zip(ats, means):
            accs = [jnp.zeros((16, 128), F32) for _ in range(2)]
            for k in range(tiles):
                centred = obuf[at, lanes[k]].astype(F32) - mean
                accs[k % 2] = accs[k % 2] + centred * centred
            var = jnp.sum(accs[0] + accs[1], axis=-1, keepdims=True) * (1.0 / model)
            scales.append(jnp.broadcast_to(lax.rsqrt(var + 1e-5), (16, 128)))
        for k in range(tiles):
            gain = jnp.concatenate([gainb[:, lanes[k]]] * 2, axis=0)
            bias = jnp.concatenate([biasb[:, lanes[k]]] * 2, axis=0)
            for at, mean, factor in zip(ats, means, scales):
                hbuf[at, lanes[k]] = ((obuf[at, lanes[k]].astype(F32) - mean) * factor * gain + bias).astype(BF16)
        return carry

    lax.fori_loop(0, rows // 64, norm, 0)
    for i in range(SLOTS):
        k_copy(i).start()
        v_copy(i).start()
    x_copy.start()

    lane_r = lax.broadcasted_iota(jnp.int32, (rows, 128), 1)

    def rotate(v):
        other = jnp.where(lane_r < 32, -pltpu.roll(v, 96, 1), pltpu.roll(v, 32, 1))
        return jnp.where(lane_r < 64, v * cosb[...] + other * sinb[...], v)

    def spread_out(slot, core, v):
        if slot < 6:
            q_ref[pl.ds(6 * core + slot, rows, stride=16), :] = v
        else:
            dst = kf if slot == 6 else vf
            dst[pl.ds(core, rows, stride=2), :] = v

    for h in range(12, 16):
        q_ref[pl.ds(h, rows, stride=16), :] = jnp.zeros((rows, 128), F32)

    for g in range(2):
        for n in range(4):
            for copy in ([q_copy(n)] if g == 0 else g_copies(n)):
                copy.wait()
        parts = [jnp.dot(hbuf[:, n * depth:(n + 1) * depth], wbuf[4 * g + n], preferred_element_type=F32) for n in range(4)]
        acc_ref[...] = (parts[0] + parts[1]) + (parts[2] + parts[3])
        if g == 0:
            pl.semaphore_wait(barrier, 2 + (z + 2) // 3 + (5 - z) // 3)
        for slot in range(4 * g, 4 * g + 4):
            v = acc_ref[:, (slot % 4) * 128:(slot % 4 + 1) * 128]
            xs[slot] = rotate(v) if slot < 7 else v
            share(slot).start()
        for slot in range(4 * g, 4 * g + 4):
            spread_out(slot, c, xs[slot])
    for slot in range(8):
        share(slot).wait_recv()
        spread_out(slot, co, xr[slot])
    kn_ref[...] = kf[...].astype(BF16)
    vn_ref[...] = vf[...].astype(BF16)

    first = s * positions
    col = lax.broadcasted_iota(jnp.int32, (16, 2 * positions), 1)
    row = lax.broadcasted_iota(jnp.int32, (16, 2 * positions), 0)
    place = jnp.where(lax.rem(col, 2) == jnp.where(row >= 6, 1, 0), first + col // 2, 1 << 30)
    pick_row = lax.broadcasted_iota(jnp.int32, (128, 16), 0)
    pick_col = lax.broadcasted_iota(jnp.int32, (128, 16), 1)
    pick = pick_col == 2 * (pick_row // 16) + jnp.where(lax.rem(pick_row, 16) >= 6, 1, 0)
    nt = (((1,), (1,)), ((), ()))

    def attention(i):
        k_copy(i).wait()
        v_copy(i).wait()
        slot = i % SLOTS
        base = first_row(i)
        spread = jnp.where(pick, 1.0, 0.0).astype(BF16)
        lane = lax.broadcasted_iota(jnp.int32, (128, 128), 1)
        begin = lax.broadcasted_iota(jnp.int32, (16, 16), 0) * 0 + first
        own_w = [None] * 4

        def scores(g):
            q8 = q_ref[pl.ds(pl.multiple_of(base * 16 + g * 128, 128), 128), :].astype(BF16)
            kn = kn_ref[pl.ds(pl.multiple_of(base * 2 + g * 16, 16), 16), :]
            self8 = lax.dot_general(q8, kn, nt, preferred_element_type=F32) * scale
            self8 = jnp.where(pick, self8, NEG)
            for b in range(8):
                at = slice(g * 128 + b * 16, g * 128 + (b + 1) * 16)
                length = len_ref[base // 128, base % 128 + g * 8 + b]
                owner = (length >= begin) & (length < begin + positions)
                sc = lax.dot_general(q8[b * 16:(b + 1) * 16, :], kbuf[slot, g * 8 + b], nt, preferred_element_type=F32) * scale
                sbuf[at, :] = jnp.where(place < length, sc, NEG)
                self_buf[at, :] = jnp.where(owner, self8[b * 16:(b + 1) * 16, :], NEG)

        def weights(g):
            at = slice(g * 128, (g + 1) * 128)
            sc = sbuf[at, :]
            own = jnp.max(self_buf[at, :], axis=1, keepdims=True)
            top = jnp.maximum(jnp.max(sc, axis=1, keepdims=True), own)
            w = jnp.exp(sc - top)
            own_w[g] = jnp.exp(own - top)
            total = jnp.sum(w, axis=1, keepdims=True) + own_w[g]
            pbuf[at, :] = w.astype(BF16)
            stat[at, :] = jnp.where(lane == 0, top, total)

        def sums(g):
            vn = vn_ref[pl.ds(pl.multiple_of(base * 2 + g * 16, 16), 16), :]
            own8 = own_w[g] * jnp.dot(spread, vn, preferred_element_type=F32)
            turned = jnp.transpose(stat[g * 128:(g + 1) * 128, :])[:8, :]
            msg[i, g, 96:104, :] = jnp.concatenate([turned[:, b * 16:b * 16 + 12] for b in range(8)] + [jnp.zeros((8, 32), F32)], axis=1)
            for b in range(8):
                at = slice(g * 128 + b * 16, g * 128 + (b + 1) * 16)
                acc = jnp.dot(pbuf[at, :], vbuf[slot, g * 8 + b], preferred_element_type=F32) + own8[b * 16:(b + 1) * 16, :]
                msg[i, g, b * 12:(b + 1) * 12, :] = acc[:12, :]

        for g in range(6):
            if g < 4:
                scores(g)
            if 1 <= g <= 4:
                weights(g - 1)
            if g >= 2:
                sums(g - 2)

    def to_partner(i):
        return remote(msg.at[i, pl.ds(2 * co, 2)], part.at[i], s_p.at[i], r_p.at[i], partner)

    def to_across(r):
        return remote(send_y.at[r], recv_y.at[r], s_y.at[r], r_y.at[r], across)

    def ctx_copy(r):
        return remote(ctx_s.at[r], ctx_r.at[r], s_c.at[r], r_c.at[r], partner)

    def merge(i, dst):
        to_partner(i).wait_recv()
        for k in range(2):
            acc, top, total, _ = scaled_sum(msg[i, 2 * c + k], part[i, k])
            dst[k, :96, :] = acc
            line = lax.broadcasted_iota(jnp.int32, (8, 128), 0)
            dst[k, 96:104, :] = jnp.where(line == 0, top, total)

    def context(r):
        to_across(r).wait_recv()
        for k in range(2):
            acc, _, _, total = scaled_sum(comb_o[r, k], recv_y[r, k])
            ctx_t[...] = acc / total
            for h in range(12):
                ctx_s[r, k * 8:(k + 1) * 8, h * 128:(h + 1) * 128] = ctx_t[pl.ds(h, 8, stride=12), :]
        ctx_copy(r).start()

    def rs(j):
        return remote(rs_out.at[j], rs_in.at[j], s_rs.at[j], r_rs.at[j], ahead)

    def rs_end(j):
        return remote(rs_out.at[j], fin.at[y, c, j], s_rs.at[j], r_re.at[j], behind)

    def final(dst, send, recv, h, core, j):
        f = fin.at[h, core, j]
        return remote(f, f, send.at[j], recv.at[j], dst)

    def ag(j):
        return final(behind, s_ag, r_ag, y, c, j)

    def ag_end(j):
        return final(ahead, s_ae, r_ag, y, c, j)

    def fy(j):
        return final(across, s_fy, r_fy, y, c, j)

    def fy_in(j):
        return final(across, s_fy, r_fy, yo, c, j)

    def fd(j):
        return final(partner, s_fd, r_fd, y, c, j)

    def fd_in(j):
        return final(partner, s_fd, r_fd, y, co, j)

    def fe(j):
        return final(partner, s_fe, r_fe, yo, c, j)

    def fe_in(j):
        return final(partner, s_fe, r_fe, yo, co, j)

    def convert(h, core, j):
        at = pl.ds(pl.multiple_of(h * 128 + (j // QCH) * 32, 32), 32)
        obuf[at, pl.ds(pl.multiple_of(core * half + (j % QCH) * width, width), width)] = fin[h, core, j].astype(BF16)

    hops = u - 2 * (u // 3)
    lag = LAG * (2 - hops)
    lag_y = lag + LAG_Y
    start = 2 * QCH + HOP * hops

    def tick(t, carry):
        i, r6 = t // PER, t // QCH

        @pl.when((t < PER * STEPS) & (t % PER == 0))
        def _():
            attention(i)
            to_partner(i).start()

            @pl.when(i < STEPS - SLOTS)
            def _():
                k_copy(i + SLOTS).start()
                v_copy(i + SLOTS).start()

            @pl.when(i < QCH)
            def _():
                w_copy(i).start()

        @pl.when((t % QCH == PER + 1) & (t < NMSG))
        def _():
            merge(2 * r6, send_y.at[r6])
            to_across(r6).start()

        @pl.when((t % QCH == 1) & (t >= QCH) & (t < NMSG + QCH))
        def _():
            merge(2 * r6 - 1, comb_o.at[r6 - 1])

        @pl.when((t % QCH == QCH - 2) & (t >= QCH) & (t < NMSG + QCH))
        def _():
            context(r6 - 1)

        j = t - start

        @pl.when((j >= 0) & (j < NMSG))
        def _():
            r, q = j // QCH, j % QCH

            @pl.when(q == 0)
            def _():
                ctx_copy(r).wait_recv()
                lhs[c] = ctx_s[r].astype(BF16)
                lhs[co] = ctx_r[r].astype(BF16)

            @pl.when(r == 0)
            def _():
                w_copy(q).wait()

            @pl.when(j == 0)
            def _():
                x_copy.wait()

            prod[...] = jnp.dot(lhs[...].reshape(32, lhs.shape[2]), wbuf[q], preferred_element_type=F32)

            @pl.when(u == 0)
            def _():
                rs_out[j] = prod[...]
                rs(j).start()

            @pl.when(u == 3)
            def _():
                rs_out[j] = prod[...]
                rs_end(j).start()

            @pl.when(u == 1)
            def _():
                rs(j).wait_recv()
                rs_out[j] = rs_in[j] + prod[...]
                rs(j).start()

            @pl.when(u == 2)
            def _():
                x = xbuf[pl.ds(pl.multiple_of(r * 32, 32), 32), pl.ds(pl.multiple_of(q * width, width), width)]
                rs_end(j).wait_recv()
                rs(j).wait_recv()
                fin[y, c, j] = (rs_in[j] + prod[...]) + fin[y, c, j] + x.astype(F32)
                ag(j).start()
                ag_end(j).start()
                fy(j).start()
                fd(j).start()
                convert(y, c, j)

        ja = j - lag

        @pl.when((lag > 0) & (ja >= 0) & (ja < NMSG))
        def _():
            ag(ja).wait_recv()

            @pl.when(u == 1)
            def _():
                ag(ja).start()

            fy(ja).start()
            fd(ja).start()
            convert(y, c, ja)

        jy = j - lag_y

        @pl.when((jy >= 0) & (jy < NMSG))
        def _():
            fy_in(jy).wait_recv()
            fe(jy).start()
            convert(yo, c, jy)

        return carry

    lax.fori_loop(0, start + NMSG + lag_y, tick, 0)

    def last(j, carry):
        fd_in(j).wait_recv()
        fe_in(j).wait_recv()
        convert(y, co, j)
        convert(yo, co, j)
        return carry

    lax.fori_loop(0, NMSG, last, 0)

    def drain(j, carry):
        @pl.when(u < 2)
        def _():
            rs(j).wait_send()

        @pl.when(u == 3)
        def _():
            rs_end(j).wait_send()

        @pl.when((u == 1) | (u == 2))
        def _():
            ag(j).wait_send()

        @pl.when(u == 2)
        def _():
            ag_end(j).wait_send()

        fy(j).wait_send()
        fd(j).wait_send()
        fe(j).wait_send()
        return carry

    lax.fori_loop(0, NMSG, drain, 0)
    for slot in range(8):
        share(slot).wait_send()
    for i in range(STEPS):
        to_partner(i).wait_send()
    for r in range(RCH):
        to_across(r).wait_send()
        ctx_copy(r).wait_send()


def block(lengths, gain, bias, hidden, w_q, w_k, w_v, k_cache, v_cache, w_o):
    batch, positions, kv, head = k_cache.shape
    rows, width = hidden.shape
    depth = w_o.shape[0]
    half = width // 2
    cols = half // QCH
    freq = 10000.0 ** (-2.0 * np.arange(32, dtype=np.float32) / np.float32(64))
    freq = np.concatenate([freq, freq, np.zeros(64)]).astype(np.float32).reshape(1, 128)
    dma = pltpu.SemaphoreType.DMA
    part = pltpu.VMEM((RCH, 2, 104, 128), F32)
    cache = pltpu.VMEM((SLOTS, 32, positions * kv, head), BF16)
    table = pltpu.VMEM((rows, 128), F32)
    pair = pltpu.VMEM((rows * 2, 128), F32)
    shared = pltpu.VMEM((8, rows, 128), F32)
    line = pltpu.VMEM((8, width), F32)
    new = jax.ShapeDtypeStruct((rows * kv, head), BF16)
    pin = functools.partial(pltpu.with_memory_space_constraint, memory_space=pltpu.HBM)
    return pl.pallas_call(
        functools.partial(block_kernel, positions=positions, scale=head ** -0.5),
        out_shape=(jax.ShapeDtypeStruct((rows, width), BF16), new, new),
        in_specs=[HBM] * 11,
        out_specs=(VMEM, VMEM, VMEM),
        scratch_shapes=[pltpu.SMEM((rows // 128, 128), jnp.int32), pltpu.VMEM((rows // 128, 128), jnp.int32), pltpu.VMEM((1, 128), F32),
                        pltpu.VMEM((width // 128, 128), BF16), pltpu.VMEM((width // 128, 128), BF16), dma((5,)),
                        pltpu.VMEM((rows, width), BF16), pltpu.VMEM((rows, 512), F32), pltpu.VMEM((rows * 16, 128), F32),
                        pair, pair, shared, shared, table, table, line, line,
                        dma((4,)), dma((4,)), dma((3, 4)), dma((8,)), dma((8,)),
                        cache, cache,
                        pltpu.VMEM((512, positions * kv), F32), pltpu.VMEM((512, 16), F32),
                        pltpu.VMEM((512, positions * kv), BF16), pltpu.VMEM((512, 128), F32),
                        pltpu.VMEM((STEPS, 4, 104, 128), F32), pltpu.VMEM((STEPS, 2, 104, 128), F32),
                        part, part, part,
                        pltpu.VMEM((96, 128), F32),
                        pltpu.VMEM((RCH, 16, depth), F32), pltpu.VMEM((RCH, 16, depth), F32),
                        pltpu.VMEM((2, 16, depth), BF16),
                        pltpu.VMEM((8, depth, cols), BF16),
                        pltpu.VMEM((rows // 2, half), BF16),
                        pltpu.VMEM((32, cols), F32),
                        pltpu.VMEM((NMSG, 32, cols), F32), pltpu.VMEM((NMSG, 32, cols), F32),
                        pltpu.VMEM((2, 2, NMSG, 32, cols), F32),
                        dma((SLOTS,)), dma((SLOTS,)), dma((STEPS,)), dma((STEPS,)), dma((RCH,)), dma((RCH,)),
                        dma((RCH,)), dma((RCH,)), dma((QCH,)), dma] + [dma((NMSG,))] * 12,
        compiler_params=pltpu.CompilerParams(collective_id=0, has_side_effects=True, vmem_limit_bytes=BLOCK_LIMIT),
        name="block",
    )(pin(lengths.reshape(rows // 128, 128)), pin(jnp.asarray(freq)), pin(gain.reshape(width // 128, 128)), pin(bias.reshape(width // 128, 128)),
      hidden, w_q, w_k, w_v, k_cache.reshape(batch, positions * kv, head), v_cache.reshape(batch, positions * kv, head), w_o)


def emit_kernel(*refs):
    n = len(refs) // 2
    copies = [pltpu.make_async_copy(refs[i], refs[n + i], refs[2 * n].at[i]) for i in range(n)]
    for copy in copies:
        copy.start()
    for copy in copies:
        copy.wait()


def emit(*values):
    n = len(values)
    return pl.pallas_call(
        emit_kernel,
        out_shape=tuple(jax.ShapeDtypeStruct(v.shape, v.dtype) for v in values),
        in_specs=[VMEM] * n, out_specs=(HBM,) * n,
        scratch_shapes=[pltpu.SemaphoreType.DMA((n,))],
        compiler_params=pltpu.CompilerParams(vmem_limit_bytes=4 * 1024 * 1024),
        name="emit",
    )(*values)


def solution(mesh):
    def local_step(hidden, ln_gain, ln_bias, w_q, w_k, w_v, w_o, k_cache, v_cache, lengths):
        batch, _, kv, head = k_cache.shape
        out, k_new, v_new = emit(*block(lengths, ln_gain, ln_bias, hidden, w_q, w_k, w_v, k_cache, v_cache, w_o))
        return out, k_new.reshape(batch, kv, head), v_new.reshape(batch, kv, head)

    row_spec = P('dp', None)
    cache_spec = P('dp', 'sp', 'tp', None)
    head_spec = P('dp', 'tp', None)
    return jax.shard_map(local_step, mesh=mesh, in_specs=(row_spec, P(None), P(None), P(None, 'tp'), P(None, 'tp'), P(None, 'tp'), P('tp', None), cache_spec, cache_spec, P('dp')), out_specs=(row_spec, head_spec, head_spec), check_vma=False)
```

```python
import functools

import jax
import jax.numpy as jnp
import numpy as np
from jax import lax
from jax.experimental import pallas as pl
from jax.experimental.pallas import tpu as pltpu
from jax.sharding import PartitionSpec as P

F32 = jnp.float32
BF16 = jnp.bfloat16
MESH = pl.DeviceIdType.MESH
NEG = -0.7 * float(np.finfo(np.float32).max)
BLOCK_LIMIT = 49 * 1024 * 1024
HBM = pl.BlockSpec(memory_space=pltpu.HBM)
VMEM = pl.BlockSpec(memory_space=pltpu.VMEM)


RCH = 4
QCH = 6
NMSG = RCH * QCH
PER = QCH // 2
STEPS = 2 * RCH
HOP = 4
LAG = 6
LAG_Y = 6
SLOTS = 3


def scaled_sum(a, b):
    m_a, l_a, m_b, l_b = a[96:97, :], a[97:98, :], b[96:97, :], b[97:98, :]
    top = jnp.maximum(m_a, m_b)
    f_a, f_b = jnp.exp(m_a - top), jnp.exp(m_b - top)
    total = l_a * f_a + l_b * f_b
    r = lax.broadcasted_iota(jnp.int32, (128, 128), 0)
    turned = jnp.transpose(jnp.where(r == 0, f_a, jnp.where(r == 1, f_b, total)))
    acc = a[:96, :] * turned[:96, 0:1] + b[:96, :] * turned[:96, 1:2]
    return acc, top, total, turned[:96, 2:3]


def block_kernel(len_hbm, freq_hbm, gain_hbm, bias_hbm, x_hbm, wq_hbm, wk_hbm, wv_hbm, k_hbm, v_hbm, w_hbm,
                 obuf, kn_ref, vn_ref,
                 len_ref, len_rows, freq_ref, gain_ref, bias_ref, s_in,
                 hbuf, acc_ref, q_ref, kf, vf, xs, xr, cosb, sinb, gainb, biasb, s_h, s_q, s_g, s_xs, r_xs,
                 kbuf, vbuf, sbuf, self_buf, pbuf, stat, msg, part, send_y, recv_y, comb_o, ctx_t, ctx_s, ctx_r,
                 lhs, wbuf, xbuf, prod, rs_in, rs_out, fin,
                 s_k, s_v, s_p, r_p, s_y, r_y, s_c, r_c, s_w, s_x,
                 s_rs, r_rs, r_re, s_ag, r_ag, s_ae, s_fy, r_fy, s_fd, r_fd, s_fe, r_fe, *, positions, scale):
    d, z, s = lax.axis_index("dp"), lax.axis_index("tp"), lax.axis_index("sp")
    y, c = s // 2, s % 2
    yo, co = 1 - y, 1 - c
    u = c * z + co * (3 - z)
    partner, across = (d, z, 2 * y + co), (d, z, 2 * yo + c)
    ahead, behind = (d, z + 2 * c - 1, s), (d, z - 2 * c + 1, s)
    width = wbuf.shape[2]
    half = QCH * width

    def remote(src, dst, send, recv, dev):
        return pltpu.make_async_remote_copy(src_ref=src, dst_ref=dst, send_sem=send, recv_sem=recv,
                                            device_id=dev, device_id_type=MESH)

    barrier = pltpu.get_barrier_semaphore()
    pl.semaphore_signal(barrier, inc=1, device_id=partner, device_id_type=MESH)
    pl.semaphore_signal(barrier, inc=1, device_id=across, device_id_type=MESH)

    @pl.when(u < 3)
    def _():
        pl.semaphore_signal(barrier, inc=1, device_id=ahead, device_id_type=MESH)

    @pl.when(u > 0)
    def _():
        pl.semaphore_signal(barrier, inc=1, device_id=behind, device_id_type=MESH)

    def first_row(i):
        return 128 * ((i % 2) * y + (1 - i % 2) * yo) + 32 * (i // 2)

    def k_copy(i):
        return pltpu.make_async_copy(k_hbm.at[pl.ds(first_row(i), 32)], kbuf.at[i % SLOTS], s_k.at[i % SLOTS])

    def v_copy(i):
        return pltpu.make_async_copy(v_hbm.at[pl.ds(first_row(i), 32)], vbuf.at[i % SLOTS], s_v.at[i % SLOTS])

    def w_copy(q):
        return pltpu.make_async_copy(w_hbm.at[:, pl.ds(c * half + q * width, width)], wbuf.at[q], s_w.at[q])

    x_copy = pltpu.make_async_copy(x_hbm.at[pl.ds(y * 128, 128), pl.ds(c * half, half)], xbuf, s_x)

    rows, model = hbuf.shape
    tiles = model // 128
    depth = wbuf.shape[1]

    def h_copy(i):
        at = pl.ds(i * 64, 64)
        return pltpu.make_async_copy(x_hbm.at[at], obuf.at[at], s_h.at[i])

    inputs = ((len_hbm, len_ref), (len_hbm, len_rows), (freq_hbm, freq_ref), (gain_hbm, gain_ref), (bias_hbm, bias_ref))
    small = [pltpu.make_async_copy(src, dst, s_in.at[n]) for n, (src, dst) in enumerate(inputs)]
    for copy in small:
        copy.start()
    for i in range(rows // 64):
        h_copy(i).start()

    def q_copy(n):
        return pltpu.make_async_copy(wq_hbm.at[pl.ds(n * depth, depth), pl.ds(c * 768, 512)], wbuf.at[n], s_q.at[n])

    def g_copies(n):
        at = pl.ds(n * depth, depth)
        return [pltpu.make_async_copy(wq_hbm.at[at, pl.ds(c * 768 + 512, 256)], wbuf.at[4 + n, :, pl.ds(0, 256)], s_g.at[0, n]),
                pltpu.make_async_copy(wk_hbm.at[at, pl.ds(c * 128, 128)], wbuf.at[4 + n, :, pl.ds(256, 128)], s_g.at[1, n]),
                pltpu.make_async_copy(wv_hbm.at[at, pl.ds(c * 128, 128)], wbuf.at[4 + n, :, pl.ds(384, 128)], s_g.at[2, n])]

    def share(slot):
        return remote(xs.at[slot], xr.at[slot], s_xs.at[slot], r_xs.at[slot], partner)

    for copy in small:
        copy.wait()
    for k in range(tiles):
        gainb[:, k * 128:(k + 1) * 128] = jnp.broadcast_to(1.0 + gain_ref[k:k + 1, :].astype(F32), (8, 128))
        biasb[:, k * 128:(k + 1) * 128] = jnp.broadcast_to(bias_ref[k:k + 1, :].astype(F32), (8, 128))
    for i in range(rows // 128):
        angle = jnp.transpose(jnp.broadcast_to(len_rows[i:i + 1, :].astype(F32), (128, 128))) * freq_ref[...]
        cosb[i * 128:(i + 1) * 128, :] = jnp.cos(angle)
        sinb[i * 128:(i + 1) * 128, :] = jnp.sin(angle)

    def norm(i, carry):
        h_copy(i).wait()

        @pl.when(i < 2)
        def _():
            q_copy(2 * i).start()
            q_copy(2 * i + 1).start()

        @pl.when(i >= 2)
        def _():
            for copy in g_copies(2 * i - 4) + g_copies(2 * i - 3):
                copy.start()

        ats = [pl.ds(pl.multiple_of(i * 64 + j * 16, 16), 16) for j in range(4)]
        lanes = [slice(k * 128, (k + 1) * 128) for k in range(tiles)]
        means, scales = [], []
        for at in ats:
            accs = [obuf[at, lanes[k]].astype(F32) for k in range(2)]
            for k in range(2, tiles):
                accs[k % 2] = accs[k % 2] + obuf[at, lanes[k]].astype(F32)
            mean = jnp.sum(accs[0] + accs[1], axis=-1, keepdims=True) * (1.0 / model)
            means.append(jnp.broadcast_to(mean, (16, 128)))
        for at, mean in zip(ats, means):
            accs = [jnp.zeros((16, 128), F32) for _ in range(2)]
            for k in range(tiles):
                centred = obuf[at, lanes[k]].astype(F32) - mean
                accs[k % 2] = accs[k % 2] + centred * centred
            var = jnp.sum(accs[0] + accs[1], axis=-1, keepdims=True) * (1.0 / model)
            scales.append(jnp.broadcast_to(lax.rsqrt(var + 1e-5), (16, 128)))
        for k in range(tiles):
            gain = jnp.concatenate([gainb[:, lanes[k]]] * 2, axis=0)
            bias = jnp.concatenate([biasb[:, lanes[k]]] * 2, axis=0)
            for at, mean, factor in zip(ats, means, scales):
                hbuf[at, lanes[k]] = ((obuf[at, lanes[k]].astype(F32) - mean) * factor * gain + bias).astype(BF16)
        return carry

    lax.fori_loop(0, rows // 64, norm, 0)
    for i in range(SLOTS):
        k_copy(i).start()
        v_copy(i).start()
    x_copy.start()

    lane_r = lax.broadcasted_iota(jnp.int32, (rows, 128), 1)

    def rotate(v):
        other = jnp.where(lane_r < 32, -pltpu.roll(v, 96, 1), pltpu.roll(v, 32, 1))
        return jnp.where(lane_r < 64, v * cosb[...] + other * sinb[...], v)

    def spread_out(slot, core, v):
        if slot < 6:
            q_ref[pl.ds(6 * core + slot, rows, stride=16), :] = v
        else:
            dst = kf if slot == 6 else vf
            dst[pl.ds(core, rows, stride=2), :] = v

    for h in range(12, 16):
        q_ref[pl.ds(h, rows, stride=16), :] = jnp.zeros((rows, 128), F32)

    for g in range(2):
        for n in range(4):
            for copy in ([q_copy(n)] if g == 0 else g_copies(n)):
                copy.wait()
        parts = [jnp.dot(hbuf[:, n * depth:(n + 1) * depth], wbuf[4 * g + n], preferred_element_type=F32) for n in range(4)]
        acc_ref[...] = (parts[0] + parts[1]) + (parts[2] + parts[3])
        if g == 0:
            pl.semaphore_wait(barrier, 2 + (z + 2) // 3 + (5 - z) // 3)
        for slot in range(4 * g, 4 * g + 4):
            v = acc_ref[:, (slot % 4) * 128:(slot % 4 + 1) * 128]
            xs[slot] = rotate(v) if slot < 7 else v
            share(slot).start()
        for slot in range(4 * g, 4 * g + 4):
            spread_out(slot, c, xs[slot])
    for slot in range(8):
        share(slot).wait_recv()
        spread_out(slot, co, xr[slot])
    kn_ref[...] = kf[...].astype(BF16)
    vn_ref[...] = vf[...].astype(BF16)

    first = s * positions
    col = lax.broadcasted_iota(jnp.int32, (16, 2 * positions), 1)
    row = lax.broadcasted_iota(jnp.int32, (16, 2 * positions), 0)
    place = jnp.where(lax.rem(col, 2) == jnp.where(row >= 6, 1, 0), first + col // 2, 1 << 30)
    pick_row = lax.broadcasted_iota(jnp.int32, (128, 16), 0)
    pick_col = lax.broadcasted_iota(jnp.int32, (128, 16), 1)
    pick = pick_col == 2 * (pick_row // 16) + jnp.where(lax.rem(pick_row, 16) >= 6, 1, 0)
    nt = (((1,), (1,)), ((), ()))

    def attention(i):
        k_copy(i).wait()
        v_copy(i).wait()
        slot = i % SLOTS
        base = first_row(i)
        spread = jnp.where(pick, 1.0, 0.0).astype(BF16)
        lane = lax.broadcasted_iota(jnp.int32, (128, 128), 1)
        begin = lax.broadcasted_iota(jnp.int32, (16, 16), 0) * 0 + first
        own_w = [None] * 4

        def scores(g):
            q8 = q_ref[pl.ds(pl.multiple_of(base * 16 + g * 128, 128), 128), :].astype(BF16)
            kn = kn_ref[pl.ds(pl.multiple_of(base * 2 + g * 16, 16), 16), :]
            self8 = lax.dot_general(q8, kn, nt, preferred_element_type=F32) * scale
            self8 = jnp.where(pick, self8, NEG)
            for b in range(8):
                at = slice(g * 128 + b * 16, g * 128 + (b + 1) * 16)
                length = len_ref[base // 128, base % 128 + g * 8 + b]
                owner = (length >= begin) & (length < begin + positions)
                sc = lax.dot_general(q8[b * 16:(b + 1) * 16, :], kbuf[slot, g * 8 + b], nt, preferred_element_type=F32) * scale
                sbuf[at, :] = jnp.where(place < length, sc, NEG)
                self_buf[at, :] = jnp.where(owner, self8[b * 16:(b + 1) * 16, :], NEG)

        def weights(g):
            at = slice(g * 128, (g + 1) * 128)
            sc = sbuf[at, :]
            own = jnp.max(self_buf[at, :], axis=1, keepdims=True)
            top = jnp.maximum(jnp.max(sc, axis=1, keepdims=True), own)
            w = jnp.exp(sc - top)
            own_w[g] = jnp.exp(own - top)
            total = jnp.sum(w, axis=1, keepdims=True) + own_w[g]
            pbuf[at, :] = w.astype(BF16)
            stat[at, :] = jnp.where(lane == 0, top, total)

        def sums(g):
            vn = vn_ref[pl.ds(pl.multiple_of(base * 2 + g * 16, 16), 16), :]
            own8 = own_w[g] * jnp.dot(spread, vn, preferred_element_type=F32)
            turned = jnp.transpose(stat[g * 128:(g + 1) * 128, :])[:8, :]
            msg[i, g, 96:104, :] = jnp.concatenate([turned[:, b * 16:b * 16 + 12] for b in range(8)] + [jnp.zeros((8, 32), F32)], axis=1)
            for b in range(8):
                at = slice(g * 128 + b * 16, g * 128 + (b + 1) * 16)
                acc = jnp.dot(pbuf[at, :], vbuf[slot, g * 8 + b], preferred_element_type=F32) + own8[b * 16:(b + 1) * 16, :]
                msg[i, g, b * 12:(b + 1) * 12, :] = acc[:12, :]

        for g in range(6):
            if g < 4:
                scores(g)
            if 1 <= g <= 4:
                weights(g - 1)
            if g >= 2:
                sums(g - 2)

    def to_partner(i):
        return remote(msg.at[i, pl.ds(2 * co, 2)], part.at[i], s_p.at[i], r_p.at[i], partner)

    def to_across(r):
        return remote(send_y.at[r], recv_y.at[r], s_y.at[r], r_y.at[r], across)

    def ctx_copy(r):
        return remote(ctx_s.at[r], ctx_r.at[r], s_c.at[r], r_c.at[r], partner)

    def merge(i, dst):
        to_partner(i).wait_recv()
        for k in range(2):
            acc, top, total, _ = scaled_sum(msg[i, 2 * c + k], part[i, k])
            dst[k, :96, :] = acc
            line = lax.broadcasted_iota(jnp.int32, (8, 128), 0)
            dst[k, 96:104, :] = jnp.where(line == 0, top, total)

    def context(r):
        to_across(r).wait_recv()
        for k in range(2):
            acc, _, _, total = scaled_sum(comb_o[r, k], recv_y[r, k])
            ctx_t[...] = acc / total
            for h in range(12):
                ctx_s[r, k * 8:(k + 1) * 8, h * 128:(h + 1) * 128] = ctx_t[pl.ds(h, 8, stride=12), :]
        ctx_copy(r).start()

    def rs(j):
        return remote(rs_out.at[j], rs_in.at[j], s_rs.at[j], r_rs.at[j], ahead)

    def rs_end(j):
        return remote(rs_out.at[j], fin.at[y, c, j], s_rs.at[j], r_re.at[j], behind)

    def final(dst, send, recv, h, core, j):
        f = fin.at[h, core, j]
        return remote(f, f, send.at[j], recv.at[j], dst)

    def ag(j):
        return final(behind, s_ag, r_ag, y, c, j)

    def ag_end(j):
        return final(ahead, s_ae, r_ag, y, c, j)

    def fy(j):
        return final(across, s_fy, r_fy, y, c, j)

    def fy_in(j):
        return final(across, s_fy, r_fy, yo, c, j)

    def fd(j):
        return final(partner, s_fd, r_fd, y, c, j)

    def fd_in(j):
        return final(partner, s_fd, r_fd, y, co, j)

    def fe(j):
        return final(partner, s_fe, r_fe, yo, c, j)

    def fe_in(j):
        return final(partner, s_fe, r_fe, yo, co, j)

    def convert(h, core, j):
        at = pl.ds(pl.multiple_of(h * 128 + (j // QCH) * 32, 32), 32)
        obuf[at, pl.ds(pl.multiple_of(core * half + (j % QCH) * width, width), width)] = fin[h, core, j].astype(BF16)

    hops = u - 2 * (u // 3)
    lag = LAG * (2 - hops)
    lag_y = lag + LAG_Y
    start = 2 * QCH + HOP * hops

    def tick(t, carry):
        i, r6 = t // PER, t // QCH

        @pl.when((t < PER * STEPS) & (t % PER == 0))
        def _():
            attention(i)
            to_partner(i).start()

            @pl.when(i < STEPS - SLOTS)
            def _():
                k_copy(i + SLOTS).start()
                v_copy(i + SLOTS).start()

            @pl.when(i < QCH)
            def _():
                w_copy(i).start()

        @pl.when((t % QCH == PER + 1) & (t < NMSG))
        def _():
            merge(2 * r6, send_y.at[r6])
            to_across(r6).start()

        @pl.when((t % QCH == 1) & (t >= QCH) & (t < NMSG + QCH))
        def _():
            merge(2 * r6 - 1, comb_o.at[r6 - 1])

        @pl.when((t % QCH == QCH - 2) & (t >= QCH) & (t < NMSG + QCH))
        def _():
            context(r6 - 1)

        j = t - start

        @pl.when((j >= 0) & (j < NMSG))
        def _():
            r, q = j // QCH, j % QCH

            @pl.when(q == 0)
            def _():
                ctx_copy(r).wait_recv()
                lhs[c] = ctx_s[r].astype(BF16)
                lhs[co] = ctx_r[r].astype(BF16)

            @pl.when(r == 0)
            def _():
                w_copy(q).wait()

            @pl.when(j == 0)
            def _():
                x_copy.wait()

            prod[...] = jnp.dot(lhs[...].reshape(32, lhs.shape[2]), wbuf[q], preferred_element_type=F32)

            @pl.when(u == 0)
            def _():
                rs_out[j] = prod[...]
                rs(j).start()

            @pl.when(u == 3)
            def _():
                rs_out[j] = prod[...]
                rs_end(j).start()

            @pl.when(u == 1)
            def _():
                rs(j).wait_recv()
                rs_out[j] = rs_in[j] + prod[...]
                rs(j).start()

            @pl.when(u == 2)
            def _():
                x = xbuf[pl.ds(pl.multiple_of(r * 32, 32), 32), pl.ds(pl.multiple_of(q * width, width), width)]
                rs_end(j).wait_recv()
                rs(j).wait_recv()
                fin[y, c, j] = (rs_in[j] + prod[...]) + fin[y, c, j] + x.astype(F32)
                ag(j).start()
                ag_end(j).start()
                fy(j).start()
                fd(j).start()
                convert(y, c, j)

        ja = j - lag

        @pl.when((lag > 0) & (ja >= 0) & (ja < NMSG))
        def _():
            ag(ja).wait_recv()

            @pl.when(u == 1)
            def _():
                ag(ja).start()

            fy(ja).start()
            fd(ja).start()
            convert(y, c, ja)

        jy = j - lag_y

        @pl.when((jy >= 0) & (jy < NMSG))
        def _():
            fy_in(jy).wait_recv()
            fe(jy).start()
            convert(yo, c, jy)

        return carry

    lax.fori_loop(0, start + NMSG + lag_y, tick, 0)

    def last(j, carry):
        fd_in(j).wait_recv()
        fe_in(j).wait_recv()
        convert(y, co, j)
        convert(yo, co, j)
        return carry

    lax.fori_loop(0, NMSG, last, 0)

    def drain(j, carry):
        @pl.when(u < 2)
        def _():
            rs(j).wait_send()

        @pl.when(u == 3)
        def _():
            rs_end(j).wait_send()

        @pl.when((u == 1) | (u == 2))
        def _():
            ag(j).wait_send()

        @pl.when(u == 2)
        def _():
            ag_end(j).wait_send()

        fy(j).wait_send()
        fd(j).wait_send()
        fe(j).wait_send()
        return carry

    lax.fori_loop(0, NMSG, drain, 0)
    for slot in range(8):
        share(slot).wait_send()
    for i in range(STEPS):
        to_partner(i).wait_send()
    for r in range(RCH):
        to_across(r).wait_send()
        ctx_copy(r).wait_send()


def block(lengths, gain, bias, hidden, w_q, w_k, w_v, k_cache, v_cache, w_o):
    batch, positions, kv, head = k_cache.shape
    rows, width = hidden.shape
    depth = w_o.shape[0]
    half = width // 2
    cols = half // QCH
    freq = 10000.0 ** (-2.0 * np.arange(32, dtype=np.float32) / np.float32(64))
    freq = np.concatenate([freq, freq, np.zeros(64)]).astype(np.float32).reshape(1, 128)
    dma = pltpu.SemaphoreType.DMA
    part = pltpu.VMEM((RCH, 2, 104, 128), F32)
    cache = pltpu.VMEM((SLOTS, 32, positions * kv, head), BF16)
    table = pltpu.VMEM((rows, 128), F32)
    pair = pltpu.VMEM((rows * 2, 128), F32)
    shared = pltpu.VMEM((8, rows, 128), F32)
    line = pltpu.VMEM((8, width), F32)
    new = jax.ShapeDtypeStruct((rows * kv, head), BF16)
    pin = functools.partial(pltpu.with_memory_space_constraint, memory_space=pltpu.HBM)
    return pl.pallas_call(
        functools.partial(block_kernel, positions=positions, scale=head ** -0.5),
        out_shape=(jax.ShapeDtypeStruct((rows, width), BF16), new, new),
        in_specs=[HBM] * 11,
        out_specs=(VMEM, VMEM, VMEM),
        scratch_shapes=[pltpu.SMEM((rows // 128, 128), jnp.int32), pltpu.VMEM((rows // 128, 128), jnp.int32), pltpu.VMEM((1, 128), F32),
                        pltpu.VMEM((width // 128, 128), BF16), pltpu.VMEM((width // 128, 128), BF16), dma((5,)),
                        pltpu.VMEM((rows, width), BF16), pltpu.VMEM((rows, 512), F32), pltpu.VMEM((rows * 16, 128), F32),
                        pair, pair, shared, shared, table, table, line, line,
                        dma((4,)), dma((4,)), dma((3, 4)), dma((8,)), dma((8,)),
                        cache, cache,
                        pltpu.VMEM((512, positions * kv), F32), pltpu.VMEM((512, 16), F32),
                        pltpu.VMEM((512, positions * kv), BF16), pltpu.VMEM((512, 128), F32),
                        pltpu.VMEM((STEPS, 4, 104, 128), F32), pltpu.VMEM((STEPS, 2, 104, 128), F32),
                        part, part, part,
                        pltpu.VMEM((96, 128), F32),
                        pltpu.VMEM((RCH, 16, depth), F32), pltpu.VMEM((RCH, 16, depth), F32),
                        pltpu.VMEM((2, 16, depth), BF16),
                        pltpu.VMEM((8, depth, cols), BF16),
                        pltpu.VMEM((rows // 2, half), BF16),
                        pltpu.VMEM((32, cols), F32),
                        pltpu.VMEM((NMSG, 32, cols), F32), pltpu.VMEM((NMSG, 32, cols), F32),
                        pltpu.VMEM((2, 2, NMSG, 32, cols), F32),
                        dma((SLOTS,)), dma((SLOTS,)), dma((STEPS,)), dma((STEPS,)), dma((RCH,)), dma((RCH,)),
                        dma((RCH,)), dma((RCH,)), dma((QCH,)), dma] + [dma((NMSG,))] * 12,
        compiler_params=pltpu.CompilerParams(collective_id=0, has_side_effects=True, vmem_limit_bytes=BLOCK_LIMIT),
        name="block",
    )(pin(lengths.reshape(rows // 128, 128)), pin(jnp.asarray(freq)), pin(gain.reshape(width // 128, 128)), pin(bias.reshape(width // 128, 128)),
      hidden, w_q, w_k, w_v, k_cache.reshape(batch, positions * kv, head), v_cache.reshape(batch, positions * kv, head), w_o)


def emit_kernel(*refs):
    n = len(refs) // 2
    copies = [pltpu.make_async_copy(refs[i], refs[n + i], refs[2 * n].at[i]) for i in range(n)]
    for copy in copies:
        copy.start()
    for copy in copies:
        copy.wait()


def emit(*values):
    n = len(values)
    return pl.pallas_call(
        emit_kernel,
        out_shape=tuple(jax.ShapeDtypeStruct(v.shape, v.dtype) for v in values),
        in_specs=[VMEM] * n, out_specs=(HBM,) * n,
        scratch_shapes=[pltpu.SemaphoreType.DMA((n,))],
        compiler_params=pltpu.CompilerParams(vmem_limit_bytes=4 * 1024 * 1024),
        name="emit",
    )(*values)


def solution(mesh):
    def local_step(hidden, ln_gain, ln_bias, w_q, w_k, w_v, w_o, k_cache, v_cache, lengths):
        batch, _, kv, head = k_cache.shape
        out, k_new, v_new = emit(*block(lengths, ln_gain, ln_bias, hidden, w_q, w_k, w_v, k_cache, v_cache, w_o))
        return out, k_new.reshape(batch, kv, head), v_new.reshape(batch, kv, head)

    row_spec = P('dp', None)
    cache_spec = P('dp', 'sp', 'tp', None)
    head_spec = P('dp', 'tp', None)
    return jax.shard_map(local_step, mesh=mesh, in_specs=(row_spec, P(None), P(None), P(None, 'tp'), P(None, 'tp'), P(None, 'tp'), P('tp', None), cache_spec, cache_spec, P('dp')), out_specs=(row_spec, head_spec, head_spec), check_vma=False)
```

```python
import functools

import jax
import jax.numpy as jnp
import numpy as np
from jax import lax
from jax.experimental import pallas as pl
from jax.experimental.pallas import tpu as pltpu
from jax.sharding import PartitionSpec as P

F32 = jnp.float32
BF16 = jnp.bfloat16
MESH = pl.DeviceIdType.MESH
NEG = -0.7 * float(np.finfo(np.float32).max)
BLOCK_LIMIT = 49 * 1024 * 1024
HBM = pl.BlockSpec(memory_space=pltpu.HBM)
VMEM = pl.BlockSpec(memory_space=pltpu.VMEM)


RCH = 4
QCH = 6
NMSG = RCH * QCH
PER = QCH // 2
STEPS = 2 * RCH
HOP = 4
LAG = 6
LAG_Y = 6
SLOTS = 3


def scaled_sum(a, b):
    m_a, l_a, m_b, l_b = a[96:97, :], a[97:98, :], b[96:97, :], b[97:98, :]
    top = jnp.maximum(m_a, m_b)
    f_a, f_b = jnp.exp(m_a - top), jnp.exp(m_b - top)
    total = l_a * f_a + l_b * f_b
    r = lax.broadcasted_iota(jnp.int32, (128, 128), 0)
    turned = jnp.transpose(jnp.where(r == 0, f_a, jnp.where(r == 1, f_b, total)))
    acc = a[:96, :] * turned[:96, 0:1] + b[:96, :] * turned[:96, 1:2]
    return acc, top, total, turned[:96, 2:3]


def block_kernel(len_hbm, freq_hbm, gain_hbm, bias_hbm, x_hbm, wq_hbm, wk_hbm, wv_hbm, k_hbm, v_hbm, w_hbm,
                 obuf, kn_ref, vn_ref,
                 len_ref, len_rows, freq_ref, gain_ref, bias_ref, s_in,
                 hbuf, acc_ref, q_ref, kf, vf, xs, xr, cosb, sinb, gainb, biasb, s_h, s_q, s_g, s_xs, r_xs,
                 kbuf, vbuf, sbuf, self_buf, pbuf, stat, msg, part, send_y, recv_y, comb_o, ctx_t, ctx_s, ctx_r,
                 lhs, wbuf, xbuf, prod, rs_in, rs_out, fin,
                 s_k, s_v, s_p, r_p, s_y, r_y, s_c, r_c, s_w, s_x,
                 s_rs, r_rs, r_re, s_ag, r_ag, s_ae, s_fy, r_fy, s_fd, r_fd, s_fe, r_fe, *, positions, scale):
    d, z, s = lax.axis_index("dp"), lax.axis_index("tp"), lax.axis_index("sp")
    y, c = s // 2, s % 2
    yo, co = 1 - y, 1 - c
    u = c * z + co * (3 - z)
    partner, across = (d, z, 2 * y + co), (d, z, 2 * yo + c)
    ahead, behind = (d, z + 2 * c - 1, s), (d, z - 2 * c + 1, s)
    width = wbuf.shape[2]
    half = QCH * width

    def remote(src, dst, send, recv, dev):
        return pltpu.make_async_remote_copy(src_ref=src, dst_ref=dst, send_sem=send, recv_sem=recv,
                                            device_id=dev, device_id_type=MESH)

    barrier = pltpu.get_barrier_semaphore()
    pl.semaphore_signal(barrier, inc=1, device_id=partner, device_id_type=MESH)
    pl.semaphore_signal(barrier, inc=1, device_id=across, device_id_type=MESH)

    @pl.when(u < 3)
    def _():
        pl.semaphore_signal(barrier, inc=1, device_id=ahead, device_id_type=MESH)

    @pl.when(u > 0)
    def _():
        pl.semaphore_signal(barrier, inc=1, device_id=behind, device_id_type=MESH)

    def first_row(i):
        return 128 * ((i % 2) * y + (1 - i % 2) * yo) + 32 * (i // 2)

    def k_copy(i):
        return pltpu.make_async_copy(k_hbm.at[pl.ds(first_row(i), 32)], kbuf.at[i % SLOTS], s_k.at[i % SLOTS])

    def v_copy(i):
        return pltpu.make_async_copy(v_hbm.at[pl.ds(first_row(i), 32)], vbuf.at[i % SLOTS], s_v.at[i % SLOTS])

    def w_copy(q):
        return pltpu.make_async_copy(w_hbm.at[:, pl.ds(c * half + q * width, width)], wbuf.at[q], s_w.at[q])

    x_copy = pltpu.make_async_copy(x_hbm.at[pl.ds(y * 128, 128), pl.ds(c * half, half)], xbuf, s_x)

    rows, model = hbuf.shape
    tiles = model // 128
    depth = wbuf.shape[1]

    def h_copy(i):
        at = pl.ds(i * 64, 64)
        return pltpu.make_async_copy(x_hbm.at[at], obuf.at[at], s_h.at[i])

    inputs = ((len_hbm, len_ref), (len_hbm, len_rows), (freq_hbm, freq_ref), (gain_hbm, gain_ref), (bias_hbm, bias_ref))
    small = [pltpu.make_async_copy(src, dst, s_in.at[n]) for n, (src, dst) in enumerate(inputs)]
    for copy in small:
        copy.start()
    for i in range(rows // 64):
        h_copy(i).start()

    def q_copy(n):
        return pltpu.make_async_copy(wq_hbm.at[pl.ds(n * depth, depth), pl.ds(c * 768, 512)], wbuf.at[n], s_q.at[n])

    def g_copies(n):
        at = pl.ds(n * depth, depth)
        return [pltpu.make_async_copy(wq_hbm.at[at, pl.ds(c * 768 + 512, 256)], wbuf.at[4 + n, :, pl.ds(0, 256)], s_g.at[0, n]),
                pltpu.make_async_copy(wk_hbm.at[at, pl.ds(c * 128, 128)], wbuf.at[4 + n, :, pl.ds(256, 128)], s_g.at[1, n]),
                pltpu.make_async_copy(wv_hbm.at[at, pl.ds(c * 128, 128)], wbuf.at[4 + n, :, pl.ds(384, 128)], s_g.at[2, n])]

    def share(slot):
        return remote(xs.at[slot], xr.at[slot], s_xs.at[slot], r_xs.at[slot], partner)

    for copy in small:
        copy.wait()
    for k in range(tiles):
        gainb[:, k * 128:(k + 1) * 128] = jnp.broadcast_to(1.0 + gain_ref[k:k + 1, :].astype(F32), (8, 128))
        biasb[:, k * 128:(k + 1) * 128] = jnp.broadcast_to(bias_ref[k:k + 1, :].astype(F32), (8, 128))
    for i in range(rows // 128):
        angle = jnp.transpose(jnp.broadcast_to(len_rows[i:i + 1, :].astype(F32), (128, 128))) * freq_ref[...]
        cosb[i * 128:(i + 1) * 128, :] = jnp.cos(angle)
        sinb[i * 128:(i + 1) * 128, :] = jnp.sin(angle)

    def norm(i, carry):
        h_copy(i).wait()

        @pl.when(i < 2)
        def _():
            q_copy(2 * i).start()
            q_copy(2 * i + 1).start()

        @pl.when(i >= 2)
        def _():
            for copy in g_copies(2 * i - 4) + g_copies(2 * i - 3):
                copy.start()

        ats = [pl.ds(pl.multiple_of(i * 64 + j * 16, 16), 16) for j in range(4)]
        lanes = [slice(k * 128, (k + 1) * 128) for k in range(tiles)]
        means, scales = [], []
        for at in ats:
            accs = [obuf[at, lanes[k]].astype(F32) for k in range(2)]
            for k in range(2, tiles):
                accs[k % 2] = accs[k % 2] + obuf[at, lanes[k]].astype(F32)
            mean = jnp.sum(accs[0] + accs[1], axis=-1, keepdims=True) * (1.0 / model)
            means.append(jnp.broadcast_to(mean, (16, 128)))
        for at, mean in zip(ats, means):
            accs = [jnp.zeros((16, 128), F32) for _ in range(2)]
            for k in range(tiles):
                centred = obuf[at, lanes[k]].astype(F32) - mean
                accs[k % 2] = accs[k % 2] + centred * centred
            var = jnp.sum(accs[0] + accs[1], axis=-1, keepdims=True) * (1.0 / model)
            scales.append(jnp.broadcast_to(lax.rsqrt(var + 1e-5), (16, 128)))
        for k in range(tiles):
            gain = jnp.concatenate([gainb[:, lanes[k]]] * 2, axis=0)
            bias = jnp.concatenate([biasb[:, lanes[k]]] * 2, axis=0)
            for at, mean, factor in zip(ats, means, scales):
                hbuf[at, lanes[k]] = ((obuf[at, lanes[k]].astype(F32) - mean) * factor * gain + bias).astype(BF16)
        return carry

    lax.fori_loop(0, rows // 64, norm, 0)
    for i in range(SLOTS):
        k_copy(i).start()
        v_copy(i).start()
    x_copy.start()

    lane_r = lax.broadcasted_iota(jnp.int32, (rows, 128), 1)

    def rotate(v):
        other = jnp.where(lane_r < 32, -pltpu.roll(v, 96, 1), pltpu.roll(v, 32, 1))
        return jnp.where(lane_r < 64, v * cosb[...] + other * sinb[...], v)

    def spread_out(slot, core, v):
        if slot < 6:
            q_ref[pl.ds(6 * core + slot, rows, stride=16), :] = v
        else:
            dst = kf if slot == 6 else vf
            dst[pl.ds(core, rows, stride=2), :] = v

    for h in range(12, 16):
        q_ref[pl.ds(h, rows, stride=16), :] = jnp.zeros((rows, 128), F32)

    for g in range(2):
        for n in range(4):
            for copy in ([q_copy(n)] if g == 0 else g_copies(n)):
                copy.wait()
        parts = [jnp.dot(hbuf[:, n * depth:(n + 1) * depth], wbuf[4 * g + n], preferred_element_type=F32) for n in range(4)]
        acc_ref[...] = (parts[0] + parts[1]) + (parts[2] + parts[3])
        if g == 0:
            pl.semaphore_wait(barrier, 2 + (z + 2) // 3 + (5 - z) // 3)
        for slot in range(4 * g, 4 * g + 4):
            v = acc_ref[:, (slot % 4) * 128:(slot % 4 + 1) * 128]
            xs[slot] = rotate(v) if slot < 7 else v
            share(slot).start()
        for slot in range(4 * g, 4 * g + 4):
            spread_out(slot, c, xs[slot])
    for slot in range(8):
        share(slot).wait_recv()
        spread_out(slot, co, xr[slot])
    kn_ref[...] = kf[...].astype(BF16)
    vn_ref[...] = vf[...].astype(BF16)

    first = s * positions
    col = lax.broadcasted_iota(jnp.int32, (16, 2 * positions), 1)
    row = lax.broadcasted_iota(jnp.int32, (16, 2 * positions), 0)
    place = jnp.where(lax.rem(col, 2) == jnp.where(row >= 6, 1, 0), first + col // 2, 1 << 30)
    pick_row = lax.broadcasted_iota(jnp.int32, (128, 16), 0)
    pick_col = lax.broadcasted_iota(jnp.int32, (128, 16), 1)
    pick = pick_col == 2 * (pick_row // 16) + jnp.where(lax.rem(pick_row, 16) >= 6, 1, 0)
    nt = (((1,), (1,)), ((), ()))

    def attention(i):
        k_copy(i).wait()
        v_copy(i).wait()
        slot = i % SLOTS
        base = first_row(i)
        spread = jnp.where(pick, 1.0, 0.0).astype(BF16)
        lane = lax.broadcasted_iota(jnp.int32, (128, 128), 1)
        begin = lax.broadcasted_iota(jnp.int32, (16, 16), 0) * 0 + first
        own_w = [None] * 4

        def scores(g):
            q8 = q_ref[pl.ds(pl.multiple_of(base * 16 + g * 128, 128), 128), :].astype(BF16)
            kn = kn_ref[pl.ds(pl.multiple_of(base * 2 + g * 16, 16), 16), :]
            self8 = lax.dot_general(q8, kn, nt, preferred_element_type=F32) * scale
            self8 = jnp.where(pick, self8, NEG)
            for b in range(8):
                at = slice(g * 128 + b * 16, g * 128 + (b + 1) * 16)
                length = len_ref[base // 128, base % 128 + g * 8 + b]
                owner = (length >= begin) & (length < begin + positions)
                sc = lax.dot_general(q8[b * 16:(b + 1) * 16, :], kbuf[slot, g * 8 + b], nt, preferred_element_type=F32) * scale
                sbuf[at, :] = jnp.where(place < length, sc, NEG)
                self_buf[at, :] = jnp.where(owner, self8[b * 16:(b + 1) * 16, :], NEG)

        def weights(g):
            at = slice(g * 128, (g + 1) * 128)
            sc = sbuf[at, :]
            own = jnp.max(self_buf[at, :], axis=1, keepdims=True)
            top = jnp.maximum(jnp.max(sc, axis=1, keepdims=True), own)
            w = jnp.exp(sc - top)
            own_w[g] = jnp.exp(own - top)
            total = jnp.sum(w, axis=1, keepdims=True) + own_w[g]
            pbuf[at, :] = w.astype(BF16)
            stat[at, :] = jnp.where(lane == 0, top, total)

        def sums(g):
            vn = vn_ref[pl.ds(pl.multiple_of(base * 2 + g * 16, 16), 16), :]
            own8 = own_w[g] * jnp.dot(spread, vn, preferred_element_type=F32)
            turned = jnp.transpose(stat[g * 128:(g + 1) * 128, :])[:8, :]
            msg[i, g, 96:104, :] = jnp.concatenate([turned[:, b * 16:b * 16 + 12] for b in range(8)] + [jnp.zeros((8, 32), F32)], axis=1)
            for b in range(8):
                at = slice(g * 128 + b * 16, g * 128 + (b + 1) * 16)
                acc = jnp.dot(pbuf[at, :], vbuf[slot, g * 8 + b], preferred_element_type=F32) + own8[b * 16:(b + 1) * 16, :]
                msg[i, g, b * 12:(b + 1) * 12, :] = acc[:12, :]

        for g in range(6):
            if g < 4:
                scores(g)
            if 1 <= g <= 4:
                weights(g - 1)
            if g >= 2:
                sums(g - 2)

    def to_partner(i):
        return remote(msg.at[i, pl.ds(2 * co, 2)], part.at[i], s_p.at[i], r_p.at[i], partner)

    def to_across(r):
        return remote(send_y.at[r], recv_y.at[r], s_y.at[r], r_y.at[r], across)

    def ctx_copy(r):
        return remote(ctx_s.at[r], ctx_r.at[r], s_c.at[r], r_c.at[r], partner)

    def merge(i, dst):
        to_partner(i).wait_recv()
        for k in range(2):
            acc, top, total, _ = scaled_sum(msg[i, 2 * c + k], part[i, k])
            dst[k, :96, :] = acc
            line = lax.broadcasted_iota(jnp.int32, (8, 128), 0)
            dst[k, 96:104, :] = jnp.where(line == 0, top, total)

    def context(r):
        to_across(r).wait_recv()
        for k in range(2):
            acc, _, _, total = scaled_sum(comb_o[r, k], recv_y[r, k])
            ctx_t[...] = acc / total
            for h in range(12):
                ctx_s[r, k * 8:(k + 1) * 8, h * 128:(h + 1) * 128] = ctx_t[pl.ds(h, 8, stride=12), :]
        ctx_copy(r).start()

    def rs(j):
        return remote(rs_out.at[j], rs_in.at[j], s_rs.at[j], r_rs.at[j], ahead)

    def rs_end(j):
        return remote(rs_out.at[j], fin.at[y, c, j], s_rs.at[j], r_re.at[j], behind)

    def final(dst, send, recv, h, core, j):
        f = fin.at[h, core, j]
        return remote(f, f, send.at[j], recv.at[j], dst)

    def ag(j):
        return final(behind, s_ag, r_ag, y, c, j)

    def ag_end(j):
        return final(ahead, s_ae, r_ag, y, c, j)

    def fy(j):
        return final(across, s_fy, r_fy, y, c, j)

    def fy_in(j):
        return final(across, s_fy, r_fy, yo, c, j)

    def fd(j):
        return final(partner, s_fd, r_fd, y, c, j)

    def fd_in(j):
        return final(partner, s_fd, r_fd, y, co, j)

    def fe(j):
        return final(partner, s_fe, r_fe, yo, c, j)

    def fe_in(j):
        return final(partner, s_fe, r_fe, yo, co, j)

    def convert(h, core, j):
        at = pl.ds(pl.multiple_of(h * 128 + (j // QCH) * 32, 32), 32)
        obuf[at, pl.ds(pl.multiple_of(core * half + (j % QCH) * width, width), width)] = fin[h, core, j].astype(BF16)

    hops = u - 2 * (u // 3)
    lag = LAG * (2 - hops)
    lag_y = lag + LAG_Y
    start = 2 * QCH + HOP * hops
    hops_p = 3 - u - 2 * ((3 - u) // 3)
    start_p = 2 * QCH + HOP * hops_p + LAG * (2 - hops_p) + LAG_Y + 4

    def tick(t, carry):
        i, r6 = t // PER, t // QCH

        @pl.when((t < PER * STEPS) & (t % PER == 0))
        def _():
            attention(i)
            to_partner(i).start()

            @pl.when(i < STEPS - SLOTS)
            def _():
                k_copy(i + SLOTS).start()
                v_copy(i + SLOTS).start()

            @pl.when((i >= 2) & (i < 5))
            def _():
                w_copy(2 * i - 4).start()
                w_copy(2 * i - 3).start()

        @pl.when((t % QCH == PER + 1) & (t < NMSG))
        def _():
            merge(2 * r6, send_y.at[r6])
            to_across(r6).start()

        @pl.when((t % QCH == 1) & (t >= QCH) & (t < NMSG + QCH))
        def _():
            merge(2 * r6 - 1, comb_o.at[r6 - 1])

        @pl.when((t % QCH == QCH - 2) & (t >= QCH) & (t < NMSG + QCH))
        def _():
            context(r6 - 1)

        j = t - start

        @pl.when((j >= 0) & (j < NMSG))
        def _():
            r, q = j // QCH, j % QCH

            @pl.when(q == 0)
            def _():
                ctx_copy(r).wait_recv()
                lhs[c] = ctx_s[r].astype(BF16)
                lhs[co] = ctx_r[r].astype(BF16)

            @pl.when(r == 0)
            def _():
                w_copy(q).wait()

            @pl.when(j == 0)
            def _():
                x_copy.wait()

            prod[...] = jnp.dot(lhs[...].reshape(32, lhs.shape[2]), wbuf[q], preferred_element_type=F32)

            @pl.when(u == 0)
            def _():
                rs_out[j] = prod[...]
                rs(j).start()

            @pl.when(u == 3)
            def _():
                rs_out[j] = prod[...]
                rs_end(j).start()

            @pl.when(u == 1)
            def _():
                rs(j).wait_recv()
                rs_out[j] = rs_in[j] + prod[...]
                rs(j).start()

            @pl.when(u == 2)
            def _():
                x = xbuf[pl.ds(pl.multiple_of(r * 32, 32), 32), pl.ds(pl.multiple_of(q * width, width), width)]
                rs_end(j).wait_recv()
                rs(j).wait_recv()
                fin[y, c, j] = (rs_in[j] + prod[...]) + fin[y, c, j] + x.astype(F32)
                ag(j).start()
                ag_end(j).start()
                fy(j).start()
                fd(j).start()
                convert(y, c, j)

        ja = j - lag

        @pl.when((lag > 0) & (ja >= 0) & (ja < NMSG))
        def _():
            ag(ja).wait_recv()

            @pl.when(u == 1)
            def _():
                ag(ja).start()

            fy(ja).start()
            fd(ja).start()
            convert(y, c, ja)

        jy = j - lag_y

        @pl.when((jy >= 0) & (jy < NMSG))
        def _():
            fy_in(jy).wait_recv()
            fe(jy).start()
            convert(yo, c, jy)

        jp = t - start_p

        @pl.when((jp >= 0) & (jp < NMSG))
        def _():
            fd_in(jp).wait_recv()
            fe_in(jp).wait_recv()
            convert(y, co, jp)
            convert(yo, co, jp)

        return carry

    lax.fori_loop(0, 2 * QCH + 2 * LAG + LAG_Y + 4 + NMSG, tick, 0)

    def drain(j, carry):
        @pl.when(u < 2)
        def _():
            rs(j).wait_send()

        @pl.when(u == 3)
        def _():
            rs_end(j).wait_send()

        @pl.when((u == 1) | (u == 2))
        def _():
            ag(j).wait_send()

        @pl.when(u == 2)
        def _():
            ag_end(j).wait_send()

        fy(j).wait_send()
        fd(j).wait_send()
        fe(j).wait_send()
        return carry

    lax.fori_loop(0, NMSG, drain, 0)
    for slot in range(8):
        share(slot).wait_send()
    for i in range(STEPS):
        to_partner(i).wait_send()
    for r in range(RCH):
        to_across(r).wait_send()
        ctx_copy(r).wait_send()


def block(lengths, gain, bias, hidden, w_q, w_k, w_v, k_cache, v_cache, w_o):
    batch, positions, kv, head = k_cache.shape
    rows, width = hidden.shape
    depth = w_o.shape[0]
    half = width // 2
    cols = half // QCH
    freq = 10000.0 ** (-2.0 * np.arange(32, dtype=np.float32) / np.float32(64))
    freq = np.concatenate([freq, freq, np.zeros(64)]).astype(np.float32).reshape(1, 128)
    dma = pltpu.SemaphoreType.DMA
    part = pltpu.VMEM((RCH, 2, 104, 128), F32)
    cache = pltpu.VMEM((SLOTS, 32, positions * kv, head), BF16)
    table = pltpu.VMEM((rows, 128), F32)
    pair = pltpu.VMEM((rows * 2, 128), F32)
    shared = pltpu.VMEM((8, rows, 128), F32)
    line = pltpu.VMEM((8, width), F32)
    new = jax.ShapeDtypeStruct((rows * kv, head), BF16)
    pin = functools.partial(pltpu.with_memory_space_constraint, memory_space=pltpu.HBM)
    return pl.pallas_call(
        functools.partial(block_kernel, positions=positions, scale=head ** -0.5),
        out_shape=(jax.ShapeDtypeStruct((rows, width), BF16), new, new),
        in_specs=[HBM] * 11,
        out_specs=(VMEM, VMEM, VMEM),
        scratch_shapes=[pltpu.SMEM((rows // 128, 128), jnp.int32), pltpu.VMEM((rows // 128, 128), jnp.int32), pltpu.VMEM((1, 128), F32),
                        pltpu.VMEM((width // 128, 128), BF16), pltpu.VMEM((width // 128, 128), BF16), dma((5,)),
                        pltpu.VMEM((rows, width), BF16), pltpu.VMEM((rows, 512), F32), pltpu.VMEM((rows * 16, 128), F32),
                        pair, pair, shared, shared, table, table, line, line,
                        dma((4,)), dma((4,)), dma((3, 4)), dma((8,)), dma((8,)),
                        cache, cache,
                        pltpu.VMEM((512, positions * kv), F32), pltpu.VMEM((512, 16), F32),
                        pltpu.VMEM((512, positions * kv), BF16), pltpu.VMEM((512, 128), F32),
                        pltpu.VMEM((STEPS, 4, 104, 128), F32), pltpu.VMEM((STEPS, 2, 104, 128), F32),
                        part, part, part,
                        pltpu.VMEM((96, 128), F32),
                        pltpu.VMEM((RCH, 16, depth), F32), pltpu.VMEM((RCH, 16, depth), F32),
                        pltpu.VMEM((2, 16, depth), BF16),
                        pltpu.VMEM((8, depth, cols), BF16),
                        pltpu.VMEM((rows // 2, half), BF16),
                        pltpu.VMEM((32, cols), F32),
                        pltpu.VMEM((NMSG, 32, cols), F32), pltpu.VMEM((NMSG, 32, cols), F32),
                        pltpu.VMEM((2, 2, NMSG, 32, cols), F32),
                        dma((SLOTS,)), dma((SLOTS,)), dma((STEPS,)), dma((STEPS,)), dma((RCH,)), dma((RCH,)),
                        dma((RCH,)), dma((RCH,)), dma((QCH,)), dma] + [dma((NMSG,))] * 12,
        compiler_params=pltpu.CompilerParams(collective_id=0, has_side_effects=True, vmem_limit_bytes=BLOCK_LIMIT),
        name="block",
    )(pin(lengths.reshape(rows // 128, 128)), pin(jnp.asarray(freq)), pin(gain.reshape(width // 128, 128)), pin(bias.reshape(width // 128, 128)),
      hidden, w_q, w_k, w_v, k_cache.reshape(batch, positions * kv, head), v_cache.reshape(batch, positions * kv, head), w_o)


def emit_kernel(*refs):
    n = len(refs) // 2
    copies = [pltpu.make_async_copy(refs[i], refs[n + i], refs[2 * n].at[i]) for i in range(n)]
    for copy in copies:
        copy.start()
    for copy in copies:
        copy.wait()


def emit(*values):
    n = len(values)
    return pl.pallas_call(
        emit_kernel,
        out_shape=tuple(jax.ShapeDtypeStruct(v.shape, v.dtype) for v in values),
        in_specs=[VMEM] * n, out_specs=(HBM,) * n,
        scratch_shapes=[pltpu.SemaphoreType.DMA((n,))],
        compiler_params=pltpu.CompilerParams(vmem_limit_bytes=4 * 1024 * 1024),
        name="emit",
    )(*values)


def solution(mesh):
    def local_step(hidden, ln_gain, ln_bias, w_q, w_k, w_v, w_o, k_cache, v_cache, lengths):
        batch, _, kv, head = k_cache.shape
        out, k_new, v_new = emit(*block(lengths, ln_gain, ln_bias, hidden, w_q, w_k, w_v, k_cache, v_cache, w_o))
        return out, k_new.reshape(batch, kv, head), v_new.reshape(batch, kv, head)

    row_spec = P('dp', None)
    cache_spec = P('dp', 'sp', 'tp', None)
    head_spec = P('dp', 'tp', None)
    return jax.shard_map(local_step, mesh=mesh, in_specs=(row_spec, P(None), P(None), P(None, 'tp'), P(None, 'tp'), P(None, 'tp'), P('tp', None), cache_spec, cache_spec, P('dp')), out_specs=(row_spec, head_spec, head_spec), check_vma=False)
```

```python
import functools

import jax
import jax.numpy as jnp
import numpy as np
from jax import lax
from jax.experimental import pallas as pl
from jax.experimental.pallas import tpu as pltpu
from jax.sharding import PartitionSpec as P

F32 = jnp.float32
BF16 = jnp.bfloat16
MESH = pl.DeviceIdType.MESH
NEG = -0.7 * float(np.finfo(np.float32).max)
BLOCK_LIMIT = 49 * 1024 * 1024
HBM = pl.BlockSpec(memory_space=pltpu.HBM)
VMEM = pl.BlockSpec(memory_space=pltpu.VMEM)


RCH = 4
QCH = 6
NMSG = RCH * QCH
PER = QCH // 2
STEPS = 2 * RCH
HOP = 4
LAG = 6
LAG_Y = 6
SLOTS = 3


def scaled_sum(a, b):
    m_a, l_a, m_b, l_b = a[96:97, :], a[97:98, :], b[96:97, :], b[97:98, :]
    top = jnp.maximum(m_a, m_b)
    f_a, f_b = jnp.exp(m_a - top), jnp.exp(m_b - top)
    total = l_a * f_a + l_b * f_b
    r = lax.broadcasted_iota(jnp.int32, (128, 128), 0)
    turned = jnp.transpose(jnp.where(r == 0, f_a, jnp.where(r == 1, f_b, total)))
    acc = a[:96, :] * turned[:96, 0:1] + b[:96, :] * turned[:96, 1:2]
    return acc, top, total, turned[:96, 2:3]


def block_kernel(len_hbm, freq_hbm, gain_hbm, bias_hbm, x_hbm, wq_hbm, wk_hbm, wv_hbm, k_hbm, v_hbm, w_hbm,
                 obuf, kn_ref, vn_ref,
                 len_ref, len_rows, freq_ref, gain_ref, bias_ref, s_in,
                 hbuf, acc_ref, q_ref, kf, vf, xs, xr, cosb, sinb, gainb, biasb, s_h, s_q, s_g, s_xs, r_xs,
                 kbuf, vbuf, sbuf, self_buf, pbuf, stat, msg, part, send_y, recv_y, comb_o, ctx_t, ctx_s, ctx_r,
                 lhs, wbuf, xbuf, prod, rs_in, rs_out, fin,
                 s_k, s_v, s_p, r_p, s_y, r_y, s_c, r_c, s_w, s_x,
                 s_rs, r_rs, r_re, s_ag, r_ag, s_ae, s_fy, r_fy, s_fd, r_fd, s_fe, r_fe, *, positions, scale):
    d, z, s = lax.axis_index("dp"), lax.axis_index("tp"), lax.axis_index("sp")
    y, c = s // 2, s % 2
    yo, co = 1 - y, 1 - c
    u = c * z + co * (3 - z)
    partner, across = (d, z, 2 * y + co), (d, z, 2 * yo + c)
    ahead, behind = (d, z + 2 * c - 1, s), (d, z - 2 * c + 1, s)
    width = wbuf.shape[2]
    half = QCH * width

    def remote(src, dst, send, recv, dev):
        return pltpu.make_async_remote_copy(src_ref=src, dst_ref=dst, send_sem=send, recv_sem=recv,
                                            device_id=dev, device_id_type=MESH)

    barrier = pltpu.get_barrier_semaphore()
    pl.semaphore_signal(barrier, inc=1, device_id=partner, device_id_type=MESH)
    pl.semaphore_signal(barrier, inc=1, device_id=across, device_id_type=MESH)

    @pl.when(u < 3)
    def _():
        pl.semaphore_signal(barrier, inc=1, device_id=ahead, device_id_type=MESH)

    @pl.when(u > 0)
    def _():
        pl.semaphore_signal(barrier, inc=1, device_id=behind, device_id_type=MESH)

    def first_row(i):
        return 128 * ((i % 2) * y + (1 - i % 2) * yo) + 32 * (i // 2)

    def k_copy(i):
        return pltpu.make_async_copy(k_hbm.at[pl.ds(first_row(i), 32)], kbuf.at[i % SLOTS], s_k.at[i % SLOTS])

    def v_copy(i):
        return pltpu.make_async_copy(v_hbm.at[pl.ds(first_row(i), 32)], vbuf.at[i % SLOTS], s_v.at[i % SLOTS])

    def w_copy(q):
        return pltpu.make_async_copy(w_hbm.at[:, pl.ds(c * half + q * width, width)], wbuf.at[q], s_w.at[q])

    x_copy = pltpu.make_async_copy(x_hbm.at[pl.ds(y * 128, 128), pl.ds(c * half, half)], xbuf, s_x)

    rows, model = hbuf.shape
    tiles = model // 128
    depth = wbuf.shape[1]

    def h_copy(i):
        at = pl.ds(i * 64, 64)
        return pltpu.make_async_copy(x_hbm.at[at], obuf.at[at], s_h.at[i])

    inputs = ((len_hbm, len_ref), (len_hbm, len_rows), (freq_hbm, freq_ref), (gain_hbm, gain_ref), (bias_hbm, bias_ref))
    small = [pltpu.make_async_copy(src, dst, s_in.at[n]) for n, (src, dst) in enumerate(inputs)]
    for copy in small:
        copy.start()
    for i in range(rows // 64):
        h_copy(i).start()

    def q_copy(n):
        return pltpu.make_async_copy(wq_hbm.at[pl.ds(n * depth, depth), pl.ds(c * 768, 512)], wbuf.at[n], s_q.at[n])

    def g_copies(n):
        at = pl.ds(n * depth, depth)
        return [pltpu.make_async_copy(wq_hbm.at[at, pl.ds(c * 768 + 512, 256)], wbuf.at[4 + n, :, pl.ds(0, 256)], s_g.at[0, n]),
                pltpu.make_async_copy(wk_hbm.at[at, pl.ds(c * 128, 128)], wbuf.at[4 + n, :, pl.ds(256, 128)], s_g.at[1, n]),
                pltpu.make_async_copy(wv_hbm.at[at, pl.ds(c * 128, 128)], wbuf.at[4 + n, :, pl.ds(384, 128)], s_g.at[2, n])]

    def share(slot):
        return remote(xs.at[slot], xr.at[slot], s_xs.at[slot], r_xs.at[slot], partner)

    for h in range(12, 16):
        q_ref[pl.ds(h, rows, stride=16), :] = jnp.zeros((rows, 128), F32)
    for copy in small:
        copy.wait()
    for k in range(tiles):
        gainb[:, k * 128:(k + 1) * 128] = jnp.broadcast_to(1.0 + gain_ref[k:k + 1, :].astype(F32), (8, 128))
        biasb[:, k * 128:(k + 1) * 128] = jnp.broadcast_to(bias_ref[k:k + 1, :].astype(F32), (8, 128))
    for i in range(rows // 128):
        angle = jnp.transpose(jnp.broadcast_to(len_rows[i:i + 1, :].astype(F32), (128, 128))) * freq_ref[...]
        cosb[i * 128:(i + 1) * 128, :] = jnp.cos(angle)
        sinb[i * 128:(i + 1) * 128, :] = jnp.sin(angle)

    def norm(i, carry):
        h_copy(i).wait()

        @pl.when(i < 2)
        def _():
            q_copy(2 * i).start()
            q_copy(2 * i + 1).start()

        @pl.when(i >= 2)
        def _():
            for copy in g_copies(2 * i - 4) + g_copies(2 * i - 3):
                copy.start()

        ats = [pl.ds(pl.multiple_of(i * 64 + j * 16, 16), 16) for j in range(4)]
        lanes = [slice(k * 128, (k + 1) * 128) for k in range(tiles)]
        means, scales = [], []
        for at in ats:
            accs = [obuf[at, lanes[k]].astype(F32) for k in range(2)]
            for k in range(2, tiles):
                accs[k % 2] = accs[k % 2] + obuf[at, lanes[k]].astype(F32)
            mean = jnp.sum(accs[0] + accs[1], axis=-1, keepdims=True) * (1.0 / model)
            means.append(jnp.broadcast_to(mean, (16, 128)))
        for at, mean in zip(ats, means):
            accs = [jnp.zeros((16, 128), F32) for _ in range(2)]
            for k in range(tiles):
                centred = obuf[at, lanes[k]].astype(F32) - mean
                accs[k % 2] = accs[k % 2] + centred * centred
            var = jnp.sum(accs[0] + accs[1], axis=-1, keepdims=True) * (1.0 / model)
            scales.append(jnp.broadcast_to(lax.rsqrt(var + 1e-5), (16, 128)))
        for k in range(tiles):
            gain = jnp.concatenate([gainb[:, lanes[k]]] * 2, axis=0)
            bias = jnp.concatenate([biasb[:, lanes[k]]] * 2, axis=0)
            for at, mean, factor in zip(ats, means, scales):
                hbuf[at, lanes[k]] = ((obuf[at, lanes[k]].astype(F32) - mean) * factor * gain + bias).astype(BF16)
        return carry

    lax.fori_loop(0, rows // 64, norm, 0)
    for i in range(SLOTS):
        k_copy(i).start()
        v_copy(i).start()
    x_copy.start()

    lane_r = lax.broadcasted_iota(jnp.int32, (rows, 128), 1)

    def rotate(v):
        other = jnp.where(lane_r < 32, -pltpu.roll(v, 96, 1), pltpu.roll(v, 32, 1))
        return jnp.where(lane_r < 64, v * cosb[...] + other * sinb[...], v)

    def spread_out(slot, core, v):
        if slot < 6:
            q_ref[pl.ds(6 * core + slot, rows, stride=16), :] = v
        else:
            dst = kf if slot == 6 else vf
            dst[pl.ds(core, rows, stride=2), :] = v

    for g in range(2):
        for n in range(4):
            for copy in ([q_copy(n)] if g == 0 else g_copies(n)):
                copy.wait()
        if g == 1:
            for slot in range(4):
                spread_out(slot, c, xs[slot])
        parts = [jnp.dot(hbuf[:, n * depth:(n + 1) * depth], wbuf[4 * g + n], preferred_element_type=F32) for n in range(4)]
        acc_ref[...] = (parts[0] + parts[1]) + (parts[2] + parts[3])
        if g == 0:
            pl.semaphore_wait(barrier, 2 + (z + 2) // 3 + (5 - z) // 3)
        for slot in range(4 * g, 4 * g + 4):
            v = acc_ref[:, (slot % 4) * 128:(slot % 4 + 1) * 128]
            xs[slot] = rotate(v) if slot < 7 else v
            share(slot).start()
    for slot in range(4, 8):
        spread_out(slot, c, xs[slot])
    for slot in range(8):
        share(slot).wait_recv()
        spread_out(slot, co, xr[slot])
    kn_ref[...] = kf[...].astype(BF16)
    vn_ref[...] = vf[...].astype(BF16)

    first = s * positions
    col = lax.broadcasted_iota(jnp.int32, (16, 2 * positions), 1)
    row = lax.broadcasted_iota(jnp.int32, (16, 2 * positions), 0)
    place = jnp.where(lax.rem(col, 2) == jnp.where(row >= 6, 1, 0), first + col // 2, 1 << 30)
    pick_row = lax.broadcasted_iota(jnp.int32, (128, 16), 0)
    pick_col = lax.broadcasted_iota(jnp.int32, (128, 16), 1)
    pick = pick_col == 2 * (pick_row // 16) + jnp.where(lax.rem(pick_row, 16) >= 6, 1, 0)
    nt = (((1,), (1,)), ((), ()))

    def attention(i):
        k_copy(i).wait()
        v_copy(i).wait()
        slot = i % SLOTS
        base = first_row(i)
        spread = jnp.where(pick, 1.0, 0.0).astype(BF16)
        lane = lax.broadcasted_iota(jnp.int32, (128, 128), 1)
        begin = lax.broadcasted_iota(jnp.int32, (16, 16), 0) * 0 + first
        own_w = [None] * 4

        def scores(g):
            q8 = q_ref[pl.ds(pl.multiple_of(base * 16 + g * 128, 128), 128), :].astype(BF16)
            kn = kn_ref[pl.ds(pl.multiple_of(base * 2 + g * 16, 16), 16), :]
            self8 = lax.dot_general(q8, kn, nt, preferred_element_type=F32) * scale
            self8 = jnp.where(pick, self8, NEG)
            for b in range(8):
                at = slice(g * 128 + b * 16, g * 128 + (b + 1) * 16)
                length = len_ref[base // 128, base % 128 + g * 8 + b]
                owner = (length >= begin) & (length < begin + positions)
                sc = lax.dot_general(q8[b * 16:(b + 1) * 16, :], kbuf[slot, g * 8 + b], nt, preferred_element_type=F32) * scale
                sbuf[at, :] = jnp.where(place < length, sc, NEG)
                self_buf[at, :] = jnp.where(owner, self8[b * 16:(b + 1) * 16, :], NEG)

        def weights(g):
            at = slice(g * 128, (g + 1) * 128)
            sc = sbuf[at, :]
            own = jnp.max(self_buf[at, :], axis=1, keepdims=True)
            top = jnp.maximum(jnp.max(sc, axis=1, keepdims=True), own)
            w = jnp.exp(sc - top)
            own_w[g] = jnp.exp(own - top)
            total = jnp.sum(w, axis=1, keepdims=True) + own_w[g]
            pbuf[at, :] = w.astype(BF16)
            stat[at, :] = jnp.where(lane == 0, top, total)

        def sums(g):
            vn = vn_ref[pl.ds(pl.multiple_of(base * 2 + g * 16, 16), 16), :]
            own8 = own_w[g] * jnp.dot(spread, vn, preferred_element_type=F32)
            turned = jnp.transpose(stat[g * 128:(g + 1) * 128, :])[:8, :]
            msg[i, g, 96:104, :] = jnp.concatenate([turned[:, b * 16:b * 16 + 12] for b in range(8)] + [jnp.zeros((8, 32), F32)], axis=1)
            for b in range(8):
                at = slice(g * 128 + b * 16, g * 128 + (b + 1) * 16)
                acc = jnp.dot(pbuf[at, :], vbuf[slot, g * 8 + b], preferred_element_type=F32) + own8[b * 16:(b + 1) * 16, :]
                msg[i, g, b * 12:(b + 1) * 12, :] = acc[:12, :]

        for g in range(6):
            if g < 4:
                scores(g)
            if 1 <= g <= 4:
                weights(g - 1)
            if g >= 2:
                sums(g - 2)

    def to_partner(i):
        return remote(msg.at[i, pl.ds(2 * co, 2)], part.at[i], s_p.at[i], r_p.at[i], partner)

    def to_across(r):
        return remote(send_y.at[r], recv_y.at[r], s_y.at[r], r_y.at[r], across)

    def ctx_copy(r):
        return remote(ctx_s.at[r], ctx_r.at[r], s_c.at[r], r_c.at[r], partner)

    def merge(i, dst):
        to_partner(i).wait_recv()
        for k in range(2):
            acc, top, total, _ = scaled_sum(msg[i, 2 * c + k], part[i, k])
            dst[k, :96, :] = acc
            line = lax.broadcasted_iota(jnp.int32, (8, 128), 0)
            dst[k, 96:104, :] = jnp.where(line == 0, top, total)

    def context(r):
        to_across(r).wait_recv()
        for k in range(2):
            acc, _, _, total = scaled_sum(comb_o[r, k], recv_y[r, k])
            ctx_t[...] = acc / total
            for h in range(12):
                ctx_s[r, k * 8:(k + 1) * 8, h * 128:(h + 1) * 128] = ctx_t[pl.ds(h, 8, stride=12), :]
        ctx_copy(r).start()

    def rs(j):
        return remote(rs_out.at[j], rs_in.at[j], s_rs.at[j], r_rs.at[j], ahead)

    def rs_end(j):
        return remote(rs_out.at[j], fin.at[y, c, j], s_rs.at[j], r_re.at[j], behind)

    def final(dst, send, recv, h, core, j):
        f = fin.at[h, core, j]
        return remote(f, f, send.at[j], recv.at[j], dst)

    def ag(j):
        return final(behind, s_ag, r_ag, y, c, j)

    def ag_end(j):
        return final(ahead, s_ae, r_ag, y, c, j)

    def fy(j):
        return final(across, s_fy, r_fy, y, c, j)

    def fy_in(j):
        return final(across, s_fy, r_fy, yo, c, j)

    def fd(j):
        return final(partner, s_fd, r_fd, y, c, j)

    def fd_in(j):
        return final(partner, s_fd, r_fd, y, co, j)

    def fe(j):
        return final(partner, s_fe, r_fe, yo, c, j)

    def fe_in(j):
        return final(partner, s_fe, r_fe, yo, co, j)

    def convert(h, core, j):
        at = pl.ds(pl.multiple_of(h * 128 + (j // QCH) * 32, 32), 32)
        obuf[at, pl.ds(pl.multiple_of(core * half + (j % QCH) * width, width), width)] = fin[h, core, j].astype(BF16)

    hops = u - 2 * (u // 3)
    lag = LAG * (2 - hops)
    lag_y = lag + LAG_Y
    start = 2 * QCH + HOP * hops
    hops_p = 3 - u - 2 * ((3 - u) // 3)
    start_p = 2 * QCH + HOP * hops_p + LAG * (2 - hops_p) + LAG_Y + 4

    def tick(t, carry):
        i, r6 = t // PER, t // QCH

        @pl.when((t < PER * STEPS) & (t % PER == 0))
        def _():
            attention(i)
            to_partner(i).start()

            @pl.when(i < STEPS - SLOTS)
            def _():
                k_copy(i + SLOTS).start()
                v_copy(i + SLOTS).start()

            @pl.when(i < QCH)
            def _():
                w_copy(i).start()

        @pl.when((t % QCH == PER + 1) & (t < NMSG))
        def _():
            merge(2 * r6, send_y.at[r6])
            to_across(r6).start()

        @pl.when((t % QCH == 1) & (t >= QCH) & (t < NMSG + QCH))
        def _():
            merge(2 * r6 - 1, comb_o.at[r6 - 1])

        @pl.when((t % QCH == QCH - 2) & (t >= QCH) & (t < NMSG + QCH))
        def _():
            context(r6 - 1)

        j = t - start

        @pl.when((j >= 0) & (j < NMSG))
        def _():
            r, q = j // QCH, j % QCH

            @pl.when(q == 0)
            def _():
                ctx_copy(r).wait_recv()
                lhs[c] = ctx_s[r].astype(BF16)
                lhs[co] = ctx_r[r].astype(BF16)

            @pl.when(r == 0)
            def _():
                w_copy(q).wait()

            @pl.when(j == 0)
            def _():
                x_copy.wait()

            prod[...] = jnp.dot(lhs[...].reshape(32, lhs.shape[2]), wbuf[q], preferred_element_type=F32)

            @pl.when(u == 0)
            def _():
                rs_out[j] = prod[...]
                rs(j).start()

            @pl.when(u == 3)
            def _():
                rs_out[j] = prod[...]
                rs_end(j).start()

            @pl.when(u == 1)
            def _():
                rs(j).wait_recv()
                rs_out[j] = rs_in[j] + prod[...]
                rs(j).start()

            @pl.when(u == 2)
            def _():
                x = xbuf[pl.ds(pl.multiple_of(r * 32, 32), 32), pl.ds(pl.multiple_of(q * width, width), width)]
                rs_end(j).wait_recv()
                rs(j).wait_recv()
                fin[y, c, j] = (rs_in[j] + prod[...]) + fin[y, c, j] + x.astype(F32)
                ag(j).start()
                ag_end(j).start()
                fy(j).start()
                fd(j).start()
                convert(y, c, j)

        ja = j - lag

        @pl.when((lag > 0) & (ja >= 0) & (ja < NMSG))
        def _():
            ag(ja).wait_recv()

            @pl.when(u == 1)
            def _():
                ag(ja).start()

            fy(ja).start()
            fd(ja).start()
            convert(y, c, ja)

        jy = j - lag_y

        @pl.when((jy >= 0) & (jy < NMSG))
        def _():
            fy_in(jy).wait_recv()
            fe(jy).start()
            convert(yo, c, jy)

        jp = t - start_p

        @pl.when((jp >= 0) & (jp < NMSG))
        def _():
            fd_in(jp).wait_recv()
            fe_in(jp).wait_recv()
            convert(y, co, jp)
            convert(yo, co, jp)

        return carry

    lax.fori_loop(0, 2 * QCH + 2 * LAG + LAG_Y + 4 + NMSG, tick, 0)

    def drain(j, carry):
        @pl.when(u < 2)
        def _():
            rs(j).wait_send()

        @pl.when(u == 3)
        def _():
            rs_end(j).wait_send()

        @pl.when((u == 1) | (u == 2))
        def _():
            ag(j).wait_send()

        @pl.when(u == 2)
        def _():
            ag_end(j).wait_send()

        fy(j).wait_send()
        fd(j).wait_send()
        fe(j).wait_send()
        return carry

    lax.fori_loop(0, NMSG, drain, 0)
    for slot in range(8):
        share(slot).wait_send()
    for i in range(STEPS):
        to_partner(i).wait_send()
    for r in range(RCH):
        to_across(r).wait_send()
        ctx_copy(r).wait_send()


def block(lengths, gain, bias, hidden, w_q, w_k, w_v, k_cache, v_cache, w_o):
    batch, positions, kv, head = k_cache.shape
    rows, width = hidden.shape
    depth = w_o.shape[0]
    half = width // 2
    cols = half // QCH
    freq = 10000.0 ** (-2.0 * np.arange(32, dtype=np.float32) / np.float32(64))
    freq = np.concatenate([freq, freq, np.zeros(64)]).astype(np.float32).reshape(1, 128)
    dma = pltpu.SemaphoreType.DMA
    part = pltpu.VMEM((RCH, 2, 104, 128), F32)
    cache = pltpu.VMEM((SLOTS, 32, positions * kv, head), BF16)
    table = pltpu.VMEM((rows, 128), F32)
    pair = pltpu.VMEM((rows * 2, 128), F32)
    shared = pltpu.VMEM((8, rows, 128), F32)
    line = pltpu.VMEM((8, width), F32)
    new = jax.ShapeDtypeStruct((rows * kv, head), BF16)
    pin = functools.partial(pltpu.with_memory_space_constraint, memory_space=pltpu.HBM)
    return pl.pallas_call(
        functools.partial(block_kernel, positions=positions, scale=head ** -0.5),
        out_shape=(jax.ShapeDtypeStruct((rows, width), BF16), new, new),
        in_specs=[HBM] * 11,
        out_specs=(VMEM, VMEM, VMEM),
        scratch_shapes=[pltpu.SMEM((rows // 128, 128), jnp.int32), pltpu.VMEM((rows // 128, 128), jnp.int32), pltpu.VMEM((1, 128), F32),
                        pltpu.VMEM((width // 128, 128), BF16), pltpu.VMEM((width // 128, 128), BF16), dma((5,)),
                        pltpu.VMEM((rows, width), BF16), pltpu.VMEM((rows, 512), F32), pltpu.VMEM((rows * 16, 128), F32),
                        pair, pair, shared, shared, table, table, line, line,
                        dma((4,)), dma((4,)), dma((3, 4)), dma((8,)), dma((8,)),
                        cache, cache,
                        pltpu.VMEM((512, positions * kv), F32), pltpu.VMEM((512, 16), F32),
                        pltpu.VMEM((512, positions * kv), BF16), pltpu.VMEM((512, 128), F32),
                        pltpu.VMEM((STEPS, 4, 104, 128), F32), pltpu.VMEM((STEPS, 2, 104, 128), F32),
                        part, part, part,
                        pltpu.VMEM((96, 128), F32),
                        pltpu.VMEM((RCH, 16, depth), F32), pltpu.VMEM((RCH, 16, depth), F32),
                        pltpu.VMEM((2, 16, depth), BF16),
                        pltpu.VMEM((8, depth, cols), BF16),
                        pltpu.VMEM((rows // 2, half), BF16),
                        pltpu.VMEM((32, cols), F32),
                        pltpu.VMEM((NMSG, 32, cols), F32), pltpu.VMEM((NMSG, 32, cols), F32),
                        pltpu.VMEM((2, 2, NMSG, 32, cols), F32),
                        dma((SLOTS,)), dma((SLOTS,)), dma((STEPS,)), dma((STEPS,)), dma((RCH,)), dma((RCH,)),
                        dma((RCH,)), dma((RCH,)), dma((QCH,)), dma] + [dma((NMSG,))] * 12,
        compiler_params=pltpu.CompilerParams(collective_id=0, has_side_effects=True, vmem_limit_bytes=BLOCK_LIMIT),
        name="block",
    )(pin(lengths.reshape(rows // 128, 128)), pin(jnp.asarray(freq)), pin(gain.reshape(width // 128, 128)), pin(bias.reshape(width // 128, 128)),
      hidden, w_q, w_k, w_v, k_cache.reshape(batch, positions * kv, head), v_cache.reshape(batch, positions * kv, head), w_o)


def emit_kernel(*refs):
    n = len(refs) // 2
    copies = [pltpu.make_async_copy(refs[i], refs[n + i], refs[2 * n].at[i]) for i in range(n)]
    for copy in copies:
        copy.start()
    for copy in copies:
        copy.wait()


def emit(*values):
    n = len(values)
    return pl.pallas_call(
        emit_kernel,
        out_shape=tuple(jax.ShapeDtypeStruct(v.shape, v.dtype) for v in values),
        in_specs=[VMEM] * n, out_specs=(HBM,) * n,
        scratch_shapes=[pltpu.SemaphoreType.DMA((n,))],
        compiler_params=pltpu.CompilerParams(vmem_limit_bytes=4 * 1024 * 1024),
        name="emit",
    )(*values)


def solution(mesh):
    def local_step(hidden, ln_gain, ln_bias, w_q, w_k, w_v, w_o, k_cache, v_cache, lengths):
        batch, _, kv, head = k_cache.shape
        out, k_new, v_new = emit(*block(lengths, ln_gain, ln_bias, hidden, w_q, w_k, w_v, k_cache, v_cache, w_o))
        return out, k_new.reshape(batch, kv, head), v_new.reshape(batch, kv, head)

    row_spec = P('dp', None)
    cache_spec = P('dp', 'sp', 'tp', None)
    head_spec = P('dp', 'tp', None)
    return jax.shard_map(local_step, mesh=mesh, in_specs=(row_spec, P(None), P(None), P(None, 'tp'), P(None, 'tp'), P(None, 'tp'), P('tp', None), cache_spec, cache_spec, P('dp')), out_specs=(row_spec, head_spec, head_spec), check_vma=False)
```

```python
import functools

import jax
import jax.numpy as jnp
import numpy as np
from jax import lax
from jax.experimental import pallas as pl
from jax.experimental.pallas import tpu as pltpu
from jax.sharding import PartitionSpec as P

F32 = jnp.float32
BF16 = jnp.bfloat16
MESH = pl.DeviceIdType.MESH
NEG = -0.7 * float(np.finfo(np.float32).max)
BLOCK_LIMIT = 49 * 1024 * 1024
HBM = pl.BlockSpec(memory_space=pltpu.HBM)
VMEM = pl.BlockSpec(memory_space=pltpu.VMEM)


RCH = 4
QCH = 6
NMSG = RCH * QCH
PER = QCH // 2
STEPS = 2 * RCH
HOP = 5
LAG = 6
LAG_Y = 6
SLOTS = 3


def scaled_sum(a, b):
    m_a, l_a, m_b, l_b = a[96:97, :], a[97:98, :], b[96:97, :], b[97:98, :]
    top = jnp.maximum(m_a, m_b)
    f_a, f_b = jnp.exp(m_a - top), jnp.exp(m_b - top)
    total = l_a * f_a + l_b * f_b
    r = lax.broadcasted_iota(jnp.int32, (128, 128), 0)
    turned = jnp.transpose(jnp.where(r == 0, f_a, jnp.where(r == 1, f_b, total)))
    acc = a[:96, :] * turned[:96, 0:1] + b[:96, :] * turned[:96, 1:2]
    return acc, top, total, turned[:96, 2:3]


def block_kernel(len_hbm, freq_hbm, gain_hbm, bias_hbm, x_hbm, wq_hbm, wk_hbm, wv_hbm, k_hbm, v_hbm, w_hbm,
                 obuf, kn_ref, vn_ref,
                 len_ref, len_rows, freq_ref, gain_ref, bias_ref, s_in,
                 hbuf, acc_ref, q_ref, kf, vf, xs, xr, cosb, sinb, gainb, biasb, s_h, s_q, s_g, s_xs, r_xs,
                 kbuf, vbuf, sbuf, self_buf, pbuf, stat, msg, part, send_y, recv_y, comb_o, ctx_t, ctx_s, ctx_r,
                 lhs, wbuf, xbuf, prod, rs_in, rs_out, fin,
                 s_k, s_v, s_p, r_p, s_y, r_y, s_c, r_c, s_w, s_x,
                 s_rs, r_rs, r_re, s_ag, r_ag, s_ae, s_fy, r_fy, s_fd, r_fd, s_fe, r_fe, *, positions, scale):
    d, z, s = lax.axis_index("dp"), lax.axis_index("tp"), lax.axis_index("sp")
    y, c = s // 2, s % 2
    yo, co = 1 - y, 1 - c
    u = c * z + co * (3 - z)
    partner, across = (d, z, 2 * y + co), (d, z, 2 * yo + c)
    ahead, behind = (d, z + 2 * c - 1, s), (d, z - 2 * c + 1, s)
    width = wbuf.shape[2]
    half = QCH * width

    def remote(src, dst, send, recv, dev):
        return pltpu.make_async_remote_copy(src_ref=src, dst_ref=dst, send_sem=send, recv_sem=recv,
                                            device_id=dev, device_id_type=MESH)

    barrier = pltpu.get_barrier_semaphore()
    pl.semaphore_signal(barrier, inc=1, device_id=partner, device_id_type=MESH)
    pl.semaphore_signal(barrier, inc=1, device_id=across, device_id_type=MESH)

    @pl.when(u < 3)
    def _():
        pl.semaphore_signal(barrier, inc=1, device_id=ahead, device_id_type=MESH)

    @pl.when(u > 0)
    def _():
        pl.semaphore_signal(barrier, inc=1, device_id=behind, device_id_type=MESH)

    def first_row(i):
        return 128 * ((i % 2) * y + (1 - i % 2) * yo) + 32 * (i // 2)

    def k_copy(i):
        return pltpu.make_async_copy(k_hbm.at[pl.ds(first_row(i), 32)], kbuf.at[i % SLOTS], s_k.at[i % SLOTS])

    def v_copy(i):
        return pltpu.make_async_copy(v_hbm.at[pl.ds(first_row(i), 32)], vbuf.at[i % SLOTS], s_v.at[i % SLOTS])

    def w_copy(q):
        return pltpu.make_async_copy(w_hbm.at[:, pl.ds(c * half + q * width, width)], wbuf.at[q], s_w.at[q])

    x_copy = pltpu.make_async_copy(x_hbm.at[pl.ds(y * 128, 128), pl.ds(c * half, half)], xbuf, s_x)

    rows, model = hbuf.shape
    tiles = model // 128
    depth = wbuf.shape[1]

    def h_copy(i):
        at = pl.ds(i * 64, 64)
        return pltpu.make_async_copy(x_hbm.at[at], obuf.at[at], s_h.at[i])

    inputs = ((len_hbm, len_ref), (len_hbm, len_rows), (freq_hbm, freq_ref), (gain_hbm, gain_ref), (bias_hbm, bias_ref))
    small = [pltpu.make_async_copy(src, dst, s_in.at[n]) for n, (src, dst) in enumerate(inputs)]
    for copy in small:
        copy.start()
    for i in range(rows // 64):
        h_copy(i).start()

    def q_copy(n):
        return pltpu.make_async_copy(wq_hbm.at[pl.ds(n * depth, depth), pl.ds(c * 768, 512)], wbuf.at[n], s_q.at[n])

    def g_copies(n):
        at = pl.ds(n * depth, depth)
        return [pltpu.make_async_copy(wq_hbm.at[at, pl.ds(c * 768 + 512, 256)], wbuf.at[4 + n, :, pl.ds(0, 256)], s_g.at[0, n]),
                pltpu.make_async_copy(wk_hbm.at[at, pl.ds(c * 128, 128)], wbuf.at[4 + n, :, pl.ds(256, 128)], s_g.at[1, n]),
                pltpu.make_async_copy(wv_hbm.at[at, pl.ds(c * 128, 128)], wbuf.at[4 + n, :, pl.ds(384, 128)], s_g.at[2, n])]

    def share(slot):
        return remote(xs.at[slot], xr.at[slot], s_xs.at[slot], r_xs.at[slot], partner)

    for h in range(12, 16):
        q_ref[pl.ds(h, rows, stride=16), :] = jnp.zeros((rows, 128), F32)
    for copy in small:
        copy.wait()
    for k in range(tiles):
        gainb[:, k * 128:(k + 1) * 128] = jnp.broadcast_to(1.0 + gain_ref[k:k + 1, :].astype(F32), (8, 128))
        biasb[:, k * 128:(k + 1) * 128] = jnp.broadcast_to(bias_ref[k:k + 1, :].astype(F32), (8, 128))
    for i in range(rows // 128):
        angle = jnp.transpose(jnp.broadcast_to(len_rows[i:i + 1, :].astype(F32), (128, 128))) * freq_ref[...]
        cosb[i * 128:(i + 1) * 128, :] = jnp.cos(angle)
        sinb[i * 128:(i + 1) * 128, :] = jnp.sin(angle)

    def norm(i, carry):
        h_copy(i).wait()

        @pl.when(i < 2)
        def _():
            q_copy(2 * i).start()
            q_copy(2 * i + 1).start()

        @pl.when(i >= 2)
        def _():
            for copy in g_copies(2 * i - 4) + g_copies(2 * i - 3):
                copy.start()

        ats = [pl.ds(pl.multiple_of(i * 64 + j * 16, 16), 16) for j in range(4)]
        lanes = [slice(k * 128, (k + 1) * 128) for k in range(tiles)]
        means, scales = [], []
        for at in ats:
            accs = [obuf[at, lanes[k]].astype(F32) for k in range(2)]
            for k in range(2, tiles):
                accs[k % 2] = accs[k % 2] + obuf[at, lanes[k]].astype(F32)
            mean = jnp.sum(accs[0] + accs[1], axis=-1, keepdims=True) * (1.0 / model)
            means.append(jnp.broadcast_to(mean, (16, 128)))
        for at, mean in zip(ats, means):
            accs = [jnp.zeros((16, 128), F32) for _ in range(2)]
            for k in range(tiles):
                centred = obuf[at, lanes[k]].astype(F32) - mean
                accs[k % 2] = accs[k % 2] + centred * centred
            var = jnp.sum(accs[0] + accs[1], axis=-1, keepdims=True) * (1.0 / model)
            scales.append(jnp.broadcast_to(lax.rsqrt(var + 1e-5), (16, 128)))
        for k in range(tiles):
            gain = jnp.concatenate([gainb[:, lanes[k]]] * 2, axis=0)
            bias = jnp.concatenate([biasb[:, lanes[k]]] * 2, axis=0)
            for at, mean, factor in zip(ats, means, scales):
                hbuf[at, lanes[k]] = ((obuf[at, lanes[k]].astype(F32) - mean) * factor * gain + bias).astype(BF16)
        return carry

    lax.fori_loop(0, rows // 64, norm, 0)
    for i in range(SLOTS):
        k_copy(i).start()
        v_copy(i).start()
    x_copy.start()

    lane_r = lax.broadcasted_iota(jnp.int32, (rows, 128), 1)

    def rotate(v):
        other = jnp.where(lane_r < 32, -pltpu.roll(v, 96, 1), pltpu.roll(v, 32, 1))
        return jnp.where(lane_r < 64, v * cosb[...] + other * sinb[...], v)

    def spread_out(slot, core, v):
        if slot < 6:
            q_ref[pl.ds(6 * core + slot, rows, stride=16), :] = v
        else:
            dst = kf if slot == 6 else vf
            dst[pl.ds(core, rows, stride=2), :] = v

    for g in range(2):
        for n in range(4):
            for copy in ([q_copy(n)] if g == 0 else g_copies(n)):
                copy.wait()
        if g == 1:
            for slot in range(4):
                spread_out(slot, c, xs[slot])
        parts = [jnp.dot(hbuf[:, n * depth:(n + 1) * depth], wbuf[4 * g + n], preferred_element_type=F32) for n in range(4)]
        acc_ref[...] = (parts[0] + parts[1]) + (parts[2] + parts[3])
        if g == 0:
            pl.semaphore_wait(barrier, 2 + (z + 2) // 3 + (5 - z) // 3)
        for slot in range(4 * g, 4 * g + 4):
            v = acc_ref[:, (slot % 4) * 128:(slot % 4 + 1) * 128]
            xs[slot] = rotate(v) if slot < 7 else v
            share(slot).start()
    for slot in range(4, 8):
        spread_out(slot, c, xs[slot])
    for slot in range(8):
        share(slot).wait_recv()
        spread_out(slot, co, xr[slot])
    kn_ref[...] = kf[...].astype(BF16)
    vn_ref[...] = vf[...].astype(BF16)

    first = s * positions
    col = lax.broadcasted_iota(jnp.int32, (16, 2 * positions), 1)
    row = lax.broadcasted_iota(jnp.int32, (16, 2 * positions), 0)
    place = jnp.where(lax.rem(col, 2) == jnp.where(row >= 6, 1, 0), first + col // 2, 1 << 30)
    pick_row = lax.broadcasted_iota(jnp.int32, (128, 16), 0)
    pick_col = lax.broadcasted_iota(jnp.int32, (128, 16), 1)
    pick = pick_col == 2 * (pick_row // 16) + jnp.where(lax.rem(pick_row, 16) >= 6, 1, 0)
    nt = (((1,), (1,)), ((), ()))

    def attention(i):
        k_copy(i).wait()
        v_copy(i).wait()
        slot = i % SLOTS
        base = first_row(i)
        spread = jnp.where(pick, 1.0, 0.0).astype(BF16)
        lane = lax.broadcasted_iota(jnp.int32, (128, 128), 1)
        begin = lax.broadcasted_iota(jnp.int32, (16, 16), 0) * 0 + first
        own_w = [None] * 4

        def scores(g):
            q8 = q_ref[pl.ds(pl.multiple_of(base * 16 + g * 128, 128), 128), :].astype(BF16)
            kn = kn_ref[pl.ds(pl.multiple_of(base * 2 + g * 16, 16), 16), :]
            self8 = lax.dot_general(q8, kn, nt, preferred_element_type=F32) * scale
            self8 = jnp.where(pick, self8, NEG)
            for b in range(8):
                at = slice(g * 128 + b * 16, g * 128 + (b + 1) * 16)
                length = len_ref[base // 128, base % 128 + g * 8 + b]
                owner = (length >= begin) & (length < begin + positions)
                sc = lax.dot_general(q8[b * 16:(b + 1) * 16, :], kbuf[slot, g * 8 + b], nt, preferred_element_type=F32) * scale
                sbuf[at, :] = jnp.where(place < length, sc, NEG)
                self_buf[at, :] = jnp.where(owner, self8[b * 16:(b + 1) * 16, :], NEG)

        def weights(g):
            at = slice(g * 128, (g + 1) * 128)
            sc = sbuf[at, :]
            own = jnp.max(self_buf[at, :], axis=1, keepdims=True)
            top = jnp.maximum(jnp.max(sc, axis=1, keepdims=True), own)
            w = jnp.exp(sc - top)
            own_w[g] = jnp.exp(own - top)
            total = jnp.sum(w, axis=1, keepdims=True) + own_w[g]
            pbuf[at, :] = w.astype(BF16)
            stat[at, :] = jnp.where(lane == 0, top, total)

        def sums(g):
            vn = vn_ref[pl.ds(pl.multiple_of(base * 2 + g * 16, 16), 16), :]
            own8 = own_w[g] * jnp.dot(spread, vn, preferred_element_type=F32)
            turned = jnp.transpose(stat[g * 128:(g + 1) * 128, :])[:8, :]
            msg[i, g, 96:104, :] = jnp.concatenate([turned[:, b * 16:b * 16 + 12] for b in range(8)] + [jnp.zeros((8, 32), F32)], axis=1)
            for b in range(8):
                at = slice(g * 128 + b * 16, g * 128 + (b + 1) * 16)
                acc = jnp.dot(pbuf[at, :], vbuf[slot, g * 8 + b], preferred_element_type=F32) + own8[b * 16:(b + 1) * 16, :]
                msg[i, g, b * 12:(b + 1) * 12, :] = acc[:12, :]

        for g in range(6):
            if g < 4:
                scores(g)
            if 1 <= g <= 4:
                weights(g - 1)
            if g >= 2:
                sums(g - 2)

    def to_partner(i):
        return remote(msg.at[i, pl.ds(2 * co, 2)], part.at[i], s_p.at[i], r_p.at[i], partner)

    def to_across(r):
        return remote(send_y.at[r], recv_y.at[r], s_y.at[r], r_y.at[r], across)

    def ctx_copy(r):
        return remote(ctx_s.at[r], ctx_r.at[r], s_c.at[r], r_c.at[r], partner)

    def merge(i, dst):
        to_partner(i).wait_recv()
        for k in range(2):
            acc, top, total, _ = scaled_sum(msg[i, 2 * c + k], part[i, k])
            dst[k, :96, :] = acc
            line = lax.broadcasted_iota(jnp.int32, (8, 128), 0)
            dst[k, 96:104, :] = jnp.where(line == 0, top, total)

    def context(r):
        to_across(r).wait_recv()
        for k in range(2):
            acc, _, _, total = scaled_sum(comb_o[r, k], recv_y[r, k])
            ctx_t[...] = acc / total
            for h in range(12):
                ctx_s[r, k * 8:(k + 1) * 8, h * 128:(h + 1) * 128] = ctx_t[pl.ds(h, 8, stride=12), :]
        ctx_copy(r).start()

    def rs(j):
        return remote(rs_out.at[j], rs_in.at[j], s_rs.at[j], r_rs.at[j], ahead)

    def rs_end(j):
        return remote(rs_out.at[j], fin.at[y, c, j], s_rs.at[j], r_re.at[j], behind)

    def final(dst, send, recv, h, core, j):
        f = fin.at[h, core, j]
        return remote(f, f, send.at[j], recv.at[j], dst)

    def ag(j):
        return final(behind, s_ag, r_ag, y, c, j)

    def ag_end(j):
        return final(ahead, s_ae, r_ag, y, c, j)

    def fy(j):
        return final(across, s_fy, r_fy, y, c, j)

    def fy_in(j):
        return final(across, s_fy, r_fy, yo, c, j)

    def fd(j):
        return final(partner, s_fd, r_fd, y, c, j)

    def fd_in(j):
        return final(partner, s_fd, r_fd, y, co, j)

    def fe(j):
        return final(partner, s_fe, r_fe, yo, c, j)

    def fe_in(j):
        return final(partner, s_fe, r_fe, yo, co, j)

    def convert(h, core, j):
        at = pl.ds(pl.multiple_of(h * 128 + (j // QCH) * 32, 32), 32)
        obuf[at, pl.ds(pl.multiple_of(core * half + (j % QCH) * width, width), width)] = fin[h, core, j].astype(BF16)

    hops = u - 2 * (u // 3)
    lag = LAG * (2 - hops)
    lag_y = lag + LAG_Y
    start = 2 * QCH + HOP * hops
    hops_p = 3 - u - 2 * ((3 - u) // 3)
    start_p = 2 * QCH + HOP * hops_p + LAG * (2 - hops_p) + LAG_Y + 4

    def tick(t, carry):
        i, r6 = t // PER, t // QCH

        @pl.when((t < PER * STEPS) & (t % PER == 0))
        def _():
            attention(i)
            to_partner(i).start()

            @pl.when(i < STEPS - SLOTS)
            def _():
                k_copy(i + SLOTS).start()
                v_copy(i + SLOTS).start()

            @pl.when((i >= 2) & (i < 5))
            def _():
                w_copy(2 * i - 4).start()
                w_copy(2 * i - 3).start()

        @pl.when((t % QCH == PER + 1) & (t < NMSG))
        def _():
            merge(2 * r6, send_y.at[r6])
            to_across(r6).start()

        @pl.when((t % QCH == 1) & (t >= QCH) & (t < NMSG + QCH))
        def _():
            merge(2 * r6 - 1, comb_o.at[r6 - 1])

        @pl.when((t % QCH == QCH - 2) & (t >= QCH) & (t < NMSG + QCH))
        def _():
            context(r6 - 1)

        j = t - start

        @pl.when((j >= 0) & (j < NMSG))
        def _():
            r, q = j // QCH, j % QCH

            @pl.when(q == 0)
            def _():
                ctx_copy(r).wait_recv()
                lhs[c] = ctx_s[r].astype(BF16)
                lhs[co] = ctx_r[r].astype(BF16)

            @pl.when(r == 0)
            def _():
                w_copy(q).wait()

            @pl.when(j == 0)
            def _():
                x_copy.wait()

            prod[...] = jnp.dot(lhs[...].reshape(32, lhs.shape[2]), wbuf[q], preferred_element_type=F32)

            @pl.when(u == 0)
            def _():
                rs_out[j] = prod[...]
                rs(j).start()

            @pl.when(u == 3)
            def _():
                rs_out[j] = prod[...]
                rs_end(j).start()

            @pl.when(u == 1)
            def _():
                rs(j).wait_recv()
                rs_out[j] = rs_in[j] + prod[...]
                rs(j).start()

            @pl.when(u == 2)
            def _():
                x = xbuf[pl.ds(pl.multiple_of(r * 32, 32), 32), pl.ds(pl.multiple_of(q * width, width), width)]
                rs_end(j).wait_recv()
                rs(j).wait_recv()
                fin[y, c, j] = (rs_in[j] + prod[...]) + fin[y, c, j] + x.astype(F32)
                ag(j).start()
                ag_end(j).start()
                fy(j).start()
                fd(j).start()
                convert(y, c, j)

        ja = j - lag

        @pl.when((lag > 0) & (ja >= 0) & (ja < NMSG))
        def _():
            ag(ja).wait_recv()

            @pl.when(u == 1)
            def _():
                ag(ja).start()

            fy(ja).start()
            fd(ja).start()
            convert(y, c, ja)

        jy = j - lag_y

        @pl.when((jy >= 0) & (jy < NMSG))
        def _():
            fy_in(jy).wait_recv()
            fe(jy).start()
            convert(yo, c, jy)

        jp = t - start_p

        @pl.when((jp >= 0) & (jp < NMSG))
        def _():
            fd_in(jp).wait_recv()
            fe_in(jp).wait_recv()
            convert(y, co, jp)
            convert(yo, co, jp)

        return carry

    lax.fori_loop(0, 2 * QCH + 2 * LAG + LAG_Y + 4 + NMSG, tick, 0)

    def drain(j, carry):
        @pl.when(u < 2)
        def _():
            rs(j).wait_send()

        @pl.when(u == 3)
        def _():
            rs_end(j).wait_send()

        @pl.when((u == 1) | (u == 2))
        def _():
            ag(j).wait_send()

        @pl.when(u == 2)
        def _():
            ag_end(j).wait_send()

        fy(j).wait_send()
        fd(j).wait_send()
        fe(j).wait_send()
        return carry

    lax.fori_loop(0, NMSG, drain, 0)
    for slot in range(8):
        share(slot).wait_send()
    for i in range(STEPS):
        to_partner(i).wait_send()
    for r in range(RCH):
        to_across(r).wait_send()
        ctx_copy(r).wait_send()


def block(lengths, gain, bias, hidden, w_q, w_k, w_v, k_cache, v_cache, w_o):
    batch, positions, kv, head = k_cache.shape
    rows, width = hidden.shape
    depth = w_o.shape[0]
    half = width // 2
    cols = half // QCH
    freq = 10000.0 ** (-2.0 * np.arange(32, dtype=np.float32) / np.float32(64))
    freq = np.concatenate([freq, freq, np.zeros(64)]).astype(np.float32).reshape(1, 128)
    dma = pltpu.SemaphoreType.DMA
    part = pltpu.VMEM((RCH, 2, 104, 128), F32)
    cache = pltpu.VMEM((SLOTS, 32, positions * kv, head), BF16)
    table = pltpu.VMEM((rows, 128), F32)
    pair = pltpu.VMEM((rows * 2, 128), F32)
    shared = pltpu.VMEM((8, rows, 128), F32)
    line = pltpu.VMEM((8, width), F32)
    new = jax.ShapeDtypeStruct((rows * kv, head), BF16)
    pin = functools.partial(pltpu.with_memory_space_constraint, memory_space=pltpu.HBM)
    return pl.pallas_call(
        functools.partial(block_kernel, positions=positions, scale=head ** -0.5),
        out_shape=(jax.ShapeDtypeStruct((rows, width), BF16), new, new),
        in_specs=[HBM] * 11,
        out_specs=(VMEM, VMEM, VMEM),
        scratch_shapes=[pltpu.SMEM((rows // 128, 128), jnp.int32), pltpu.VMEM((rows // 128, 128), jnp.int32), pltpu.VMEM((1, 128), F32),
                        pltpu.VMEM((width // 128, 128), BF16), pltpu.VMEM((width // 128, 128), BF16), dma((5,)),
                        pltpu.VMEM((rows, width), BF16), pltpu.VMEM((rows, 512), F32), pltpu.VMEM((rows * 16, 128), F32),
                        pair, pair, shared, shared, table, table, line, line,
                        dma((4,)), dma((4,)), dma((3, 4)), dma((8,)), dma((8,)),
                        cache, cache,
                        pltpu.VMEM((512, positions * kv), F32), pltpu.VMEM((512, 16), F32),
                        pltpu.VMEM((512, positions * kv), BF16), pltpu.VMEM((512, 128), F32),
                        pltpu.VMEM((STEPS, 4, 104, 128), F32), pltpu.VMEM((STEPS, 2, 104, 128), F32),
                        part, part, part,
                        pltpu.VMEM((96, 128), F32),
                        pltpu.VMEM((RCH, 16, depth), F32), pltpu.VMEM((RCH, 16, depth), F32),
                        pltpu.VMEM((2, 16, depth), BF16),
                        pltpu.VMEM((8, depth, cols), BF16),
                        pltpu.VMEM((rows // 2, half), BF16),
                        pltpu.VMEM((32, cols), F32),
                        pltpu.VMEM((NMSG, 32, cols), F32), pltpu.VMEM((NMSG, 32, cols), F32),
                        pltpu.VMEM((2, 2, NMSG, 32, cols), F32),
                        dma((SLOTS,)), dma((SLOTS,)), dma((STEPS,)), dma((STEPS,)), dma((RCH,)), dma((RCH,)),
                        dma((RCH,)), dma((RCH,)), dma((QCH,)), dma] + [dma((NMSG,))] * 12,
        compiler_params=pltpu.CompilerParams(collective_id=0, has_side_effects=True, vmem_limit_bytes=BLOCK_LIMIT),
        name="block",
    )(pin(lengths.reshape(rows // 128, 128)), pin(jnp.asarray(freq)), pin(gain.reshape(width // 128, 128)), pin(bias.reshape(width // 128, 128)),
      hidden, w_q, w_k, w_v, k_cache.reshape(batch, positions * kv, head), v_cache.reshape(batch, positions * kv, head), w_o)


def emit_kernel(*refs):
    n = len(refs) // 2
    copies = [pltpu.make_async_copy(refs[i], refs[n + i], refs[2 * n].at[i]) for i in range(n)]
    for copy in copies:
        copy.start()
    for copy in copies:
        copy.wait()


def emit(*values):
    n = len(values)
    return pl.pallas_call(
        emit_kernel,
        out_shape=tuple(jax.ShapeDtypeStruct(v.shape, v.dtype) for v in values),
        in_specs=[VMEM] * n, out_specs=(HBM,) * n,
        scratch_shapes=[pltpu.SemaphoreType.DMA((n,))],
        compiler_params=pltpu.CompilerParams(vmem_limit_bytes=4 * 1024 * 1024),
        name="emit",
    )(*values)


def solution(mesh):
    def local_step(hidden, ln_gain, ln_bias, w_q, w_k, w_v, w_o, k_cache, v_cache, lengths):
        batch, _, kv, head = k_cache.shape
        out, k_new, v_new = emit(*block(lengths, ln_gain, ln_bias, hidden, w_q, w_k, w_v, k_cache, v_cache, w_o))
        return out, k_new.reshape(batch, kv, head), v_new.reshape(batch, kv, head)

    row_spec = P('dp', None)
    cache_spec = P('dp', 'sp', 'tp', None)
    head_spec = P('dp', 'tp', None)
    return jax.shard_map(local_step, mesh=mesh, in_specs=(row_spec, P(None), P(None), P(None, 'tp'), P(None, 'tp'), P(None, 'tp'), P('tp', None), cache_spec, cache_spec, P('dp')), out_specs=(row_spec, head_spec, head_spec), check_vma=False)
```

```python
import functools

import jax
import jax.numpy as jnp
import numpy as np
from jax import lax
from jax.experimental import pallas as pl
from jax.experimental.pallas import tpu as pltpu
from jax.sharding import PartitionSpec as P

F32 = jnp.float32
BF16 = jnp.bfloat16
MESH = pl.DeviceIdType.MESH
NEG = -0.7 * float(np.finfo(np.float32).max)
BLOCK_LIMIT = 49 * 1024 * 1024
HBM = pl.BlockSpec(memory_space=pltpu.HBM)
VMEM = pl.BlockSpec(memory_space=pltpu.VMEM)


RCH = 4
QCH = 6
NMSG = RCH * QCH
PER = QCH // 2
STEPS = 2 * RCH
HOP = 4
LAG = 6
LAG_Y = 6
SLOTS = 3


def scaled_sum(a, b):
    m_a, l_a, m_b, l_b = a[96:97, :], a[97:98, :], b[96:97, :], b[97:98, :]
    top = jnp.maximum(m_a, m_b)
    f_a, f_b = jnp.exp(m_a - top), jnp.exp(m_b - top)
    total = l_a * f_a + l_b * f_b
    r = lax.broadcasted_iota(jnp.int32, (128, 128), 0)
    turned = jnp.transpose(jnp.where(r == 0, f_a, jnp.where(r == 1, f_b, total)))
    acc = a[:96, :] * turned[:96, 0:1] + b[:96, :] * turned[:96, 1:2]
    return acc, top, total, turned[:96, 2:3]


def block_kernel(len_hbm, freq_hbm, gain_hbm, bias_hbm, x_hbm, wq_hbm, wk_hbm, wv_hbm, k_hbm, v_hbm, w_hbm,
                 obuf, kn_ref, vn_ref,
                 len_ref, len_rows, freq_ref, gain_ref, bias_ref, s_in,
                 hbuf, acc_ref, q_ref, kf, vf, xs, xr, cosb, sinb, gainb, biasb, s_h, s_q, s_g, s_xs, r_xs,
                 kbuf, vbuf, sbuf, self_buf, pbuf, stat, msg, part, send_y, recv_y, comb_o, ctx_t, ctx_s, ctx_r,
                 lhs, wbuf, xbuf, prod, rs_in, rs_out, fin,
                 s_k, s_v, s_p, r_p, s_y, r_y, s_c, r_c, s_w, s_x,
                 s_rs, r_rs, r_re, s_ag, r_ag, s_ae, s_fy, r_fy, s_fd, r_fd, s_fe, r_fe, *, positions, scale):
    d, z, s = lax.axis_index("dp"), lax.axis_index("tp"), lax.axis_index("sp")
    y, c = s // 2, s % 2
    yo, co = 1 - y, 1 - c
    u = c * z + co * (3 - z)
    partner, across = (d, z, 2 * y + co), (d, z, 2 * yo + c)
    ahead, behind = (d, z + 2 * c - 1, s), (d, z - 2 * c + 1, s)
    width = wbuf.shape[2]
    half = QCH * width

    def remote(src, dst, send, recv, dev):
        return pltpu.make_async_remote_copy(src_ref=src, dst_ref=dst, send_sem=send, recv_sem=recv,
                                            device_id=dev, device_id_type=MESH)

    barrier = pltpu.get_barrier_semaphore()
    pl.semaphore_signal(barrier, inc=1, device_id=partner, device_id_type=MESH)
    pl.semaphore_signal(barrier, inc=1, device_id=across, device_id_type=MESH)

    @pl.when(u < 3)
    def _():
        pl.semaphore_signal(barrier, inc=1, device_id=ahead, device_id_type=MESH)

    @pl.when(u > 0)
    def _():
        pl.semaphore_signal(barrier, inc=1, device_id=behind, device_id_type=MESH)

    def first_row(i):
        return 128 * ((i % 2) * y + (1 - i % 2) * yo) + 32 * (i // 2)

    def k_copy(i):
        return pltpu.make_async_copy(k_hbm.at[pl.ds(first_row(i), 32)], kbuf.at[i % SLOTS], s_k.at[i % SLOTS])

    def v_copy(i):
        return pltpu.make_async_copy(v_hbm.at[pl.ds(first_row(i), 32)], vbuf.at[i % SLOTS], s_v.at[i % SLOTS])

    def w_copy(q):
        return pltpu.make_async_copy(w_hbm.at[:, pl.ds(c * half + q * width, width)], wbuf.at[q], s_w.at[q])

    x_copy = pltpu.make_async_copy(x_hbm.at[pl.ds(y * 128, 128), pl.ds(c * half, half)], xbuf, s_x)

    rows, model = hbuf.shape
    tiles = model // 128
    depth = wbuf.shape[1]

    def h_copy(i):
        at = pl.ds(i * 64, 64)
        return pltpu.make_async_copy(x_hbm.at[at], obuf.at[at], s_h.at[i])

    inputs = ((len_hbm, len_ref), (len_hbm, len_rows), (freq_hbm, freq_ref), (gain_hbm, gain_ref), (bias_hbm, bias_ref))
    small = [pltpu.make_async_copy(src, dst, s_in.at[n]) for n, (src, dst) in enumerate(inputs)]
    for copy in small:
        copy.start()
    for i in range(rows // 64):
        h_copy(i).start()

    def q_copy(n):
        return pltpu.make_async_copy(wq_hbm.at[pl.ds(n * depth, depth), pl.ds(c * 768, 512)], wbuf.at[n], s_q.at[n])

    def g_copies(n):
        at = pl.ds(n * depth, depth)
        return [pltpu.make_async_copy(wq_hbm.at[at, pl.ds(c * 768 + 512, 256)], wbuf.at[4 + n, :, pl.ds(0, 256)], s_g.at[0, n]),
                pltpu.make_async_copy(wk_hbm.at[at, pl.ds(c * 128, 128)], wbuf.at[4 + n, :, pl.ds(256, 128)], s_g.at[1, n]),
                pltpu.make_async_copy(wv_hbm.at[at, pl.ds(c * 128, 128)], wbuf.at[4 + n, :, pl.ds(384, 128)], s_g.at[2, n])]

    def share(slot):
        return remote(xs.at[slot], xr.at[slot], s_xs.at[slot], r_xs.at[slot], partner)

    for copy in small:
        copy.wait()
    for k in range(tiles):
        gainb[:, k * 128:(k + 1) * 128] = jnp.broadcast_to(1.0 + gain_ref[k:k + 1, :].astype(F32), (8, 128))
        biasb[:, k * 128:(k + 1) * 128] = jnp.broadcast_to(bias_ref[k:k + 1, :].astype(F32), (8, 128))
    for i in range(rows // 128):
        angle = jnp.transpose(jnp.broadcast_to(len_rows[i:i + 1, :].astype(F32), (128, 128))) * freq_ref[...]
        cosb[i * 128:(i + 1) * 128, :] = jnp.cos(angle)
        sinb[i * 128:(i + 1) * 128, :] = jnp.sin(angle)

    def norm(i, carry):
        h_copy(i).wait()

        @pl.when(i < 2)
        def _():
            q_copy(2 * i).start()
            q_copy(2 * i + 1).start()

        @pl.when(i >= 2)
        def _():
            for copy in g_copies(2 * i - 4) + g_copies(2 * i - 3):
                copy.start()

        ats = [pl.ds(pl.multiple_of(i * 64 + j * 16, 16), 16) for j in range(4)]
        lanes = [slice(k * 128, (k + 1) * 128) for k in range(tiles)]
        means, scales = [], []
        for at in ats:
            accs = [obuf[at, lanes[k]].astype(F32) for k in range(2)]
            for k in range(2, tiles):
                accs[k % 2] = accs[k % 2] + obuf[at, lanes[k]].astype(F32)
            mean = jnp.sum(accs[0] + accs[1], axis=-1, keepdims=True) * (1.0 / model)
            means.append(jnp.broadcast_to(mean, (16, 128)))
        for at, mean in zip(ats, means):
            accs = [jnp.zeros((16, 128), F32) for _ in range(2)]
            for k in range(tiles):
                centred = obuf[at, lanes[k]].astype(F32) - mean
                accs[k % 2] = accs[k % 2] + centred * centred
            var = jnp.sum(accs[0] + accs[1], axis=-1, keepdims=True) * (1.0 / model)
            scales.append(jnp.broadcast_to(lax.rsqrt(var + 1e-5), (16, 128)))
        for k in range(tiles):
            gain = jnp.concatenate([gainb[:, lanes[k]]] * 2, axis=0)
            bias = jnp.concatenate([biasb[:, lanes[k]]] * 2, axis=0)
            for at, mean, factor in zip(ats, means, scales):
                hbuf[at, lanes[k]] = ((obuf[at, lanes[k]].astype(F32) - mean) * factor * gain + bias).astype(BF16)
        return carry

    lax.fori_loop(0, rows // 64, norm, 0)
    for i in range(SLOTS):
        k_copy(i).start()
        v_copy(i).start()
    x_copy.start()

    lane_r = lax.broadcasted_iota(jnp.int32, (rows, 128), 1)

    def rotate(v):
        other = jnp.where(lane_r < 32, -pltpu.roll(v, 96, 1), pltpu.roll(v, 32, 1))
        return jnp.where(lane_r < 64, v * cosb[...] + other * sinb[...], v)

    def spread_out(slot, core, v):
        if slot < 6:
            q_ref[pl.ds(6 * core + slot, rows, stride=16), :] = v
        else:
            dst = kf if slot == 6 else vf
            dst[pl.ds(core, rows, stride=2), :] = v

    for h in range(12, 16):
        q_ref[pl.ds(h, rows, stride=16), :] = jnp.zeros((rows, 128), F32)

    for g in range(2):
        for n in range(4):
            for copy in ([q_copy(n)] if g == 0 else g_copies(n)):
                copy.wait()
        parts = [jnp.dot(hbuf[:, n * depth:(n + 1) * depth], wbuf[4 * g + n], preferred_element_type=F32) for n in range(4)]
        acc_ref[...] = (parts[0] + parts[1]) + (parts[2] + parts[3])
        if g == 0:
            pl.semaphore_wait(barrier, 2 + (z + 2) // 3 + (5 - z) // 3)
        for slot in range(4 * g, 4 * g + 4):
            v = acc_ref[:, (slot % 4) * 128:(slot % 4 + 1) * 128]
            xs[slot] = rotate(v) if slot < 7 else v
            share(slot).start()
        for slot in range(4 * g, 4 * g + 4):
            spread_out(slot, c, xs[slot])
    for slot in range(8):
        share(slot).wait_recv()
        spread_out(slot, co, xr[slot])
    kn_ref[...] = kf[...].astype(BF16)
    vn_ref[...] = vf[...].astype(BF16)

    first = s * positions
    col = lax.broadcasted_iota(jnp.int32, (16, 2 * positions), 1)
    row = lax.broadcasted_iota(jnp.int32, (16, 2 * positions), 0)
    place = jnp.where(lax.rem(col, 2) == jnp.where(row >= 6, 1, 0), first + col // 2, 1 << 30)
    pick_row = lax.broadcasted_iota(jnp.int32, (128, 16), 0)
    pick_col = lax.broadcasted_iota(jnp.int32, (128, 16), 1)
    pick = pick_col == 2 * (pick_row // 16) + jnp.where(lax.rem(pick_row, 16) >= 6, 1, 0)
    nt = (((1,), (1,)), ((), ()))

    def attention(i):
        k_copy(i).wait()
        v_copy(i).wait()
        slot = i % SLOTS
        base = first_row(i)
        spread = jnp.where(pick, 1.0, 0.0).astype(BF16)
        lane = lax.broadcasted_iota(jnp.int32, (128, 128), 1)
        begin = lax.broadcasted_iota(jnp.int32, (16, 16), 0) * 0 + first
        own_w = [None] * 4

        def scores(g):
            q8 = q_ref[pl.ds(pl.multiple_of(base * 16 + g * 128, 128), 128), :].astype(BF16)
            kn = kn_ref[pl.ds(pl.multiple_of(base * 2 + g * 16, 16), 16), :]
            self8 = lax.dot_general(q8, kn, nt, preferred_element_type=F32) * scale
            self8 = jnp.where(pick, self8, NEG)
            for b in range(8):
                at = slice(g * 128 + b * 16, g * 128 + (b + 1) * 16)
                length = len_ref[base // 128, base % 128 + g * 8 + b]
                owner = (length >= begin) & (length < begin + positions)
                sc = lax.dot_general(q8[b * 16:(b + 1) * 16, :], kbuf[slot, g * 8 + b], nt, preferred_element_type=F32) * scale
                sbuf[at, :] = jnp.where(place < length, sc, NEG)
                self_buf[at, :] = jnp.where(owner, self8[b * 16:(b + 1) * 16, :], NEG)

        def weights(g):
            at = slice(g * 128, (g + 1) * 128)
            sc = sbuf[at, :]
            own = jnp.max(self_buf[at, :], axis=1, keepdims=True)
            top = jnp.maximum(jnp.max(sc, axis=1, keepdims=True), own)
            w = jnp.exp(sc - top)
            own_w[g] = jnp.exp(own - top)
            total = jnp.sum(w, axis=1, keepdims=True) + own_w[g]
            pbuf[at, :] = w.astype(BF16)
            stat[at, :] = jnp.where(lane == 0, top, total)

        def sums(g):
            vn = vn_ref[pl.ds(pl.multiple_of(base * 2 + g * 16, 16), 16), :]
            own8 = own_w[g] * jnp.dot(spread, vn, preferred_element_type=F32)
            turned = jnp.transpose(stat[g * 128:(g + 1) * 128, :])[:8, :]
            msg[i, g, 96:104, :] = jnp.concatenate([turned[:, b * 16:b * 16 + 12] for b in range(8)] + [jnp.zeros((8, 32), F32)], axis=1)
            for b in range(8):
                at = slice(g * 128 + b * 16, g * 128 + (b + 1) * 16)
                acc = jnp.dot(pbuf[at, :], vbuf[slot, g * 8 + b], preferred_element_type=F32) + own8[b * 16:(b + 1) * 16, :]
                msg[i, g, b * 12:(b + 1) * 12, :] = acc[:12, :]

        for g in range(6):
            if g < 4:
                scores(g)
            if 1 <= g <= 4:
                weights(g - 1)
            if g >= 2:
                sums(g - 2)

    def to_partner(i):
        return remote(msg.at[i, pl.ds(2 * co, 2)], part.at[i], s_p.at[i], r_p.at[i], partner)

    def to_across(r):
        return remote(send_y.at[r], recv_y.at[r], s_y.at[r], r_y.at[r], across)

    def ctx_copy(r):
        return remote(ctx_s.at[r], ctx_r.at[r], s_c.at[r], r_c.at[r], partner)

    def merge(i, dst):
        to_partner(i).wait_recv()
        for k in range(2):
            acc, top, total, _ = scaled_sum(msg[i, 2 * c + k], part[i, k])
            dst[k, :96, :] = acc
            line = lax.broadcasted_iota(jnp.int32, (8, 128), 0)
            dst[k, 96:104, :] = jnp.where(line == 0, top, total)

    def context(r):
        to_across(r).wait_recv()
        for k in range(2):
            acc, _, _, total = scaled_sum(comb_o[r, k], recv_y[r, k])
            ctx_t[...] = acc / total
            for h in range(12):
                ctx_s[r, k * 8:(k + 1) * 8, h * 128:(h + 1) * 128] = ctx_t[pl.ds(h, 8, stride=12), :]
        ctx_copy(r).start()

    def rs(j):
        return remote(rs_out.at[j], rs_in.at[j], s_rs.at[j], r_rs.at[j], ahead)

    def rs_end(j):
        return remote(rs_out.at[j], fin.at[y, c, j], s_rs.at[j], r_re.at[j], behind)

    def final(dst, send, recv, h, core, j):
        f = fin.at[h, core, j]
        return remote(f, f, send.at[j], recv.at[j], dst)

    def ag(j):
        return final(behind, s_ag, r_ag, y, c, j)

    def ag_end(j):
        return final(ahead, s_ae, r_ag, y, c, j)

    def fy(j):
        return final(across, s_fy, r_fy, y, c, j)

    def fy_in(j):
        return final(across, s_fy, r_fy, yo, c, j)

    def fd(j):
        return final(partner, s_fd, r_fd, y, c, j)

    def fd_in(j):
        return final(partner, s_fd, r_fd, y, co, j)

    def fe(j):
        return final(partner, s_fe, r_fe, yo, c, j)

    def fe_in(j):
        return final(partner, s_fe, r_fe, yo, co, j)

    def convert(h, core, j):
        at = pl.ds(pl.multiple_of(h * 128 + (j // QCH) * 32, 32), 32)
        obuf[at, pl.ds(pl.multiple_of(core * half + (j % QCH) * width, width), width)] = fin[h, core, j].astype(BF16)

    hops = u - 2 * (u // 3)
    lag = LAG * (2 - hops)
    lag_y = lag + LAG_Y
    start = 2 * QCH + HOP * hops

    def tick(t, carry):
        i, r6 = t // PER, t // QCH

        @pl.when((t < PER * STEPS) & (t % PER == 0))
        def _():
            attention(i)
            to_partner(i).start()

            @pl.when(i < STEPS - SLOTS)
            def _():
                k_copy(i + SLOTS).start()
                v_copy(i + SLOTS).start()

            @pl.when((i >= 2) & (i < 5))
            def _():
                w_copy(2 * i - 4).start()
                w_copy(2 * i - 3).start()

        @pl.when((t % QCH == PER + 1) & (t < NMSG))
        def _():
            merge(2 * r6, send_y.at[r6])
            to_across(r6).start()

        @pl.when((t % QCH == 1) & (t >= QCH) & (t < NMSG + QCH))
        def _():
            merge(2 * r6 - 1, comb_o.at[r6 - 1])

        @pl.when((t % QCH == QCH - 2) & (t >= QCH) & (t < NMSG + QCH))
        def _():
            context(r6 - 1)

        j = t - start

        @pl.when((j >= 0) & (j < NMSG))
        def _():
            r, q = j // QCH, j % QCH

            @pl.when(q == 0)
            def _():
                ctx_copy(r).wait_recv()
                lhs[c] = ctx_s[r].astype(BF16)
                lhs[co] = ctx_r[r].astype(BF16)

            @pl.when(r == 0)
            def _():
                w_copy(q).wait()

            @pl.when(j == 0)
            def _():
                x_copy.wait()

            prod[...] = jnp.dot(lhs[...].reshape(32, lhs.shape[2]), wbuf[q], preferred_element_type=F32)

            @pl.when(u == 0)
            def _():
                rs_out[j] = prod[...]
                rs(j).start()

            @pl.when(u == 3)
            def _():
                rs_out[j] = prod[...]
                rs_end(j).start()

            @pl.when(u == 1)
            def _():
                rs(j).wait_recv()
                rs_out[j] = rs_in[j] + prod[...]
                rs(j).start()

            @pl.when(u == 2)
            def _():
                x = xbuf[pl.ds(pl.multiple_of(r * 32, 32), 32), pl.ds(pl.multiple_of(q * width, width), width)]
                rs_end(j).wait_recv()
                rs(j).wait_recv()
                fin[y, c, j] = (rs_in[j] + prod[...]) + fin[y, c, j] + x.astype(F32)
                ag(j).start()
                ag_end(j).start()
                fy(j).start()
                fd(j).start()
                convert(y, c, j)

        ja = j - lag

        @pl.when((lag > 0) & (ja >= 0) & (ja < NMSG))
        def _():
            ag(ja).wait_recv()

            @pl.when(u == 1)
            def _():
                ag(ja).start()

            fy(ja).start()
            fd(ja).start()
            convert(y, c, ja)

        jy = j - lag_y

        @pl.when((jy >= 0) & (jy < NMSG))
        def _():
            fy_in(jy).wait_recv()
            fe(jy).start()
            convert(yo, c, jy)

        return carry

    lax.fori_loop(0, start + NMSG + lag_y, tick, 0)

    def last(j, carry):
        fd_in(j).wait_recv()
        fe_in(j).wait_recv()
        convert(y, co, j)
        convert(yo, co, j)
        return carry

    lax.fori_loop(0, NMSG, last, 0)

    def drain(j, carry):
        @pl.when(u < 2)
        def _():
            rs(j).wait_send()

        @pl.when(u == 3)
        def _():
            rs_end(j).wait_send()

        @pl.when((u == 1) | (u == 2))
        def _():
            ag(j).wait_send()

        @pl.when(u == 2)
        def _():
            ag_end(j).wait_send()

        fy(j).wait_send()
        fd(j).wait_send()
        fe(j).wait_send()
        return carry

    lax.fori_loop(0, NMSG, drain, 0)
    for slot in range(8):
        share(slot).wait_send()
    for i in range(STEPS):
        to_partner(i).wait_send()
    for r in range(RCH):
        to_across(r).wait_send()
        ctx_copy(r).wait_send()


def block(lengths, gain, bias, hidden, w_q, w_k, w_v, k_cache, v_cache, w_o):
    batch, positions, kv, head = k_cache.shape
    rows, width = hidden.shape
    depth = w_o.shape[0]
    half = width // 2
    cols = half // QCH
    freq = 10000.0 ** (-2.0 * np.arange(32, dtype=np.float32) / np.float32(64))
    freq = np.concatenate([freq, freq, np.zeros(64)]).astype(np.float32).reshape(1, 128)
    dma = pltpu.SemaphoreType.DMA
    part = pltpu.VMEM((RCH, 2, 104, 128), F32)
    cache = pltpu.VMEM((SLOTS, 32, positions * kv, head), BF16)
    table = pltpu.VMEM((rows, 128), F32)
    pair = pltpu.VMEM((rows * 2, 128), F32)
    shared = pltpu.VMEM((8, rows, 128), F32)
    line = pltpu.VMEM((8, width), F32)
    new = jax.ShapeDtypeStruct((rows * kv, head), BF16)
    pin = functools.partial(pltpu.with_memory_space_constraint, memory_space=pltpu.HBM)
    return pl.pallas_call(
        functools.partial(block_kernel, positions=positions, scale=head ** -0.5),
        out_shape=(jax.ShapeDtypeStruct((rows, width), BF16), new, new),
        in_specs=[HBM] * 11,
        out_specs=(VMEM, VMEM, VMEM),
        scratch_shapes=[pltpu.SMEM((rows // 128, 128), jnp.int32), pltpu.VMEM((rows // 128, 128), jnp.int32), pltpu.VMEM((1, 128), F32),
                        pltpu.VMEM((width // 128, 128), BF16), pltpu.VMEM((width // 128, 128), BF16), dma((5,)),
                        pltpu.VMEM((rows, width), BF16), pltpu.VMEM((rows, 512), F32), pltpu.VMEM((rows * 16, 128), F32),
                        pair, pair, shared, shared, table, table, line, line,
                        dma((4,)), dma((4,)), dma((3, 4)), dma((8,)), dma((8,)),
                        cache, cache,
                        pltpu.VMEM((512, positions * kv), F32), pltpu.VMEM((512, 16), F32),
                        pltpu.VMEM((512, positions * kv), BF16), pltpu.VMEM((512, 128), F32),
                        pltpu.VMEM((STEPS, 4, 104, 128), F32), pltpu.VMEM((STEPS, 2, 104, 128), F32),
                        part, part, part,
                        pltpu.VMEM((96, 128), F32),
                        pltpu.VMEM((RCH, 16, depth), F32), pltpu.VMEM((RCH, 16, depth), F32),
                        pltpu.VMEM((2, 16, depth), BF16),
                        pltpu.VMEM((8, depth, cols), BF16),
                        pltpu.VMEM((rows // 2, half), BF16),
                        pltpu.VMEM((32, cols), F32),
                        pltpu.VMEM((NMSG, 32, cols), F32), pltpu.VMEM((NMSG, 32, cols), F32),
                        pltpu.VMEM((2, 2, NMSG, 32, cols), F32),
                        dma((SLOTS,)), dma((SLOTS,)), dma((STEPS,)), dma((STEPS,)), dma((RCH,)), dma((RCH,)),
                        dma((RCH,)), dma((RCH,)), dma((QCH,)), dma] + [dma((NMSG,))] * 12,
        compiler_params=pltpu.CompilerParams(collective_id=0, has_side_effects=True, vmem_limit_bytes=BLOCK_LIMIT),
        name="block",
    )(pin(lengths.reshape(rows // 128, 128)), pin(jnp.asarray(freq)), pin(gain.reshape(width // 128, 128)), pin(bias.reshape(width // 128, 128)),
      hidden, w_q, w_k, w_v, k_cache.reshape(batch, positions * kv, head), v_cache.reshape(batch, positions * kv, head), w_o)


def emit_kernel(*refs):
    n = len(refs) // 2
    copies = [pltpu.make_async_copy(refs[i], refs[n + i], refs[2 * n].at[i]) for i in range(n)]
    for copy in copies:
        copy.start()
    for copy in copies:
        copy.wait()


def emit(*values):
    n = len(values)
    return pl.pallas_call(
        emit_kernel,
        out_shape=tuple(jax.ShapeDtypeStruct(v.shape, v.dtype) for v in values),
        in_specs=[VMEM] * n, out_specs=(HBM,) * n,
        scratch_shapes=[pltpu.SemaphoreType.DMA((n,))],
        compiler_params=pltpu.CompilerParams(vmem_limit_bytes=4 * 1024 * 1024),
        name="emit",
    )(*values)


def solution(mesh):
    def local_step(hidden, ln_gain, ln_bias, w_q, w_k, w_v, w_o, k_cache, v_cache, lengths):
        batch, _, kv, head = k_cache.shape
        out, k_new, v_new = emit(*block(lengths, ln_gain, ln_bias, hidden, w_q, w_k, w_v, k_cache, v_cache, w_o))
        return out, k_new.reshape(batch, kv, head), v_new.reshape(batch, kv, head)

    row_spec = P('dp', None)
    cache_spec = P('dp', 'sp', 'tp', None)
    head_spec = P('dp', 'tp', None)
    return jax.shard_map(local_step, mesh=mesh, in_specs=(row_spec, P(None), P(None), P(None, 'tp'), P(None, 'tp'), P(None, 'tp'), P('tp', None), cache_spec, cache_spec, P('dp')), out_specs=(row_spec, head_spec, head_spec), check_vma=False)
```

```python
import functools

import jax
import jax.numpy as jnp
import numpy as np
from jax import lax
from jax.experimental import pallas as pl
from jax.experimental.pallas import tpu as pltpu
from jax.sharding import PartitionSpec as P

F32 = jnp.float32
BF16 = jnp.bfloat16
MESH = pl.DeviceIdType.MESH
NEG = -0.7 * float(np.finfo(np.float32).max)
BLOCK_LIMIT = 49 * 1024 * 1024
HBM = pl.BlockSpec(memory_space=pltpu.HBM)
VMEM = pl.BlockSpec(memory_space=pltpu.VMEM)


RCH = 4
QCH = 6
NMSG = RCH * QCH
PER = QCH // 2
STEPS = 2 * RCH
HOP = 3
LAG = 6
LAG_Y = 6
SLOTS = 3


def scaled_sum(a, b):
    m_a, l_a, m_b, l_b = a[96:97, :], a[97:98, :], b[96:97, :], b[97:98, :]
    top = jnp.maximum(m_a, m_b)
    f_a, f_b = jnp.exp(m_a - top), jnp.exp(m_b - top)
    total = l_a * f_a + l_b * f_b
    r = lax.broadcasted_iota(jnp.int32, (128, 128), 0)
    turned = jnp.transpose(jnp.where(r == 0, f_a, jnp.where(r == 1, f_b, total)))
    acc = a[:96, :] * turned[:96, 0:1] + b[:96, :] * turned[:96, 1:2]
    return acc, top, total, turned[:96, 2:3]


def block_kernel(len_hbm, freq_hbm, gain_hbm, bias_hbm, x_hbm, wq_hbm, wk_hbm, wv_hbm, k_hbm, v_hbm, w_hbm,
                 obuf, kn_ref, vn_ref,
                 len_ref, len_rows, freq_ref, gain_ref, bias_ref, s_in,
                 hbuf, acc_ref, q_ref, kf, vf, xs, xr, cosb, sinb, gainb, biasb, s_h, s_q, s_g, s_xs, r_xs,
                 kbuf, vbuf, sbuf, self_buf, pbuf, stat, msg, part, send_y, recv_y, comb_o, ctx_t, ctx_s, ctx_r,
                 lhs, wbuf, xbuf, prod, rs_in, rs_out, fin,
                 s_k, s_v, s_p, r_p, s_y, r_y, s_c, r_c, s_w, s_x,
                 s_rs, r_rs, r_re, s_ag, r_ag, s_ae, s_fy, r_fy, s_fd, r_fd, s_fe, r_fe, *, positions, scale):
    d, z, s = lax.axis_index("dp"), lax.axis_index("tp"), lax.axis_index("sp")
    y, c = s // 2, s % 2
    yo, co = 1 - y, 1 - c
    u = c * z + co * (3 - z)
    partner, across = (d, z, 2 * y + co), (d, z, 2 * yo + c)
    ahead, behind = (d, z + 2 * c - 1, s), (d, z - 2 * c + 1, s)
    width = wbuf.shape[2]
    half = QCH * width

    def remote(src, dst, send, recv, dev):
        return pltpu.make_async_remote_copy(src_ref=src, dst_ref=dst, send_sem=send, recv_sem=recv,
                                            device_id=dev, device_id_type=MESH)

    barrier = pltpu.get_barrier_semaphore()
    pl.semaphore_signal(barrier, inc=1, device_id=partner, device_id_type=MESH)
    pl.semaphore_signal(barrier, inc=1, device_id=across, device_id_type=MESH)

    @pl.when(u < 3)
    def _():
        pl.semaphore_signal(barrier, inc=1, device_id=ahead, device_id_type=MESH)

    @pl.when(u > 0)
    def _():
        pl.semaphore_signal(barrier, inc=1, device_id=behind, device_id_type=MESH)

    def first_row(i):
        return 128 * ((i % 2) * y + (1 - i % 2) * yo) + 32 * (i // 2)

    def k_copy(i):
        return pltpu.make_async_copy(k_hbm.at[pl.ds(first_row(i), 32)], kbuf.at[i % SLOTS], s_k.at[i % SLOTS])

    def v_copy(i):
        return pltpu.make_async_copy(v_hbm.at[pl.ds(first_row(i), 32)], vbuf.at[i % SLOTS], s_v.at[i % SLOTS])

    def w_copy(q):
        return pltpu.make_async_copy(w_hbm.at[:, pl.ds(c * half + q * width, width)], wbuf.at[q], s_w.at[q])

    x_copy = pltpu.make_async_copy(x_hbm.at[pl.ds(y * 128, 128), pl.ds(c * half, half)], xbuf, s_x)

    rows, model = hbuf.shape
    tiles = model // 128
    depth = wbuf.shape[1]

    def h_copy(i):
        at = pl.ds(i * 64, 64)
        return pltpu.make_async_copy(x_hbm.at[at], obuf.at[at], s_h.at[i])

    inputs = ((len_hbm, len_ref), (len_hbm, len_rows), (freq_hbm, freq_ref), (gain_hbm, gain_ref), (bias_hbm, bias_ref))
    small = [pltpu.make_async_copy(src, dst, s_in.at[n]) for n, (src, dst) in enumerate(inputs)]
    for copy in small:
        copy.start()
    for i in range(rows // 64):
        h_copy(i).start()

    def q_copy(n):
        return pltpu.make_async_copy(wq_hbm.at[pl.ds(n * depth, depth), pl.ds(c * 768, 512)], wbuf.at[n], s_q.at[n])

    def g_copies(n):
        at = pl.ds(n * depth, depth)
        return [pltpu.make_async_copy(wq_hbm.at[at, pl.ds(c * 768 + 512, 256)], wbuf.at[4 + n, :, pl.ds(0, 256)], s_g.at[0, n]),
                pltpu.make_async_copy(wk_hbm.at[at, pl.ds(c * 128, 128)], wbuf.at[4 + n, :, pl.ds(256, 128)], s_g.at[1, n]),
                pltpu.make_async_copy(wv_hbm.at[at, pl.ds(c * 128, 128)], wbuf.at[4 + n, :, pl.ds(384, 128)], s_g.at[2, n])]

    def share(slot):
        return remote(xs.at[slot], xr.at[slot], s_xs.at[slot], r_xs.at[slot], partner)

    for copy in small:
        copy.wait()
    for k in range(tiles):
        gainb[:, k * 128:(k + 1) * 128] = jnp.broadcast_to(1.0 + gain_ref[k:k + 1, :].astype(F32), (8, 128))
        biasb[:, k * 128:(k + 1) * 128] = jnp.broadcast_to(bias_ref[k:k + 1, :].astype(F32), (8, 128))
    for i in range(rows // 128):
        angle = jnp.transpose(jnp.broadcast_to(len_rows[i:i + 1, :].astype(F32), (128, 128))) * freq_ref[...]
        cosb[i * 128:(i + 1) * 128, :] = jnp.cos(angle)
        sinb[i * 128:(i + 1) * 128, :] = jnp.sin(angle)

    def norm(i, carry):
        h_copy(i).wait()

        @pl.when(i < 2)
        def _():
            q_copy(2 * i).start()
            q_copy(2 * i + 1).start()

        @pl.when(i >= 2)
        def _():
            for copy in g_copies(2 * i - 4) + g_copies(2 * i - 3):
                copy.start()

        ats = [pl.ds(pl.multiple_of(i * 64 + j * 16, 16), 16) for j in range(4)]
        lanes = [slice(k * 128, (k + 1) * 128) for k in range(tiles)]
        means, scales = [], []
        for at in ats:
            accs = [obuf[at, lanes[k]].astype(F32) for k in range(2)]
            for k in range(2, tiles):
                accs[k % 2] = accs[k % 2] + obuf[at, lanes[k]].astype(F32)
            mean = jnp.sum(accs[0] + accs[1], axis=-1, keepdims=True) * (1.0 / model)
            means.append(jnp.broadcast_to(mean, (16, 128)))
        for at, mean in zip(ats, means):
            accs = [jnp.zeros((16, 128), F32) for _ in range(2)]
            for k in range(tiles):
                centred = obuf[at, lanes[k]].astype(F32) - mean
                accs[k % 2] = accs[k % 2] + centred * centred
            var = jnp.sum(accs[0] + accs[1], axis=-1, keepdims=True) * (1.0 / model)
            scales.append(jnp.broadcast_to(lax.rsqrt(var + 1e-5), (16, 128)))
        for k in range(tiles):
            gain = jnp.concatenate([gainb[:, lanes[k]]] * 2, axis=0)
            bias = jnp.concatenate([biasb[:, lanes[k]]] * 2, axis=0)
            for at, mean, factor in zip(ats, means, scales):
                hbuf[at, lanes[k]] = ((obuf[at, lanes[k]].astype(F32) - mean) * factor * gain + bias).astype(BF16)
        return carry

    lax.fori_loop(0, rows // 64, norm, 0)
    for i in range(SLOTS):
        k_copy(i).start()
        v_copy(i).start()
    x_copy.start()

    lane_r = lax.broadcasted_iota(jnp.int32, (rows, 128), 1)

    def rotate(v):
        other = jnp.where(lane_r < 32, -pltpu.roll(v, 96, 1), pltpu.roll(v, 32, 1))
        return jnp.where(lane_r < 64, v * cosb[...] + other * sinb[...], v)

    def spread_out(slot, core, v):
        if slot < 6:
            q_ref[pl.ds(6 * core + slot, rows, stride=16), :] = v
        else:
            dst = kf if slot == 6 else vf
            dst[pl.ds(core, rows, stride=2), :] = v

    for h in range(12, 16):
        q_ref[pl.ds(h, rows, stride=16), :] = jnp.zeros((rows, 128), F32)

    for g in range(2):
        for n in range(4):
            for copy in ([q_copy(n)] if g == 0 else g_copies(n)):
                copy.wait()
        parts = [jnp.dot(hbuf[:, n * depth:(n + 1) * depth], wbuf[4 * g + n], preferred_element_type=F32) for n in range(4)]
        acc_ref[...] = (parts[0] + parts[1]) + (parts[2] + parts[3])
        if g == 0:
            pl.semaphore_wait(barrier, 2 + (z + 2) // 3 + (5 - z) // 3)
        for slot in range(4 * g, 4 * g + 4):
            v = acc_ref[:, (slot % 4) * 128:(slot % 4 + 1) * 128]
            xs[slot] = rotate(v) if slot < 7 else v
            share(slot).start()
        for slot in range(4 * g, 4 * g + 4):
            spread_out(slot, c, xs[slot])
    for slot in range(8):
        share(slot).wait_recv()
        spread_out(slot, co, xr[slot])
    kn_ref[...] = kf[...].astype(BF16)
    vn_ref[...] = vf[...].astype(BF16)

    first = s * positions
    col = lax.broadcasted_iota(jnp.int32, (16, 2 * positions), 1)
    row = lax.broadcasted_iota(jnp.int32, (16, 2 * positions), 0)
    place = jnp.where(lax.rem(col, 2) == jnp.where(row >= 6, 1, 0), first + col // 2, 1 << 30)
    pick_row = lax.broadcasted_iota(jnp.int32, (128, 16), 0)
    pick_col = lax.broadcasted_iota(jnp.int32, (128, 16), 1)
    pick = pick_col == 2 * (pick_row // 16) + jnp.where(lax.rem(pick_row, 16) >= 6, 1, 0)
    nt = (((1,), (1,)), ((), ()))

    def attention(i):
        k_copy(i).wait()
        v_copy(i).wait()
        slot = i % SLOTS
        base = first_row(i)
        spread = jnp.where(pick, 1.0, 0.0).astype(BF16)
        lane = lax.broadcasted_iota(jnp.int32, (128, 128), 1)
        begin = lax.broadcasted_iota(jnp.int32, (16, 16), 0) * 0 + first
        own_w = [None] * 4

        def scores(g):
            q8 = q_ref[pl.ds(pl.multiple_of(base * 16 + g * 128, 128), 128), :].astype(BF16)
            kn = kn_ref[pl.ds(pl.multiple_of(base * 2 + g * 16, 16), 16), :]
            self8 = lax.dot_general(q8, kn, nt, preferred_element_type=F32) * scale
            self8 = jnp.where(pick, self8, NEG)
            for b in range(8):
                at = slice(g * 128 + b * 16, g * 128 + (b + 1) * 16)
                length = len_ref[base // 128, base % 128 + g * 8 + b]
                owner = (length >= begin) & (length < begin + positions)
                sc = lax.dot_general(q8[b * 16:(b + 1) * 16, :], kbuf[slot, g * 8 + b], nt, preferred_element_type=F32) * scale
                sbuf[at, :] = jnp.where(place < length, sc, NEG)
                self_buf[at, :] = jnp.where(owner, self8[b * 16:(b + 1) * 16, :], NEG)

        def weights(g):
            at = slice(g * 128, (g + 1) * 128)
            sc = sbuf[at, :]
            own = jnp.max(self_buf[at, :], axis=1, keepdims=True)
            top = jnp.maximum(jnp.max(sc, axis=1, keepdims=True), own)
            w = jnp.exp(sc - top)
            own_w[g] = jnp.exp(own - top)
            total = jnp.sum(w, axis=1, keepdims=True) + own_w[g]
            pbuf[at, :] = w.astype(BF16)
            stat[at, :] = jnp.where(lane == 0, top, total)

        def sums(g):
            vn = vn_ref[pl.ds(pl.multiple_of(base * 2 + g * 16, 16), 16), :]
            own8 = own_w[g] * jnp.dot(spread, vn, preferred_element_type=F32)
            turned = jnp.transpose(stat[g * 128:(g + 1) * 128, :])[:8, :]
            msg[i, g, 96:104, :] = jnp.concatenate([turned[:, b * 16:b * 16 + 12] for b in range(8)] + [jnp.zeros((8, 32), F32)], axis=1)
            for b in range(8):
                at = slice(g * 128 + b * 16, g * 128 + (b + 1) * 16)
                acc = jnp.dot(pbuf[at, :], vbuf[slot, g * 8 + b], preferred_element_type=F32) + own8[b * 16:(b + 1) * 16, :]
                msg[i, g, b * 12:(b + 1) * 12, :] = acc[:12, :]

        for g in range(6):
            if g < 4:
                scores(g)
            if 1 <= g <= 4:
                weights(g - 1)
            if g >= 2:
                sums(g - 2)

    def to_partner(i):
        return remote(msg.at[i, pl.ds(2 * co, 2)], part.at[i], s_p.at[i], r_p.at[i], partner)

    def to_across(r):
        return remote(send_y.at[r], recv_y.at[r], s_y.at[r], r_y.at[r], across)

    def ctx_copy(r):
        return remote(ctx_s.at[r], ctx_r.at[r], s_c.at[r], r_c.at[r], partner)

    def merge(i, dst):
        to_partner(i).wait_recv()
        for k in range(2):
            acc, top, total, _ = scaled_sum(msg[i, 2 * c + k], part[i, k])
            dst[k, :96, :] = acc
            line = lax.broadcasted_iota(jnp.int32, (8, 128), 0)
            dst[k, 96:104, :] = jnp.where(line == 0, top, total)

    def context(r):
        to_across(r).wait_recv()
        for k in range(2):
            acc, _, _, total = scaled_sum(comb_o[r, k], recv_y[r, k])
            ctx_t[...] = acc / total
            for h in range(12):
                ctx_s[r, k * 8:(k + 1) * 8, h * 128:(h + 1) * 128] = ctx_t[pl.ds(h, 8, stride=12), :]
        ctx_copy(r).start()

    def rs(j):
        return remote(rs_out.at[j], rs_in.at[j], s_rs.at[j], r_rs.at[j], ahead)

    def rs_end(j):
        return remote(rs_out.at[j], fin.at[y, c, j], s_rs.at[j], r_re.at[j], behind)

    def final(dst, send, recv, h, core, j):
        f = fin.at[h, core, j]
        return remote(f, f, send.at[j], recv.at[j], dst)

    def ag(j):
        return final(behind, s_ag, r_ag, y, c, j)

    def ag_end(j):
        return final(ahead, s_ae, r_ag, y, c, j)

    def fy(j):
        return final(across, s_fy, r_fy, y, c, j)

    def fy_in(j):
        return final(across, s_fy, r_fy, yo, c, j)

    def fd(j):
        return final(partner, s_fd, r_fd, y, c, j)

    def fd_in(j):
        return final(partner, s_fd, r_fd, y, co, j)

    def fe(j):
        return final(partner, s_fe, r_fe, yo, c, j)

    def fe_in(j):
        return final(partner, s_fe, r_fe, yo, co, j)

    def convert(h, core, j):
        at = pl.ds(pl.multiple_of(h * 128 + (j // QCH) * 32, 32), 32)
        obuf[at, pl.ds(pl.multiple_of(core * half + (j % QCH) * width, width), width)] = fin[h, core, j].astype(BF16)

    hops = u - 2 * (u // 3)
    lag = LAG * (2 - hops)
    lag_y = lag + LAG_Y
    start = 2 * QCH + HOP * hops

    def tick(t, carry):
        i, r6 = t // PER, t // QCH

        @pl.when((t < PER * STEPS) & (t % PER == 0))
        def _():
            attention(i)
            to_partner(i).start()

            @pl.when(i < STEPS - SLOTS)
            def _():
                k_copy(i + SLOTS).start()
                v_copy(i + SLOTS).start()

            @pl.when((i >= 2) & (i < 5))
            def _():
                w_copy(2 * i - 4).start()
                w_copy(2 * i - 3).start()

        @pl.when((t % QCH == PER + 1) & (t < NMSG))
        def _():
            merge(2 * r6, send_y.at[r6])
            to_across(r6).start()

        @pl.when((t % QCH == 1) & (t >= QCH) & (t < NMSG + QCH))
        def _():
            merge(2 * r6 - 1, comb_o.at[r6 - 1])

        @pl.when((t % QCH == QCH - 2) & (t >= QCH) & (t < NMSG + QCH))
        def _():
            context(r6 - 1)

        j = t - start

        @pl.when((j >= 0) & (j < NMSG))
        def _():
            r, q = j // QCH, j % QCH

            @pl.when(q == 0)
            def _():
                ctx_copy(r).wait_recv()
                lhs[c] = ctx_s[r].astype(BF16)
                lhs[co] = ctx_r[r].astype(BF16)

            @pl.when(r == 0)
            def _():
                w_copy(q).wait()

            @pl.when(j == 0)
            def _():
                x_copy.wait()

            prod[...] = jnp.dot(lhs[...].reshape(32, lhs.shape[2]), wbuf[q], preferred_element_type=F32)

            @pl.when(u == 0)
            def _():
                rs_out[j] = prod[...]
                rs(j).start()

            @pl.when(u == 3)
            def _():
                rs_out[j] = prod[...]
                rs_end(j).start()

            @pl.when(u == 1)
            def _():
                rs(j).wait_recv()
                rs_out[j] = rs_in[j] + prod[...]
                rs(j).start()

            @pl.when(u == 2)
            def _():
                x = xbuf[pl.ds(pl.multiple_of(r * 32, 32), 32), pl.ds(pl.multiple_of(q * width, width), width)]
                rs_end(j).wait_recv()
                rs(j).wait_recv()
                fin[y, c, j] = (rs_in[j] + prod[...]) + fin[y, c, j] + x.astype(F32)
                ag(j).start()
                ag_end(j).start()
                fy(j).start()
                fd(j).start()
                convert(y, c, j)

        ja = j - lag

        @pl.when((lag > 0) & (ja >= 0) & (ja < NMSG))
        def _():
            ag(ja).wait_recv()

            @pl.when(u == 1)
            def _():
                ag(ja).start()

            fy(ja).start()
            fd(ja).start()
            convert(y, c, ja)

        jy = j - lag_y

        @pl.when((jy >= 0) & (jy < NMSG))
        def _():
            fy_in(jy).wait_recv()
            fe(jy).start()
            convert(yo, c, jy)

        return carry

    lax.fori_loop(0, start + NMSG + lag_y, tick, 0)

    def last(j, carry):
        fd_in(j).wait_recv()
        fe_in(j).wait_recv()
        convert(y, co, j)
        convert(yo, co, j)
        return carry

    lax.fori_loop(0, NMSG, last, 0)

    def drain(j, carry):
        @pl.when(u < 2)
        def _():
            rs(j).wait_send()

        @pl.when(u == 3)
        def _():
            rs_end(j).wait_send()

        @pl.when((u == 1) | (u == 2))
        def _():
            ag(j).wait_send()

        @pl.when(u == 2)
        def _():
            ag_end(j).wait_send()

        fy(j).wait_send()
        fd(j).wait_send()
        fe(j).wait_send()
        return carry

    lax.fori_loop(0, NMSG, drain, 0)
    for slot in range(8):
        share(slot).wait_send()
    for i in range(STEPS):
        to_partner(i).wait_send()
    for r in range(RCH):
        to_across(r).wait_send()
        ctx_copy(r).wait_send()


def block(lengths, gain, bias, hidden, w_q, w_k, w_v, k_cache, v_cache, w_o):
    batch, positions, kv, head = k_cache.shape
    rows, width = hidden.shape
    depth = w_o.shape[0]
    half = width // 2
    cols = half // QCH
    freq = 10000.0 ** (-2.0 * np.arange(32, dtype=np.float32) / np.float32(64))
    freq = np.concatenate([freq, freq, np.zeros(64)]).astype(np.float32).reshape(1, 128)
    dma = pltpu.SemaphoreType.DMA
    part = pltpu.VMEM((RCH, 2, 104, 128), F32)
    cache = pltpu.VMEM((SLOTS, 32, positions * kv, head), BF16)
    table = pltpu.VMEM((rows, 128), F32)
    pair = pltpu.VMEM((rows * 2, 128), F32)
    shared = pltpu.VMEM((8, rows, 128), F32)
    line = pltpu.VMEM((8, width), F32)
    new = jax.ShapeDtypeStruct((rows * kv, head), BF16)
    pin = functools.partial(pltpu.with_memory_space_constraint, memory_space=pltpu.HBM)
    return pl.pallas_call(
        functools.partial(block_kernel, positions=positions, scale=head ** -0.5),
        out_shape=(jax.ShapeDtypeStruct((rows, width), BF16), new, new),
        in_specs=[HBM] * 11,
        out_specs=(VMEM, VMEM, VMEM),
        scratch_shapes=[pltpu.SMEM((rows // 128, 128), jnp.int32), pltpu.VMEM((rows // 128, 128), jnp.int32), pltpu.VMEM((1, 128), F32),
                        pltpu.VMEM((width // 128, 128), BF16), pltpu.VMEM((width // 128, 128), BF16), dma((5,)),
                        pltpu.VMEM((rows, width), BF16), pltpu.VMEM((rows, 512), F32), pltpu.VMEM((rows * 16, 128), F32),
                        pair, pair, shared, shared, table, table, line, line,
                        dma((4,)), dma((4,)), dma((3, 4)), dma((8,)), dma((8,)),
                        cache, cache,
                        pltpu.VMEM((512, positions * kv), F32), pltpu.VMEM((512, 16), F32),
                        pltpu.VMEM((512, positions * kv), BF16), pltpu.VMEM((512, 128), F32),
                        pltpu.VMEM((STEPS, 4, 104, 128), F32), pltpu.VMEM((STEPS, 2, 104, 128), F32),
                        part, part, part,
                        pltpu.VMEM((96, 128), F32),
                        pltpu.VMEM((RCH, 16, depth), F32), pltpu.VMEM((RCH, 16, depth), F32),
                        pltpu.VMEM((2, 16, depth), BF16),
                        pltpu.VMEM((8, depth, cols), BF16),
                        pltpu.VMEM((rows // 2, half), BF16),
                        pltpu.VMEM((32, cols), F32),
                        pltpu.VMEM((NMSG, 32, cols), F32), pltpu.VMEM((NMSG, 32, cols), F32),
                        pltpu.VMEM((2, 2, NMSG, 32, cols), F32),
                        dma((SLOTS,)), dma((SLOTS,)), dma((STEPS,)), dma((STEPS,)), dma((RCH,)), dma((RCH,)),
                        dma((RCH,)), dma((RCH,)), dma((QCH,)), dma] + [dma((NMSG,))] * 12,
        compiler_params=pltpu.CompilerParams(collective_id=0, has_side_effects=True, vmem_limit_bytes=BLOCK_LIMIT),
        name="block",
    )(pin(lengths.reshape(rows // 128, 128)), pin(jnp.asarray(freq)), pin(gain.reshape(width // 128, 128)), pin(bias.reshape(width // 128, 128)),
      hidden, w_q, w_k, w_v, k_cache.reshape(batch, positions * kv, head), v_cache.reshape(batch, positions * kv, head), w_o)


def emit_kernel(*refs):
    n = len(refs) // 2
    copies = [pltpu.make_async_copy(refs[i], refs[n + i], refs[2 * n].at[i]) for i in range(n)]
    for copy in copies:
        copy.start()
    for copy in copies:
        copy.wait()


def emit(*values):
    n = len(values)
    return pl.pallas_call(
        emit_kernel,
        out_shape=tuple(jax.ShapeDtypeStruct(v.shape, v.dtype) for v in values),
        in_specs=[VMEM] * n, out_specs=(HBM,) * n,
        scratch_shapes=[pltpu.SemaphoreType.DMA((n,))],
        compiler_params=pltpu.CompilerParams(vmem_limit_bytes=4 * 1024 * 1024),
        name="emit",
    )(*values)


def solution(mesh):
    def local_step(hidden, ln_gain, ln_bias, w_q, w_k, w_v, w_o, k_cache, v_cache, lengths):
        batch, _, kv, head = k_cache.shape
        out, k_new, v_new = emit(*block(lengths, ln_gain, ln_bias, hidden, w_q, w_k, w_v, k_cache, v_cache, w_o))
        return out, k_new.reshape(batch, kv, head), v_new.reshape(batch, kv, head)

    row_spec = P('dp', None)
    cache_spec = P('dp', 'sp', 'tp', None)
    head_spec = P('dp', 'tp', None)
    return jax.shard_map(local_step, mesh=mesh, in_specs=(row_spec, P(None), P(None), P(None, 'tp'), P(None, 'tp'), P(None, 'tp'), P('tp', None), cache_spec, cache_spec, P('dp')), out_specs=(row_spec, head_spec, head_spec), check_vma=False)
```
